128 devices in a mesh: section: 2 (over core), dev: 64 (over x, z, y).
Axes of the slice: x: 4, y: 4, z: 4, core: 2. Of those that a mesh axis runs over, the one named last changes fastest.
Arguments:
- indices: int32 [8192, 32, 8], P(('section', 'dev')), may hold values from 0 to 131071
- pool_len: int32 [32], replicated, may hold values from 1 to 8
- tables: bfloat16 [4194304, 128], P(('section', 'dev')), may hold values from -3 to 3
- w_first: bfloat16 [4096, 4096], P('dev', 'section'), may hold values from -0.09375 to 0.09375
- b_first: bfloat16 [4096], P('section'), may hold values from -3 to 3
- w_out: bfloat16 [4096], P('section'), may hold values from -0.09375 to 0.09375
Outputs:
- logits: float32 [8192], P('dev')
The draws below stay inside these ranges and needn't reach their ends.
Inputs may be any that keep to these rules, and one draw needn't show every extreme that they name: `indices`: ids of rows of the table named by the second index.
All inputs are finite; a program needn't handle non-finite values.
Results may differ from the reference program's by a relative error of at most 0.0095.
Values may be sent and summed in bfloat16 or wider, within the bound.
No kernel may reach another device: no remote copies, remote signals or barrier semaphores. Data moves between devices by JAX's collectives and lax.ppermute only.
A program may use at most 128 MiB of HBM per device.

```python
import jax
import jax.numpy as jnp
from jax import lax

E = 128
HID = 4096
TABLES = 32
POOL = 8
ROWS_DEV = 32768
RSPLIT = 4
ROWS = 131072
FEAT = 4096
BATCH = 8192


def plant(array, key, low, top_value):
    longest = array.shape.index(max(array.shape))
    spots = []
    for shift in (0, 1):
        where = [jax.random.randint(jax.random.fold_in(key, axis), (), 0, length) for axis, length in enumerate(array.shape)]
        where[longest] = (where[longest] + shift) % array.shape[longest]
        spots.append(tuple(where))
    return array.at[spots[0]].set(low).at[spots[1]].set(top_value)


def block_levels(key, shape, split, smallest, largest):
    level, own = 1.0, jax.random.fold_in(key, 6)
    for position, parts in split:
        draws = jnp.exp(jax.random.uniform(jax.random.fold_in(own, position), (parts,), jnp.float32, smallest / len(split), largest / len(split)))
        level = level * jnp.repeat(draws, shape[position] // parts).reshape([-1 if axis == position else 1 for axis in range(len(shape))])
    return level


def scatter_about(rng, dims, spread, limit, split=(), dtype=jnp.bfloat16):
    factor_of = block_levels(rng, dims, split, -0.22, 0.18) if split else 1.0
    values = jax.random.normal(rng, dims, jnp.float32) * spread * factor_of
    return jnp.minimum(jnp.maximum(values, -limit), limit).astype(dtype)


def setup_inputs(seed: int = 0) -> dict:
    arg_keys = jax.random.split(jax.random.key(seed), 7)
    indices = plant(jax.random.randint(arg_keys[0], (BATCH, TABLES, POOL), 0, ROWS), jax.random.fold_in(arg_keys[0], 1), 0, ROWS - 1).astype(jnp.int32)
    pool_len = plant(jax.random.randint(arg_keys[1], (TABLES,), 1, POOL + 1), jax.random.fold_in(arg_keys[1], 1), 1, POOL).astype(jnp.int32)
    tables = scatter_about(arg_keys[2], (TABLES * ROWS, E), 0.5, 3.0, ((0, 128),))
    w_first = scatter_about(arg_keys[3], (FEAT, HID), FEAT ** -0.5, 0.09375, ((0, 64), (1, 2)))
    b_first = scatter_about(arg_keys[4], (HID,), 0.5, 3.0, ((0, 2),))
    w_out = scatter_about(arg_keys[5], (HID,), HID ** -0.5, 0.09375, ((0, 2),))
    return {"indices": indices, "pool_len": pool_len, "tables": tables, "w_first": w_first, "b_first": b_first, "w_out": w_out}


def pool_table(inputs):
    table_rows, bag_ids, live_count = inputs
    gathered = jnp.take(table_rows, bag_ids, axis=0).astype(jnp.float32)
    slot_live = (jnp.arange(POOL) < live_count).astype(jnp.float32)
    row_block = bag_ids // ROWS_DEV
    owners = (row_block[:, :, None] == jnp.arange(RSPLIT)[None, None, :]).astype(jnp.float32)
    owners = owners * slot_live[None, :, None]
    partial_value = jnp.einsum('bpr,bpe->rbe', owners, gathered).astype(jnp.bfloat16)
    return jnp.sum(partial_value.astype(jnp.float32), axis=0).astype(jnp.bfloat16)


def reference(indices, pool_len, tables, w_first, b_first, w_out):
    table_view = tables.reshape(TABLES, ROWS, E)
    pooled = lax.map(pool_table, (table_view, jnp.transpose(indices, (1, 0, 2)), pool_len))
    flat_feat = jnp.transpose(pooled, (1, 0, 2)).reshape(BATCH, FEAT)
    pre_act = jnp.dot(flat_feat, w_first, preferred_element_type=jnp.float32) + b_first.astype(jnp.float32)
    hidden = jnp.maximum(pre_act, 0.0)
    return jnp.sum(hidden * w_out.astype(jnp.float32)[None, :], axis=1)
```

```python
import functools

import jax
import jax.numpy as jnp
from jax import lax
from jax.experimental import pallas as pl
from jax.experimental.pallas import tpu as pltpu
from jax.sharding import PartitionSpec as P

E = 128
ROWS_DEV = 32768
POOL = 8
CHUNK = 64
SLOTS = POOL * CHUNK
DEAD = ROWS_DEV | (8 << 16)
PIECES = 8
TBLK = 4096
SORT8 = (
    (0, 2), (1, 3), (4, 6), (5, 7), (0, 4), (1, 5), (2, 6), (3, 7), (0, 1), (2, 3),
    (4, 5), (6, 7), (2, 4), (3, 5), (1, 4), (3, 6), (1, 2), (3, 4), (5, 6),
)


def prep_body(x_ref, live_ref, list_ref, bag_ref):
    shape = (CHUNK, 128)
    lane = lax.broadcasted_iota(jnp.int32, shape, 1)
    bag = lax.broadcasted_iota(jnp.int32, shape, 0)
    first = ((lane >> 1) & 3) * ROWS_DEV
    live = jnp.broadcast_to(live_ref[...], shape)
    v = []
    for p in range(POOL):
        row = x_ref[p] - first
        ok = (row >= 0) & (row < ROWS_DEV) & (live > p)
        v.append(jnp.where(ok, row, ROWS_DEV))
    for a, b in SORT8:
        v[a], v[b] = jnp.minimum(v[a], v[b]), jnp.maximum(v[a], v[b])
    kept = sum((w < ROWS_DEV).astype(jnp.int32) for w in v)
    cols = [(POOL - kept) * CHUNK + bag]
    cols += [v[2 * k] | (v[2 * k + 1] << 16) for k in range(POOL // 2)]
    size = 2
    while size <= CHUNK:
        step = size // 2
        while step:
            upper = (bag & step) != 0
            small = ((bag & size) == 0) != upper
            other = [
                jnp.where(upper, pltpu.roll(c, step, 0), pltpu.roll(c, CHUNK - step, 0)) for c in cols
            ]
            take = jnp.where(small, other[0] - cols[0], cols[0] - other[0]) < 0
            cols = [jnp.where(take, o, c) for o, c in zip(other, cols)]
            step //= 2
        size *= 2
    key = cols[0]
    bag_ref[...] = (key & (CHUNK - 1)).T
    kept = POOL - (key >> 6)
    v = []
    for w in cols[1:]:
        v += [w & 0xFFFF, lax.shift_right_logical(w, 16)]
    tile = (8, 128)
    groups = []
    total = jnp.zeros((1, 128), jnp.int32)
    for g in range(CHUNK // 8):
        n = kept[8 * g : 8 * g + 1]
        shift = jnp.broadcast_to((8 * g - total) << 20, tile)
        n_all = jnp.broadcast_to(n, tile)
        for p in range(POOL):
            word = v[p][8 * g : 8 * g + 8] | (g << 16) | shift
            groups.append(jnp.where(n_all > p, word, DEAD))
        total = total + n
    for k in range(6):
        gap = 1 << k
        moves = [((w >> (20 + k)) & 1) != 0 for w in groups]
        new = []
        for i in range(64):
            stay = jnp.where(moves[i], DEAD, groups[i])
            if i + gap < 64:
                stay = jnp.where(moves[i + gap], groups[i + gap], stay)
            new.append(stay)
        groups = new
    head = lax.broadcasted_iota(jnp.int32, tile, 0) == 0
    mask = jnp.where(head, 0xFFFFF, 0xFFFF)
    groups = [w & mask for w in groups]
    groups[0] = groups[0] | jnp.where(head, jnp.broadcast_to(total << 20, tile), 0)
    for i in range(4):
        block = jnp.concatenate(groups[16 * i : 16 * i + 16], axis=0)
        list_ref[:, 128 * i : 128 * i + 128] = block.T


def prep(x, live):
    return pl.pallas_call(
        prep_body,
        out_shape=(
            jax.ShapeDtypeStruct((128, SLOTS), jnp.int32),
            jax.ShapeDtypeStruct((128, CHUNK), jnp.int32),
        ),
        name="bag_lists",
    )(x, live)


def gather_body(lists_ref, table_ref, out_ref, tab, tbuf, smem, acc, tsem, lsem, *, unroll):
    chunks = out_ref.shape[0]
    piece = chunks * SLOTS // PIECES

    def list_copy(i):
        part = pl.ds(i * piece, piece)
        return pltpu.make_async_copy(lists_ref.at[part], smem.at[part], lsem.at[i])

    def table_copy(b):
        return pltpu.make_async_copy(
            table_ref.at[pl.ds(b * TBLK, TBLK)], tbuf.at[b % 2], tsem.at[b % 2]
        )

    blocks = ROWS_DEV // TBLK
    table_copy(0).start()
    for i in range(PIECES):
        list_copy(i).start()
    tab[pl.ds(ROWS_DEV, 8), :] = jnp.zeros((8, E), jnp.float32)
    for b in range(blocks):
        if b + 1 < blocks:
            table_copy(b + 1).start()
        table_copy(b).wait()
        tab[pl.ds(b * TBLK, TBLK), :] = tbuf[b % 2].astype(jnp.float32)

    def level(base):
        head = smem[base]
        rows = [head & 0xFFFF] + [smem[base + i] for i in range(1, 8)]
        return (head >> 16) & 15, jnp.concatenate([tab[pl.ds(r, 1), :] for r in rows], axis=0)

    def chunk(c, carry):
        base = c * SLOTS
        acc[...] = jnp.zeros(acc.shape, jnp.float32)
        levels = smem[base] >> 20

        def step(k, carry):
            at = base + k * (8 * unroll)
            for g, rows in [level(at + 8 * u) for u in range(unroll)]:
                acc[pl.ds(pl.multiple_of(g * 8, 8), 8), :] += rows
            return carry

        lax.fori_loop(0, (levels + unroll - 1) // unroll, step, 0)
        out_ref[c] = acc[pl.ds(0, CHUNK), :].astype(jnp.bfloat16)
        return carry

    per = chunks // PIECES
    for i in range(PIECES):
        list_copy(i).wait()
        lax.fori_loop(i * per, (i + 1) * per, chunk, 0)


def gather(lists, table, chunks, unroll=4):
    return pl.pallas_call(
        functools.partial(gather_body, unroll=unroll),
        out_shape=jax.ShapeDtypeStruct((chunks, CHUNK, E), jnp.bfloat16),
        in_specs=[pl.BlockSpec(memory_space=pl.ANY), pl.BlockSpec(memory_space=pl.ANY)],
        out_specs=pl.BlockSpec(memory_space=pltpu.VMEM),
        scratch_shapes=[
            pltpu.VMEM((ROWS_DEV + 8, E), jnp.float32),
            pltpu.VMEM((2, TBLK, E), jnp.bfloat16),
            pltpu.SMEM((chunks * SLOTS,), jnp.int32),
            pltpu.VMEM((CHUNK + 8, E), jnp.float32),
            pltpu.SemaphoreType.DMA((2,)),
            pltpu.SemaphoreType.DMA((PIECES,)),
        ],
        compiler_params=pltpu.CompilerParams(vmem_limit_bytes=32 * 2**20),
        name="bag_gather",
    )(lists, table)


def unsort_body(part_ref, bag_ref, out_ref):
    tables = out_ref.shape[1] // E
    bag = lax.broadcasted_iota(jnp.int32, (CHUNK, 4 * CHUNK), 0)
    for t in range(tables):
        for h in range(2):
            where = bag_ref[2 * t + h : 2 * t + h + 1, :]
            pick = (bag == where).astype(jnp.float32).astype(jnp.bfloat16)
            rows = part_ref[4 * t : 4 * t + 4, h].reshape(4 * CHUNK, E)
            total = jnp.dot(pick, rows, preferred_element_type=jnp.float32)
            out_ref[h * CHUNK : (h + 1) * CHUNK, t * E : (t + 1) * E] = total.astype(jnp.bfloat16)


def unsort(parts, bags):
    return pl.pallas_call(
        unsort_body,
        out_shape=jax.ShapeDtypeStruct((2 * CHUNK, parts.shape[0] // 4 * E), jnp.bfloat16),
        name="bag_unsort",
    )(parts, bags)


def swap(x, axis):
    return lax.all_to_all(jnp.broadcast_to(x[None], (2, *x.shape)), axis, 0, 0, tiled=True)


def body(indices, pool_len, tables, w_first, b_first, w_out):
    n_dev = lax.axis_size("dev")
    n_sec = lax.axis_size("section")
    n_tables = indices.shape[1]
    half = n_tables // n_sec
    section = lax.axis_index("section")
    dev = lax.axis_index("dev")
    ids = jnp.transpose(indices, (1, 2, 0)).reshape(n_sec, half, POOL, CHUNK)
    odd = dev % 2
    own = lax.dynamic_index_in_dim(ids, odd, 0, keepdims=False)
    other = lax.dynamic_index_in_dim(ids, 1 - odd, 0, keepdims=False)
    blocks = range(n_sec * n_dev)
    straight = [(b, (b % 2) * n_dev + b // 2) for b in blocks]
    crossed = [(b, (1 - b % 2) * n_dev + b // 2) for b in blocks]
    same = lax.ppermute(own, ("section", "dev"), straight)
    cross = lax.ppermute(other, ("section", "dev"), crossed)
    low = jnp.where(section == 0, same, cross)
    high = jnp.where(section == 0, cross, same)
    x = jnp.transpose(jnp.stack([low, high]), (2, 3, 1, 0))
    x = jnp.broadcast_to(x[:, :, :, None, :], (POOL, CHUNK, half, 4, 2)).reshape(POOL, CHUNK, 128)
    live = jnp.repeat(lax.dynamic_slice(pool_len, (section * half,), (half,)), 8).reshape(1, 128)
    lists, bags = prep(x, live)
    bags = jnp.transpose(bags.reshape(half, 4, 2, CHUNK), (0, 2, 1, 3)).reshape(2 * half, 4 * CHUNK)
    arrived = lax.all_to_all(lists.reshape(n_dev, 2 * SLOTS), "dev", 0, 0, tiled=True)
    parts = gather(arrived.reshape(-1), tables, 2 * n_dev)
    parts = lax.all_to_all(parts.reshape(n_dev, 2 * CHUNK, E), "dev", 0, 0, tiled=True)
    features = unsort(parts.reshape(n_dev, 2, CHUNK, E), bags)
    both = swap(features, "section")
    samples = jnp.moveaxis(both, 0, 1).reshape(2 * CHUNK, n_tables * E)
    whole_weights = lax.all_gather(w_first, "dev", axis=0, tiled=True)
    pre_act = jnp.dot(samples, whole_weights, preferred_element_type=jnp.float32)
    hidden = jnp.maximum(pre_act + b_first.astype(jnp.float32)[None, :], 0.0)
    logit_part = jnp.sum(hidden * w_out.astype(jnp.float32)[None, :], axis=1)
    return lax.all_gather(logit_part, "section").sum(0)


def solution(mesh):
    placed = (
        P(("section", "dev"), None, None),
        P(),
        P(("section", "dev"), None),
        P("dev", "section"),
        P("section"),
        P("section"),
    )
    return jax.shard_map(body, mesh=mesh, in_specs=placed, out_specs=P("dev"), check_vma=False)
```

```python
import functools

import jax
import jax.numpy as jnp
from jax import lax
from jax.experimental import pallas as pl
from jax.experimental.pallas import tpu as pltpu
from jax.sharding import PartitionSpec as P

E = 128
ROWS_DEV = 32768
POOL = 8
CHUNK = 64
SLOTS = POOL * CHUNK
DEAD = ROWS_DEV | (8 << 16)
PIECES = 8
TBLK = 4096
HID_SPLIT = 2
SORT8 = (
    (0, 2), (1, 3), (4, 6), (5, 7), (0, 4), (1, 5), (2, 6), (3, 7), (0, 1), (2, 3),
    (4, 5), (6, 7), (2, 4), (3, 5), (1, 4), (3, 6), (1, 2), (3, 4), (5, 6),
)


def prep_body(x_ref, live_ref, list_ref, bag_ref):
    shape = (CHUNK, 128)
    lane = lax.broadcasted_iota(jnp.int32, shape, 1)
    bag = lax.broadcasted_iota(jnp.int32, shape, 0)
    first = ((lane >> 1) & 3) * ROWS_DEV
    live = jnp.broadcast_to(live_ref[...], shape)
    v = []
    for p in range(POOL):
        row = x_ref[p] - first
        ok = (row >= 0) & (row < ROWS_DEV) & (live > p)
        v.append(jnp.where(ok, row, ROWS_DEV))
    for a, b in SORT8:
        v[a], v[b] = jnp.minimum(v[a], v[b]), jnp.maximum(v[a], v[b])
    kept = sum((w < ROWS_DEV).astype(jnp.int32) for w in v)
    cols = [(POOL - kept) * CHUNK + bag]
    cols += [v[2 * k] | (v[2 * k + 1] << 16) for k in range(POOL // 2)]
    size = 2
    while size <= CHUNK:
        step = size // 2
        while step:
            upper = (bag & step) != 0
            small = ((bag & size) == 0) != upper
            other = [
                jnp.where(upper, pltpu.roll(c, step, 0), pltpu.roll(c, CHUNK - step, 0)) for c in cols
            ]
            take = jnp.where(small, other[0] - cols[0], cols[0] - other[0]) < 0
            cols = [jnp.where(take, o, c) for o, c in zip(other, cols)]
            step //= 2
        size *= 2
    key = cols[0]
    bag_ref[...] = (key & (CHUNK - 1)).T
    kept = POOL - (key >> 6)
    v = []
    for w in cols[1:]:
        v += [w & 0xFFFF, lax.shift_right_logical(w, 16)]
    tile = (8, 128)
    groups = []
    total = jnp.zeros((1, 128), jnp.int32)
    for g in range(CHUNK // 8):
        n = kept[8 * g : 8 * g + 1]
        shift = jnp.broadcast_to((8 * g - total) << 20, tile)
        n_all = jnp.broadcast_to(n, tile)
        for p in range(POOL):
            word = v[p][8 * g : 8 * g + 8] | (g << 16) | shift
            groups.append(jnp.where(n_all > p, word, DEAD))
        total = total + n
    for k in range(6):
        gap = 1 << k
        moves = [((w >> (20 + k)) & 1) != 0 for w in groups]
        new = []
        for i in range(64):
            stay = jnp.where(moves[i], DEAD, groups[i])
            if i + gap < 64:
                stay = jnp.where(moves[i + gap], groups[i + gap], stay)
            new.append(stay)
        groups = new
    head = lax.broadcasted_iota(jnp.int32, tile, 0) == 0
    mask = jnp.where(head, 0xFFFFF, 0xFFFF)
    groups = [w & mask for w in groups]
    groups[0] = groups[0] | jnp.where(head, jnp.broadcast_to(total << 20, tile), 0)
    for i in range(4):
        block = jnp.concatenate(groups[16 * i : 16 * i + 16], axis=0)
        list_ref[:, 128 * i : 128 * i + 128] = block.T


def prep(x, live):
    return pl.pallas_call(
        prep_body,
        out_shape=(
            jax.ShapeDtypeStruct((128, SLOTS), jnp.int32),
            jax.ShapeDtypeStruct((128, CHUNK), jnp.int32),
        ),
        name="bag_lists",
    )(x, live)


def gather_body(lists_ref, table_ref, out_ref, tab, tbuf, smem, acc, tsem, lsem, *, unroll):
    chunks = out_ref.shape[0]
    piece = chunks * SLOTS // PIECES

    def list_copy(i):
        part = pl.ds(i * piece, piece)
        return pltpu.make_async_copy(lists_ref.at[part], smem.at[part], lsem.at[i])

    def table_copy(b):
        return pltpu.make_async_copy(
            table_ref.at[pl.ds(b * TBLK, TBLK)], tbuf.at[b % 2], tsem.at[b % 2]
        )

    blocks = ROWS_DEV // TBLK
    table_copy(0).start()
    for i in range(PIECES):
        list_copy(i).start()
    tab[pl.ds(ROWS_DEV, 8), :] = jnp.zeros((8, E), jnp.float32)
    for b in range(blocks):
        if b + 1 < blocks:
            table_copy(b + 1).start()
        table_copy(b).wait()
        tab[pl.ds(b * TBLK, TBLK), :] = tbuf[b % 2].astype(jnp.float32)

    def level(base):
        head = smem[base]
        rows = [head & 0xFFFF] + [smem[base + i] for i in range(1, 8)]
        return (head >> 16) & 15, jnp.concatenate([tab[pl.ds(r, 1), :] for r in rows], axis=0)

    def chunk(c, carry):
        base = c * SLOTS
        acc[...] = jnp.zeros(acc.shape, jnp.float32)
        levels = smem[base] >> 20

        def step(k, carry):
            at = base + k * (8 * unroll)
            for g, rows in [level(at + 8 * u) for u in range(unroll)]:
                acc[pl.ds(pl.multiple_of(g * 8, 8), 8), :] += rows
            return carry

        lax.fori_loop(0, (levels + unroll - 1) // unroll, step, 0)
        out_ref[c] = acc[pl.ds(0, CHUNK), :].astype(jnp.bfloat16)
        return carry

    per = chunks // PIECES
    for i in range(PIECES):
        list_copy(i).wait()
        lax.fori_loop(i * per, (i + 1) * per, chunk, 0)


def gather(lists, table, chunks, unroll=4):
    return pl.pallas_call(
        functools.partial(gather_body, unroll=unroll),
        out_shape=jax.ShapeDtypeStruct((chunks, CHUNK, E), jnp.bfloat16),
        in_specs=[pl.BlockSpec(memory_space=pl.ANY), pl.BlockSpec(memory_space=pl.ANY)],
        out_specs=pl.BlockSpec(memory_space=pltpu.VMEM),
        scratch_shapes=[
            pltpu.VMEM((ROWS_DEV + 8, E), jnp.float32),
            pltpu.VMEM((2, TBLK, E), jnp.bfloat16),
            pltpu.SMEM((chunks * SLOTS,), jnp.int32),
            pltpu.VMEM((CHUNK + 8, E), jnp.float32),
            pltpu.SemaphoreType.DMA((2,)),
            pltpu.SemaphoreType.DMA((PIECES,)),
        ],
        compiler_params=pltpu.CompilerParams(vmem_limit_bytes=32 * 2**20),
        name="bag_gather",
    )(lists, table)


def unsort_body(part_ref, bag_ref, out_ref):
    tables = out_ref.shape[1] // E
    bag = lax.broadcasted_iota(jnp.int32, (CHUNK, 4 * CHUNK), 0)
    for t in range(tables):
        for h in range(2):
            where = bag_ref[2 * t + h : 2 * t + h + 1, :]
            pick = (bag == where).astype(jnp.float32).astype(jnp.bfloat16)
            rows = part_ref[4 * t : 4 * t + 4, h].reshape(4 * CHUNK, E)
            total = jnp.dot(pick, rows, preferred_element_type=jnp.float32)
            out_ref[h * CHUNK : (h + 1) * CHUNK, t * E : (t + 1) * E] = total.astype(jnp.bfloat16)


def unsort(parts, bags):
    return pl.pallas_call(
        unsort_body,
        out_shape=jax.ShapeDtypeStruct((2 * CHUNK, parts.shape[0] // 4 * E), jnp.bfloat16),
        name="bag_unsort",
    )(parts, bags)


def swap(x, axis):
    return lax.all_to_all(jnp.broadcast_to(x[None], (2, *x.shape)), axis, 0, 0, tiled=True)


def body(indices, pool_len, tables, w_first, b_first, w_out):
    n_dev = lax.axis_size("dev")
    n_sec = lax.axis_size("section")
    n_tables = indices.shape[1]
    half = n_tables // n_sec
    section = lax.axis_index("section")
    dev = lax.axis_index("dev")
    ids = jnp.transpose(indices, (1, 2, 0)).reshape(n_sec, half, POOL, CHUNK)
    odd = dev % 2
    own = lax.dynamic_index_in_dim(ids, odd, 0, keepdims=False)
    other = lax.dynamic_index_in_dim(ids, 1 - odd, 0, keepdims=False)
    blocks = range(n_sec * n_dev)
    straight = [(b, (b % 2) * n_dev + b // 2) for b in blocks]
    crossed = [(b, (1 - b % 2) * n_dev + b // 2) for b in blocks]
    same = lax.ppermute(own, ("section", "dev"), straight)
    cross = lax.ppermute(other, ("section", "dev"), crossed)
    low = jnp.where(section == 0, same, cross)
    high = jnp.where(section == 0, cross, same)
    x = jnp.transpose(jnp.stack([low, high]), (2, 3, 1, 0))
    x = jnp.broadcast_to(x[:, :, :, None, :], (POOL, CHUNK, half, 4, 2)).reshape(POOL, CHUNK, 128)
    live = jnp.repeat(lax.dynamic_slice(pool_len, (section * half,), (half,)), 8).reshape(1, 128)
    lists, bags = prep(x, live)
    bags = jnp.transpose(bags.reshape(half, 4, 2, CHUNK), (0, 2, 1, 3)).reshape(2 * half, 4 * CHUNK)
    arrived = lax.all_to_all(lists.reshape(n_dev, 2 * SLOTS), "dev", 0, 0, tiled=True)
    parts = gather(arrived.reshape(-1), tables, 2 * n_dev)
    parts = lax.all_to_all(parts.reshape(n_dev, 2 * CHUNK, E), "dev", 0, 0, tiled=True)
    features = unsort(parts.reshape(n_dev, 2, CHUNK, E), bags)
    ring = 4
    rows, cols = w_first.shape
    part = cols // HID_SPLIT
    planes = n_dev // ring
    rings = [[ring * p + y for y in range(ring)] for p in range(planes)]
    levels = [[ring * p + y for p in range(planes)] for y in range(ring)]
    pieces = jnp.moveaxis(w_first.reshape(rows, HID_SPLIT, part), 1, 0)
    pieces = jnp.concatenate([pieces] * (ring // HID_SPLIT))
    mine = lax.all_to_all(pieces, "dev", 0, 0, axis_index_groups=rings, tiled=True)
    whole = lax.all_gather(mine.reshape(ring * rows, part), "dev", axis_index_groups=levels, tiled=True)
    q = dev % HID_SPLIT
    bias = lax.dynamic_slice(b_first, (q * part,), (part,)).astype(jnp.float32)
    scale = lax.dynamic_slice(w_out, (q * part,), (part,)).astype(jnp.float32)
    pairs = [(d, d ^ 1) for d in range(n_dev)]
    shared = jnp.stack([features, lax.ppermute(features, "dev", pairs)])
    both = swap(shared, "section")
    samples = jnp.moveaxis(both, 0, 2).reshape(HID_SPLIT * 2 * CHUNK, n_tables * E)
    pre_act = jnp.dot(samples, whole, preferred_element_type=jnp.float32)
    hidden = jnp.maximum(pre_act + bias[None, :], 0.0)
    logit_part = jnp.sum(hidden * scale[None, :], axis=1).reshape(HID_SPLIT, 2 * CHUNK)
    total = logit_part[0] + lax.ppermute(logit_part[1], "dev", pairs)
    return lax.all_gather(total, "section").sum(0)


def solution(mesh):
    placed = (
        P(("section", "dev"), None, None),
        P(),
        P(("section", "dev"), None),
        P("dev", "section"),
        P("section"),
        P("section"),
    )
    return jax.shard_map(body, mesh=mesh, in_specs=placed, out_specs=P("dev"), check_vma=False)
```

```python
import functools

import jax
import jax.numpy as jnp
from jax import lax
from jax.experimental import pallas as pl
from jax.experimental.pallas import tpu as pltpu
from jax.sharding import PartitionSpec as P

E = 128
ROWS_DEV = 32768
POOL = 8
CHUNK = 64
SLOTS = POOL * CHUNK
DEAD = ROWS_DEV | (8 << 16)
PIECES = 8
TBLK = 2048
TSLOTS = 4
HID_SPLIT = 2
SORT8 = (
    (0, 2), (1, 3), (4, 6), (5, 7), (0, 4), (1, 5), (2, 6), (3, 7), (0, 1), (2, 3),
    (4, 5), (6, 7), (2, 4), (3, 5), (1, 4), (3, 6), (1, 2), (3, 4), (5, 6),
)


def prep_body(x_ref, pool_ref, list_ref, bag_ref):
    shape = (CHUNK, 128)
    tables = x_ref.shape[0]
    lane = lax.broadcasted_iota(jnp.int32, shape, 1)
    bag = lax.broadcasted_iota(jnp.int32, shape, 0)
    table = lax.broadcasted_iota(jnp.int32, (8, 128), 1) & (tables - 1)
    live = jnp.zeros((8, 128), jnp.int32)
    for t in range(tables):
        live = jnp.where(table == t, pool_ref[t], live)
    live = jnp.concatenate([live] * (CHUNK // 8), axis=0)
    first = (lane // tables) * ROWS_DEV
    v = []
    for p in range(POOL):
        row = jnp.concatenate([x_ref[:, p, :]] * 4, axis=0).T - first
        ok = (row >= 0) & (row < ROWS_DEV) & (live > p)
        v.append(jnp.where(ok, row, ROWS_DEV))
    for a, b in SORT8:
        v[a], v[b] = jnp.minimum(v[a], v[b]), jnp.maximum(v[a], v[b])
    kept = sum((w < ROWS_DEV).astype(jnp.int32) for w in v)
    cols = [(POOL - kept) * CHUNK + bag]
    cols += [v[2 * k] | (v[2 * k + 1] << 16) for k in range(POOL // 2)]
    size = 2
    while size <= CHUNK:
        step = size // 2
        while step:
            upper = (bag & step) != 0
            small = ((bag & size) == 0) != upper
            other = [
                jnp.where(upper, pltpu.roll(c, step, 0), pltpu.roll(c, CHUNK - step, 0)) for c in cols
            ]
            take = jnp.where(small, other[0] - cols[0], cols[0] - other[0]) < 0
            cols = [jnp.where(take, o, c) for o, c in zip(other, cols)]
            step //= 2
        size *= 2
    key = cols[0]
    order = (key & (CHUNK - 1)).T
    for j in range(4):
        bag_ref[:, j * CHUNK : (j + 1) * CHUNK] = order[j * tables : (j + 1) * tables, :]
    kept = POOL - (key >> 6)
    v = []
    for w in cols[1:]:
        v += [w & 0xFFFF, lax.shift_right_logical(w, 16)]
    tile = (8, 128)
    groups = []
    total = jnp.zeros((1, 128), jnp.int32)
    for g in range(CHUNK // 8):
        n = kept[8 * g : 8 * g + 1]
        shift = jnp.broadcast_to((8 * g - total) << 20, tile)
        n_all = jnp.broadcast_to(n, tile)
        for p in range(POOL):
            word = v[p][8 * g : 8 * g + 8] | (g << 16) | shift
            groups.append(jnp.where(n_all > p, word, DEAD))
        total = total + n
    for k in range(6):
        gap = 1 << k
        moves = [((w >> (20 + k)) & 1) != 0 for w in groups]
        new = []
        for i in range(64):
            stay = jnp.where(moves[i], DEAD, groups[i])
            if i + gap < 64:
                stay = jnp.where(moves[i + gap], groups[i + gap], stay)
            new.append(stay)
        groups = new
    head = lax.broadcasted_iota(jnp.int32, tile, 0) == 0
    mask = jnp.where(head, 0xFFFFF, 0xFFFF)
    groups = [w & mask for w in groups]
    groups[0] = groups[0] | jnp.where(head, jnp.broadcast_to(total << 20, tile), 0)
    for i in range(4):
        block = jnp.concatenate(groups[16 * i : 16 * i + 16], axis=0)
        block = block.T
        for j in range(4):
            list_ref[pl.ds(4 * j + i, tables, stride=16), :] = block[j * tables : (j + 1) * tables, :]


def prep(ids, pool_len):
    tables = ids.shape[0]
    return pl.pallas_call(
        prep_body,
        out_shape=(
            pltpu.VMEM((128 * 4, 128), jnp.int32),
            pltpu.VMEM((tables, 4 * CHUNK), jnp.int32),
        ),
        out_specs=(pl.BlockSpec(memory_space=pltpu.VMEM), pl.BlockSpec(memory_space=pltpu.VMEM)),
        in_specs=[pl.BlockSpec(memory_space=pltpu.VMEM), pl.BlockSpec(memory_space=pltpu.SMEM)],
        name="bag_lists",
    )(ids, pool_len)


def gather_body(lists_ref, table_ref, out_ref, tab, tbuf, smem, acc, obuf, tsem, lsem, osem, *, unroll):
    chunks = out_ref.shape[0]
    per = chunks // PIECES
    piece = chunks * SLOTS // PIECES

    def list_copy(i):
        part = pl.ds(i * piece, piece)
        return pltpu.make_async_copy(lists_ref.at[part], smem.at[part], lsem.at[i])

    def table_copy(b):
        slot = b % TSLOTS
        return pltpu.make_async_copy(
            table_ref.at[pl.ds(b * TBLK, TBLK)], tbuf.at[slot], tsem.at[slot]
        )

    def out_copy(i):
        return pltpu.make_async_copy(obuf.at[i % 2], out_ref.at[pl.ds(i * per, per)], osem.at[i % 2])

    blocks = ROWS_DEV // TBLK
    for b in range(TSLOTS):
        table_copy(b).start()
    for i in range(PIECES):
        list_copy(i).start()
    tab[pl.ds(ROWS_DEV, 8), :] = jnp.zeros((8, E), jnp.float32)
    for b in range(blocks):
        table_copy(b).wait()
        tab[pl.ds(b * TBLK, TBLK), :] = tbuf[b % TSLOTS].astype(jnp.float32)
        if b + TSLOTS < blocks:
            table_copy(b + TSLOTS).start()

    def level(base):
        head = smem[base]
        rows = [head & 0xFFFF] + [smem[base + i] for i in range(1, 8)]
        return (head >> 16) & 15, jnp.concatenate([tab[pl.ds(r, 1), :] for r in rows], axis=0)

    def chunk(c, piece):
        base = (piece * per + c) * SLOTS
        acc[...] = jnp.zeros(acc.shape, jnp.float32)
        levels = smem[base] >> 20

        def step(k, carry):
            at = base + k * (8 * unroll)
            for g, rows in [level(at + 8 * u) for u in range(unroll)]:
                acc[pl.ds(pl.multiple_of(g * 8, 8), 8), :] += rows
            return carry

        lax.fori_loop(0, (levels + unroll - 1) // unroll, step, 0)
        obuf[piece % 2, c] = acc[pl.ds(0, CHUNK), :].astype(jnp.bfloat16)

    for i in range(PIECES):
        list_copy(i).wait()
        if i >= 2:
            out_copy(i - 2).wait()
        lax.fori_loop(0, per, lambda c, carry: (chunk(c, i), carry)[1], 0)
        out_copy(i).start()
    out_copy(PIECES - 2).wait()
    out_copy(PIECES - 1).wait()


def gather(lists, table, chunks, unroll=4):
    return pl.pallas_call(
        functools.partial(gather_body, unroll=unroll),
        out_shape=pltpu.HBM((chunks, CHUNK, E), jnp.bfloat16),
        in_specs=[pl.BlockSpec(memory_space=pl.ANY), pl.BlockSpec(memory_space=pltpu.HBM)],
        out_specs=pl.BlockSpec(memory_space=pltpu.HBM),
        scratch_shapes=[
            pltpu.VMEM((ROWS_DEV + 8, E), jnp.float32),
            pltpu.VMEM((TSLOTS, TBLK, E), jnp.bfloat16),
            pltpu.SMEM((chunks * SLOTS,), jnp.int32),
            pltpu.VMEM((CHUNK + 8, E), jnp.float32),
            pltpu.VMEM((2, chunks // PIECES, CHUNK, E), jnp.bfloat16),
            pltpu.SemaphoreType.DMA((TSLOTS,)),
            pltpu.SemaphoreType.DMA((PIECES,)),
            pltpu.SemaphoreType.DMA((2,)),
        ],
        compiler_params=pltpu.CompilerParams(vmem_limit_bytes=32 * 2**20),
        name="bag_gather",
    )(lists, pltpu.with_memory_space_constraint(table, pltpu.HBM))


def unsort_body(part_ref, low_ref, high_ref, out_ref):
    tables = out_ref.shape[1] // E
    bag = lax.broadcasted_iota(jnp.int32, (CHUNK, 4 * CHUNK), 0)
    for t in range(tables):
        for h in range(2):
            where = (low_ref, high_ref)[h][t : t + 1, :]
            pick = (bag == where).astype(jnp.float32).astype(jnp.bfloat16)
            rows = part_ref[4 * t : 4 * t + 4, h].reshape(4 * CHUNK, E)
            total = jnp.dot(pick, rows, preferred_element_type=jnp.float32)
            out_ref[h * CHUNK : (h + 1) * CHUNK, t * E : (t + 1) * E] = total.astype(jnp.bfloat16)


def unsort(parts, low, high):
    return pl.pallas_call(
        unsort_body,
        out_shape=pltpu.VMEM((2 * CHUNK, parts.shape[0] // 4 * E), jnp.bfloat16),
        in_specs=[pl.BlockSpec(memory_space=pltpu.VMEM)] * 3,
        out_specs=pl.BlockSpec(memory_space=pltpu.VMEM),
        name="bag_unsort",
    )(pltpu.with_memory_space_constraint(parts, pltpu.VMEM), low, high)


def swap(x, axis):
    return lax.all_to_all(jnp.broadcast_to(x[None], (2, *x.shape)), axis, 0, 0, tiled=True)


def body(indices, pool_len, tables, w_first, b_first, w_out):
    n_dev = lax.axis_size("dev")
    n_sec = lax.axis_size("section")
    n_tables = indices.shape[1]
    half = n_tables // n_sec
    section = lax.axis_index("section")
    dev = lax.axis_index("dev")
    lists, order = prep(jnp.transpose(indices, (1, 2, 0)), pool_len)
    ring = 4
    rows, cols = w_first.shape
    part = cols // HID_SPLIT
    planes = n_dev // ring
    levels = [[ring * p + y for p in range(planes)] for y in range(ring)]
    y = dev % ring
    q = dev % HID_SPLIT
    keep = lax.dynamic_slice(w_first, (0, q * part), (rows, part))
    give = lax.dynamic_slice(w_first, (0, (1 - q) * part), (rows, part))

    def along(x, k):
        return lax.ppermute(x, "dev", [(d, d // ring * ring + (d + k) % ring) for d in range(n_dev)])

    pieces = [keep, along(give, 1), along(keep, 2), along(give, 3)]
    pieces, lists = lax.optimization_barrier((pieces, lists))
    pieces = jnp.stack(pieces)
    pieces = [lax.dynamic_index_in_dim(pieces, (y - k) % ring, 0, False) for k in range(ring)]
    whole = lax.all_gather(jnp.concatenate(pieces), "dev", axis_index_groups=levels, tiled=True)
    both_axes = ("section", "dev")
    blocks = range(n_sec * n_dev)
    arrived = lax.all_to_all(lists.reshape(n_sec * n_dev, 4, 128), both_axes, 0, 0, tiled=True)
    order = order.reshape(n_sec, half, 4 * CHUNK)
    odd = dev % 2
    straight = [(b, (b % 2) * n_dev + b // 2) for b in blocks]
    crossed = [(b, (1 - b % 2) * n_dev + b // 2) for b in blocks]
    same = lax.ppermute(lax.dynamic_index_in_dim(order, odd, 0, False), both_axes, straight)
    cross = lax.ppermute(lax.dynamic_index_in_dim(order, 1 - odd, 0, False), both_axes, crossed)
    low = jnp.where(section == 0, same, cross)
    high = jnp.where(section == 0, cross, same)
    parts = gather(arrived.reshape(-1), tables, n_sec * n_dev)
    parts = lax.all_to_all(parts.reshape(n_dev, 2 * CHUNK, E), "dev", 0, 0, tiled=True)
    features = unsort(parts.reshape(n_dev, 2, CHUNK, E), low, high)
    bias = lax.dynamic_slice(b_first, (q * part,), (part,)).astype(jnp.float32)
    scale = lax.dynamic_slice(w_out, (q * part,), (part,)).astype(jnp.float32)
    far = lax.ppermute(features, "dev", [(d, d ^ 1) for d in range(n_dev)])
    k_half = half * E

    def logits_of(mine):
        both = swap(mine, "section")
        pre_act = jnp.dot(both[0], whole[:k_half], preferred_element_type=jnp.float32)
        pre_act += jnp.dot(both[1], whole[k_half:], preferred_element_type=jnp.float32)
        hidden = jnp.maximum(pre_act + bias[None, :], 0.0)
        return jnp.sum(hidden * scale[None, :], axis=1)

    near_part = logits_of(features)
    far, near_part = lax.optimization_barrier((far, near_part))
    far_part = logits_of(far)
    by_chip = jnp.stack([jnp.where(q == 0, near_part, far_part), jnp.where(q == 0, far_part, near_part)])
    quads = [[s * n_dev + 2 * p + i for s in range(n_sec) for i in range(2)] for p in range(n_dev // 2)]
    quarters = lax.all_gather(by_chip, both_axes, axis_index_groups=quads)
    return lax.dynamic_index_in_dim(quarters.sum(0), q, 0, False)


def solution(mesh):
    placed = (
        P(("section", "dev"), None, None),
        P(),
        P(("section", "dev"), None),
        P("dev", "section"),
        P("section"),
        P("section"),
    )
    return jax.shard_map(body, mesh=mesh, in_specs=placed, out_specs=P("dev"), check_vma=False)
```

```python
import functools

import jax
import jax.numpy as jnp
from jax import lax
from jax.experimental import pallas as pl
from jax.experimental.pallas import tpu as pltpu
from jax.sharding import PartitionSpec as P

E = 128
ROWS_DEV = 32768
POOL = 8
CHUNK = 64
SLOTS = POOL * CHUNK
DEAD = ROWS_DEV | (8 << 16)
PIECES = 8
TBLK = 2048
TSLOTS = 4
HID_SPLIT = 4
SORT8 = (
    (0, 2), (1, 3), (4, 6), (5, 7), (0, 4), (1, 5), (2, 6), (3, 7), (0, 1), (2, 3),
    (4, 5), (6, 7), (2, 4), (3, 5), (1, 4), (3, 6), (1, 2), (3, 4), (5, 6),
)


def prep_body(x_ref, pool_ref, list_ref, bag_ref):
    shape = (CHUNK, 128)
    tables = x_ref.shape[0]
    lane = lax.broadcasted_iota(jnp.int32, shape, 1)
    bag = lax.broadcasted_iota(jnp.int32, shape, 0)
    table = lax.broadcasted_iota(jnp.int32, (8, 128), 1) & (tables - 1)
    live = jnp.zeros((8, 128), jnp.int32)
    for t in range(tables):
        live = jnp.where(table == t, pool_ref[t], live)
    live = jnp.concatenate([live] * (CHUNK // 8), axis=0)
    first = (lane // tables) * ROWS_DEV
    v = []
    for p in range(POOL):
        row = jnp.concatenate([x_ref[:, p, :]] * 4, axis=0).T - first
        ok = (row >= 0) & (row < ROWS_DEV) & (live > p)
        v.append(jnp.where(ok, row, ROWS_DEV))
    for a, b in SORT8:
        v[a], v[b] = jnp.minimum(v[a], v[b]), jnp.maximum(v[a], v[b])
    kept = sum((w < ROWS_DEV).astype(jnp.int32) for w in v)
    cols = [(POOL - kept) * CHUNK + bag]
    cols += [v[2 * k] | (v[2 * k + 1] << 16) for k in range(POOL // 2)]
    size = 2
    while size <= CHUNK:
        step = size // 2
        while step:
            upper = (bag & step) != 0
            small = ((bag & size) == 0) != upper
            other = [
                jnp.where(upper, pltpu.roll(c, step, 0), pltpu.roll(c, CHUNK - step, 0)) for c in cols
            ]
            take = jnp.where(small, other[0] - cols[0], cols[0] - other[0]) < 0
            cols = [jnp.where(take, o, c) for o, c in zip(other, cols)]
            step //= 2
        size *= 2
    key = cols[0]
    order = (key & (CHUNK - 1)).T
    for j in range(4):
        bag_ref[:, j * CHUNK : (j + 1) * CHUNK] = order[j * tables : (j + 1) * tables, :]
    kept = POOL - (key >> 6)
    v = []
    for w in cols[1:]:
        v += [w & 0xFFFF, lax.shift_right_logical(w, 16)]
    tile = (8, 128)
    groups = []
    total = jnp.zeros((1, 128), jnp.int32)
    for g in range(CHUNK // 8):
        n = kept[8 * g : 8 * g + 1]
        shift = jnp.broadcast_to((8 * g - total) << 20, tile)
        n_all = jnp.broadcast_to(n, tile)
        for p in range(POOL):
            word = v[p][8 * g : 8 * g + 8] | (g << 16) | shift
            groups.append(jnp.where(n_all > p, word, DEAD))
        total = total + n
    for k in range(6):
        gap = 1 << k
        moves = [((w >> (20 + k)) & 1) != 0 for w in groups]
        new = []
        for i in range(64):
            stay = jnp.where(moves[i], DEAD, groups[i])
            if i + gap < 64:
                stay = jnp.where(moves[i + gap], groups[i + gap], stay)
            new.append(stay)
        groups = new
    head = lax.broadcasted_iota(jnp.int32, tile, 0) == 0
    mask = jnp.where(head, 0xFFFFF, 0xFFFF)
    groups = [w & mask for w in groups]
    groups[0] = groups[0] | jnp.where(head, jnp.broadcast_to(total << 20, tile), 0)
    for i in range(4):
        block = jnp.concatenate(groups[16 * i : 16 * i + 16], axis=0)
        block = block.T
        for j in range(4):
            list_ref[pl.ds(4 * j + i, tables, stride=16), :] = block[j * tables : (j + 1) * tables, :]


def prep(ids, pool_len):
    tables = ids.shape[0]
    return pl.pallas_call(
        prep_body,
        out_shape=(
            pltpu.VMEM((128 * 4, 128), jnp.int32),
            pltpu.VMEM((tables, 4 * CHUNK), jnp.int32),
        ),
        out_specs=(pl.BlockSpec(memory_space=pltpu.VMEM), pl.BlockSpec(memory_space=pltpu.VMEM)),
        in_specs=[pl.BlockSpec(memory_space=pltpu.VMEM), pl.BlockSpec(memory_space=pltpu.SMEM)],
        name="bag_lists",
    )(ids, pool_len)


def gather_body(lists_ref, table_ref, out_ref, tab, tbuf, smem, acc, obuf, tsem, lsem, osem, *, unroll):
    chunks = out_ref.shape[0]
    per = chunks // PIECES
    piece = chunks * SLOTS // PIECES

    def list_copy(i):
        part = pl.ds(i * piece, piece)
        return pltpu.make_async_copy(lists_ref.at[part], smem.at[part], lsem.at[i])

    def table_copy(b):
        slot = b % TSLOTS
        return pltpu.make_async_copy(
            table_ref.at[pl.ds(b * TBLK, TBLK)], tbuf.at[slot], tsem.at[slot]
        )

    def out_copy(i):
        return pltpu.make_async_copy(obuf.at[i % 2], out_ref.at[pl.ds(i * per, per)], osem.at[i % 2])

    blocks = ROWS_DEV // TBLK
    for b in range(TSLOTS):
        table_copy(b).start()
    for i in range(PIECES):
        list_copy(i).start()
    tab[pl.ds(ROWS_DEV, 8), :] = jnp.zeros((8, E), jnp.float32)
    for b in range(blocks):
        table_copy(b).wait()
        tab[pl.ds(b * TBLK, TBLK), :] = tbuf[b % TSLOTS].astype(jnp.float32)
        if b + TSLOTS < blocks:
            table_copy(b + TSLOTS).start()

    def level(base):
        head = smem[base]
        rows = [head & 0xFFFF] + [smem[base + i] for i in range(1, 8)]
        return (head >> 16) & 15, jnp.concatenate([tab[pl.ds(r, 1), :] for r in rows], axis=0)

    def chunk(c, piece):
        base = (piece * per + c) * SLOTS
        acc[...] = jnp.zeros(acc.shape, jnp.float32)
        levels = smem[base] >> 20

        def step(k, carry):
            at = base + k * (8 * unroll)
            for g, rows in [level(at + 8 * u) for u in range(unroll)]:
                acc[pl.ds(pl.multiple_of(g * 8, 8), 8), :] += rows
            return carry

        lax.fori_loop(0, (levels + unroll - 1) // unroll, step, 0)
        obuf[piece % 2, c] = acc[pl.ds(0, CHUNK), :].astype(jnp.bfloat16)

    for i in range(PIECES):
        list_copy(i).wait()
        if i >= 2:
            out_copy(i - 2).wait()
        lax.fori_loop(0, per, lambda c, carry: (chunk(c, i), carry)[1], 0)
        out_copy(i).start()
    out_copy(PIECES - 2).wait()
    out_copy(PIECES - 1).wait()


def gather(lists, table, chunks, unroll=4):
    return pl.pallas_call(
        functools.partial(gather_body, unroll=unroll),
        out_shape=pltpu.HBM((chunks, CHUNK, E), jnp.bfloat16),
        in_specs=[pl.BlockSpec(memory_space=pl.ANY), pl.BlockSpec(memory_space=pltpu.HBM)],
        out_specs=pl.BlockSpec(memory_space=pltpu.HBM),
        scratch_shapes=[
            pltpu.VMEM((ROWS_DEV + 8, E), jnp.float32),
            pltpu.VMEM((TSLOTS, TBLK, E), jnp.bfloat16),
            pltpu.SMEM((chunks * SLOTS,), jnp.int32),
            pltpu.VMEM((CHUNK + 8, E), jnp.float32),
            pltpu.VMEM((2, chunks // PIECES, CHUNK, E), jnp.bfloat16),
            pltpu.SemaphoreType.DMA((TSLOTS,)),
            pltpu.SemaphoreType.DMA((PIECES,)),
            pltpu.SemaphoreType.DMA((2,)),
        ],
        compiler_params=pltpu.CompilerParams(vmem_limit_bytes=32 * 2**20),
        name="bag_gather",
    )(lists, pltpu.with_memory_space_constraint(table, pltpu.HBM))


def unsort_body(part_ref, low_ref, high_ref, out_ref):
    tables = out_ref.shape[1] // E
    bag = lax.broadcasted_iota(jnp.int32, (CHUNK, 4 * CHUNK), 0)
    for t in range(tables):
        for h in range(2):
            where = (low_ref, high_ref)[h][t : t + 1, :]
            pick = (bag == where).astype(jnp.float32).astype(jnp.bfloat16)
            rows = part_ref[4 * t : 4 * t + 4, h].reshape(4 * CHUNK, E)
            total = jnp.dot(pick, rows, preferred_element_type=jnp.float32)
            out_ref[h * CHUNK : (h + 1) * CHUNK, t * E : (t + 1) * E] = total.astype(jnp.bfloat16)


def unsort(parts, low, high):
    return pl.pallas_call(
        unsort_body,
        out_shape=pltpu.VMEM((2 * CHUNK, parts.shape[0] // 4 * E), jnp.bfloat16),
        in_specs=[pl.BlockSpec(memory_space=pltpu.VMEM)] * 3,
        out_specs=pl.BlockSpec(memory_space=pltpu.VMEM),
        name="bag_unsort",
    )(pltpu.with_memory_space_constraint(parts, pltpu.VMEM), low, high)


def swap(x, axis):
    return lax.all_to_all(jnp.broadcast_to(x[None], (2, *x.shape)), axis, 0, 0, tiled=True)


def body(indices, pool_len, tables, w_first, b_first, w_out):
    n_dev = lax.axis_size("dev")
    n_sec = lax.axis_size("section")
    n_tables = indices.shape[1]
    half = n_tables // n_sec
    section = lax.axis_index("section")
    dev = lax.axis_index("dev")
    lists, order = prep(jnp.transpose(indices, (1, 2, 0)), pool_len)
    lists, order, w_first = lax.optimization_barrier((lists, order, w_first))
    both_axes = ("section", "dev")
    blocks = range(n_sec * n_dev)
    arrived = lax.all_to_all(lists.reshape(n_sec * n_dev, 4, 128), both_axes, 0, 0, tiled=True)
    order = order.reshape(n_sec, half, 4 * CHUNK)
    odd = dev % 2
    straight = [(b, (b % 2) * n_dev + b // 2) for b in blocks]
    crossed = [(b, (1 - b % 2) * n_dev + b // 2) for b in blocks]
    same = lax.ppermute(lax.dynamic_index_in_dim(order, odd, 0, False), both_axes, straight)
    cross = lax.ppermute(lax.dynamic_index_in_dim(order, 1 - odd, 0, False), both_axes, crossed)
    low = jnp.where(section == 0, same, cross)
    high = jnp.where(section == 0, cross, same)
    ring = HID_SPLIT
    rows, cols = w_first.shape
    part = cols // ring
    planes = n_dev // ring
    levels = [[ring * p + y for p in range(planes)] for y in range(ring)]
    y = dev % ring

    def along(x, k):
        return lax.ppermute(x, "dev", [(d, d // ring * ring + (d + k) % ring) for d in range(n_dev)])

    def slab(k):
        return lax.dynamic_slice(w_first, (0, (y + k) % ring * part), (rows, part))

    pieces = jnp.stack([slab(0)] + [along(slab(k), k) for k in range(1, ring)])
    pieces = [lax.dynamic_index_in_dim(pieces, (y - k) % ring, 0, False) for k in range(ring)]
    mine = jnp.concatenate(pieces)
    arrived, low, high = lax.optimization_barrier((arrived, low, high))
    whole = lax.all_gather(mine, "dev", axis_index_groups=levels, tiled=True)
    bias = lax.dynamic_slice(b_first, (y * part,), (part,)).astype(jnp.float32)
    scale = lax.dynamic_slice(w_out, (y * part,), (part,)).astype(jnp.float32)
    parts = gather(arrived.reshape(-1), tables, n_sec * n_dev)
    parts = lax.all_to_all(parts.reshape(n_dev, 2 * CHUNK, E), "dev", 0, 0, tiled=True)
    features = unsort(parts.reshape(n_dev, 2, CHUNK, E), low, high)
    k_half = half * E

    def logits_of(mine):
        both = swap(mine, "section")
        pre_act = jnp.dot(both[0], whole[:k_half], preferred_element_type=jnp.float32)
        pre_act += jnp.dot(both[1], whole[k_half:], preferred_element_type=jnp.float32)
        hidden = jnp.maximum(pre_act + bias[None, :], 0.0)
        return jnp.sum(hidden * scale[None, :], axis=1)

    after, before, far = along(features, 1), along(features, 3), along(features, 2)
    part_0 = logits_of(features)
    after, before, part_0 = lax.optimization_barrier((after, before, part_0))
    part_13 = logits_of(jnp.concatenate([after, before]))
    far, part_13 = lax.optimization_barrier((far, part_13))
    part_2 = logits_of(far)
    shifts = jnp.stack([part_0, part_13[: 2 * CHUNK], part_2, part_13[2 * CHUNK :]])
    by_chip = jnp.stack([lax.dynamic_index_in_dim(shifts, (y - k) % ring, 0, False) for k in range(ring)])
    rings = [[s * n_dev + ring * p + i for s in range(n_sec) for i in range(ring)] for p in range(planes)]
    eighths = lax.all_gather(by_chip, both_axes, axis_index_groups=rings)
    return lax.dynamic_index_in_dim(eighths.sum(0), y, 0, False)


def solution(mesh):
    placed = (
        P(("section", "dev"), None, None),
        P(),
        P(("section", "dev"), None),
        P("dev", "section"),
        P("section"),
        P("section"),
    )
    return jax.shard_map(body, mesh=mesh, in_specs=placed, out_specs=P("dev"), check_vma=False)
```

```python
import functools

import jax
import jax.numpy as jnp
from jax import lax
from jax.experimental import pallas as pl
from jax.experimental.pallas import tpu as pltpu
from jax.sharding import PartitionSpec as P

E = 128
ROWS_DEV = 32768
POOL = 8
CHUNK = 64
SLOTS = POOL * CHUNK
DEAD = ROWS_DEV | (8 << 16)
TBLK = 2048
TSLOTS = 4
HID_SPLIT = 2
SORT8 = (
    (0, 2), (1, 3), (4, 6), (5, 7), (0, 4), (1, 5), (2, 6), (3, 7), (0, 1), (2, 3),
    (4, 5), (6, 7), (2, 4), (3, 5), (1, 4), (3, 6), (1, 2), (3, 4), (5, 6),
)


def prep_body(x_ref, pool_ref, list_ref, order_ref):
    shape = (CHUNK, 128)
    tables = x_ref.shape[0]
    lane = lax.broadcasted_iota(jnp.int32, shape, 1)
    bag = lax.broadcasted_iota(jnp.int32, shape, 0)
    table = lax.broadcasted_iota(jnp.int32, (8, 128), 1) & (tables - 1)
    live = jnp.zeros((8, 128), jnp.int32)
    for t in range(tables):
        live = jnp.where(table == t, pool_ref[t], live)
    live = jnp.concatenate([live] * (CHUNK // 8), axis=0)
    first = (lane // tables) * ROWS_DEV
    v = []
    for p in range(POOL):
        row = jnp.concatenate([x_ref[:, p, :]] * 4, axis=0).T - first
        ok = (row >= 0) & (row < ROWS_DEV) & (live > p)
        v.append(jnp.where(ok, row, ROWS_DEV))
    for a, b in SORT8:
        v[a], v[b] = jnp.minimum(v[a], v[b]), jnp.maximum(v[a], v[b])
    kept = sum((w < ROWS_DEV).astype(jnp.int32) for w in v)
    cols = [(POOL - kept) * CHUNK + bag]
    cols += [v[2 * k] | (v[2 * k + 1] << 16) for k in range(POOL // 2)]
    size = 2
    while size <= CHUNK:
        step = size // 2
        while step:
            upper = (bag & step) != 0
            small = ((bag & size) == 0) != upper
            other = [
                jnp.where(upper, pltpu.roll(c, step, 0), pltpu.roll(c, CHUNK - step, 0)) for c in cols
            ]
            take = jnp.where(small, other[0] - cols[0], cols[0] - other[0]) < 0
            cols = [jnp.where(take, o, c) for o, c in zip(other, cols)]
            step //= 2
        size *= 2
    key = cols[0]
    order = (((key & (CHUNK - 1)) | CHUNK) << 20).T
    for j in range(4):
        order_ref[:, j * CHUNK : (j + 1) * CHUNK] = order[j * tables : (j + 1) * tables, :]
    kept = POOL - (key >> 6)
    v = []
    for w in cols[1:]:
        v += [w & 0xFFFF, lax.shift_right_logical(w, 16)]
    tile = (8, 128)
    groups = []
    total = jnp.zeros((1, 128), jnp.int32)
    for g in range(CHUNK // 8):
        n = kept[8 * g : 8 * g + 1]
        shift = jnp.broadcast_to((8 * g - total) << 20, tile)
        n_all = jnp.broadcast_to(n, tile)
        for p in range(POOL):
            word = v[p][8 * g : 8 * g + 8] | (g << 16) | shift
            groups.append(jnp.where(n_all > p, word, DEAD))
        total = total + n
    for k in range(6):
        gap = 1 << k
        moves = [((w >> (20 + k)) & 1) != 0 for w in groups]
        new = []
        for i in range(64):
            stay = jnp.where(moves[i], DEAD, groups[i])
            if i + gap < 64:
                stay = jnp.where(moves[i + gap], groups[i + gap], stay)
            new.append(stay)
        groups = new
    head = lax.broadcasted_iota(jnp.int32, tile, 0) == 0
    mask = jnp.where(head, 0xFFFFF, 0xFFFF)
    groups = [w & mask for w in groups]
    groups[0] = groups[0] | jnp.where(head, jnp.broadcast_to(total << 20, tile), 0)
    for i in range(4):
        block = jnp.concatenate(groups[16 * i : 16 * i + 16], axis=0)
        block = block.T
        for j in range(4):
            rows = block[j * tables : (j + 1) * tables, :]
            if i >= 2:
                rows = rows | order_ref[:, (i - 2) * 128 : (i - 1) * 128]
            list_ref[pl.ds(4 * j + i, tables, stride=16), :] = rows


def prep(ids, pool_len):
    return pl.pallas_call(
        prep_body,
        out_shape=pltpu.VMEM((128 * 4, 128), jnp.int32),
        out_specs=pl.BlockSpec(memory_space=pltpu.VMEM),
        in_specs=[pl.BlockSpec(memory_space=pltpu.VMEM), pl.BlockSpec(memory_space=pltpu.SMEM)],
        scratch_shapes=[pltpu.VMEM((ids.shape[0], 4 * CHUNK), jnp.int32)],
        name="bag_lists",
    )(ids, pool_len)


def widen_body(table_ref, tab, tbuf, tsem):
    def table_copy(b):
        slot = b % TSLOTS
        return pltpu.make_async_copy(
            table_ref.at[pl.ds(b * TBLK, TBLK)], tbuf.at[slot], tsem.at[slot]
        )

    blocks = ROWS_DEV // TBLK
    for b in range(TSLOTS):
        table_copy(b).start()
    tab[pl.ds(ROWS_DEV, 8), :] = jnp.zeros((8, E), jnp.float32)
    for b in range(blocks):
        table_copy(b).wait()
        tab[pl.ds(b * TBLK, TBLK), :] = tbuf[b % TSLOTS].astype(jnp.float32)
        if b + TSLOTS < blocks:
            table_copy(b + TSLOTS).start()


def widen(table):
    return pl.pallas_call(
        widen_body,
        out_shape=pltpu.VMEM((ROWS_DEV + 8, E), jnp.float32),
        in_specs=[pl.BlockSpec(memory_space=pltpu.HBM)],
        out_specs=pl.BlockSpec(memory_space=pltpu.VMEM),
        scratch_shapes=[
            pltpu.VMEM((TSLOTS, TBLK, E), jnp.bfloat16),
            pltpu.SemaphoreType.DMA((TSLOTS,)),
        ],
        compiler_params=pltpu.CompilerParams(vmem_limit_bytes=6 * 2**20),
        name="table_widen",
    )(pltpu.with_memory_space_constraint(table, pltpu.HBM))


def gather_body(quarter_ref, lists_ref, tab, out_ref, smem, acc, lsem, *, unroll):
    quarter = quarter_ref[0]
    planes = out_ref.shape[0] // 2
    piece = 2 * SLOTS

    def list_copy(m):
        start = pl.multiple_of((4 * m + quarter) * piece, piece)
        return pltpu.make_async_copy(
            lists_ref.at[pl.ds(start, piece)], smem.at[pl.ds(m * piece, piece)], lsem.at[m]
        )

    for m in range(planes):
        list_copy(m).start()

    def level(at):
        head = smem[at]
        rows = [head & 0xFFFF] + [smem[at + i] for i in range(1, 8)]
        rows = jnp.concatenate([tab[pl.ds(r, 1), :] for r in rows], axis=0)
        return pl.multiple_of((head >> 13) & 0x78, 8), rows

    def chunk(c, carry):
        base = c * SLOTS
        acc[...] = jnp.zeros(acc.shape, jnp.float32)
        levels = smem[base] >> 20

        def step(k, carry):
            at = base + k * (8 * unroll)
            for g, rows in [level(at + 8 * u) for u in range(unroll)]:
                acc[pl.ds(g, 8), :] += rows
            return carry

        lax.fori_loop(0, (levels + unroll - 1) >> (unroll.bit_length() - 1), step, 0)
        out_ref[c] = acc[pl.ds(0, CHUNK), :].astype(jnp.bfloat16)
        return carry

    for m in range(planes):
        list_copy(m).wait()
    lax.fori_loop(0, 2 * planes, chunk, 0)


def gather(quarter, lists, tab, planes, unroll=4):
    return pl.pallas_call(
        functools.partial(gather_body, unroll=unroll),
        out_shape=pltpu.VMEM((2 * planes, CHUNK, E), jnp.bfloat16),
        in_specs=[
            pl.BlockSpec(memory_space=pltpu.SMEM),
            pl.BlockSpec(memory_space=pl.ANY),
            pl.BlockSpec(memory_space=pltpu.VMEM),
        ],
        out_specs=pl.BlockSpec(memory_space=pltpu.VMEM),
        scratch_shapes=[
            pltpu.SMEM((2 * planes * SLOTS,), jnp.int32),
            pltpu.VMEM((CHUNK + 8, E), jnp.float32),
            pltpu.SemaphoreType.DMA((planes,)),
        ],
        compiler_params=pltpu.CompilerParams(vmem_limit_bytes=4 * 2**20),
        name="bag_gather",
    )(quarter, lists, tab)


def combine_body(y_ref, lists_ref, part_0, part_1, part_2, part_3, out_ref):
    y = y_ref[0]
    parts = (part_0, part_1, part_2, part_3)
    bag = lax.broadcasted_iota(jnp.int32, (CHUNK, 4 * CHUNK), 0)
    for c in range(out_ref.shape[0]):
        source = 8 * (c // 2) + 2 * y + c % 2
        words = lax.shift_right_logical(lists_ref[source], 20) & (CHUNK - 1)
        where = jnp.concatenate([words[2:3, :], words[3:4, :]], axis=1)
        pick = (bag == where).astype(jnp.float32).astype(jnp.bfloat16)
        rows = []
        for j in range(4):
            came = (y - j) & 3
            row = parts[3][c]
            for k in range(3):
                row = jnp.where(came == k, parts[k][c], row)
            rows.append(row)
        total = jnp.dot(pick, jnp.concatenate(rows, axis=0), preferred_element_type=jnp.float32)
        out_ref[c] = total.astype(jnp.bfloat16)


def combine(y, lists, parts):
    vmem = pl.BlockSpec(memory_space=pltpu.VMEM)
    return pl.pallas_call(
        combine_body,
        out_shape=pltpu.VMEM(parts[0].shape, jnp.bfloat16),
        in_specs=[pl.BlockSpec(memory_space=pltpu.SMEM)] + [vmem] * 5,
        out_specs=vmem,
        compiler_params=pltpu.CompilerParams(vmem_limit_bytes=4 * 2**20),
        name="bag_combine",
    )(y, lists, *[pltpu.with_memory_space_constraint(p, pltpu.VMEM) for p in parts])


def rows_body(pooled_ref, out_ref):
    for t in range(pooled_ref.shape[0]):
        out_ref[:, t * E : (t + 1) * E] = pooled_ref[t]


def feature_rows(pooled):
    tables, samples, _ = pooled.shape
    vmem = pl.BlockSpec(memory_space=pltpu.VMEM)
    return pl.pallas_call(
        rows_body,
        out_shape=pltpu.VMEM((samples, tables * E), jnp.bfloat16),
        in_specs=[vmem],
        out_specs=vmem,
        compiler_params=pltpu.CompilerParams(vmem_limit_bytes=2 * 2**20),
        name="feature_rows",
    )(pltpu.with_memory_space_constraint(pooled, pltpu.VMEM))


def swap(x, axis):
    return lax.all_to_all(jnp.broadcast_to(x[None], (2, *x.shape)), axis, 0, 0, tiled=True)


def body(indices, pool_len, tables, w_first, b_first, w_out):
    n_dev = lax.axis_size("dev")
    n_sec = lax.axis_size("section")
    n_tables = indices.shape[1]
    half = n_tables // n_sec
    section = lax.axis_index("section")
    dev = lax.axis_index("dev")
    lists = prep(jnp.transpose(indices, (1, 2, 0)), pool_len)
    ring = 4
    rows, cols = w_first.shape
    part = cols // HID_SPLIT
    planes = n_dev // ring
    levels = [[ring * p + y for p in range(planes)] for y in range(ring)]
    y = dev % ring
    q = dev % HID_SPLIT
    keep = lax.dynamic_slice(w_first, (0, q * part), (rows, part))
    give = lax.dynamic_slice(w_first, (0, (1 - q) * part), (rows, part))

    def along(x, k):
        return lax.ppermute(x, "dev", [(d, d // ring * ring + (d + k) % ring) for d in range(n_dev)])

    pieces = [keep, along(give, 1), along(keep, 2), along(give, 3)]
    pieces, lists = lax.optimization_barrier((pieces, lists))
    pieces = jnp.stack(pieces)
    pieces = [lax.dynamic_index_in_dim(pieces, (y - k) % ring, 0, False) for k in range(ring)]
    whole = lax.all_gather(jnp.concatenate(pieces), "dev", axis_index_groups=levels, tiled=True)
    both_axes = ("section", "dev")
    arrived = lax.all_to_all(lists.reshape(n_sec * n_dev, 4, 128), both_axes, 0, 0, tiled=True)
    line = lax.broadcasted_iota(jnp.int32, arrived.shape, 1)
    clean = jnp.where(line < 2, arrived, arrived & 0xFFFFF).reshape(-1)
    tab = widen(tables)
    parts = {}
    for k in (2, 1, 3, 0):
        quarter = ((y + k) % ring).reshape(1)
        sums = gather(quarter, clean, tab, planes)
        parts[k] = along(sums, k) if k else sums
    pooled = combine(y.reshape(1), arrived, [parts[k] for k in range(ring)])
    pooled = pooled.reshape(planes, 2 * CHUNK, E)
    pooled = lax.all_to_all(pooled, "dev", 0, 0, axis_index_groups=levels, tiled=True)
    features = feature_rows(pooled)
    bias = lax.dynamic_slice(b_first, (q * part,), (part,)).astype(jnp.float32)
    scale = lax.dynamic_slice(w_out, (q * part,), (part,)).astype(jnp.float32)
    far = lax.ppermute(features, "dev", [(d, d ^ 1) for d in range(n_dev)])
    k_half = half * E

    def logits_of(mine):
        both = swap(mine, "section")
        pre_act = jnp.dot(both[0], whole[:k_half], preferred_element_type=jnp.float32)
        pre_act += jnp.dot(both[1], whole[k_half:], preferred_element_type=jnp.float32)
        hidden = jnp.maximum(pre_act + bias[None, :], 0.0)
        return jnp.sum(hidden * scale[None, :], axis=1)

    near_part = logits_of(features)
    far, near_part = lax.optimization_barrier((far, near_part))
    far_part = logits_of(far)
    by_chip = jnp.stack([jnp.where(q == 0, near_part, far_part), jnp.where(q == 0, far_part, near_part)])
    quads = [[s * n_dev + 2 * p + i for s in range(n_sec) for i in range(2)] for p in range(n_dev // 2)]
    quarters = lax.all_gather(by_chip, both_axes, axis_index_groups=quads)
    return lax.dynamic_index_in_dim(quarters.sum(0), q, 0, False)


def solution(mesh):
    placed = (
        P(("section", "dev"), None, None),
        P(),
        P(("section", "dev"), None),
        P("dev", "section"),
        P("section"),
        P("section"),
    )
    return jax.shard_map(body, mesh=mesh, in_specs=placed, out_specs=P("dev"), check_vma=False)
```

```python
import functools

import jax
import jax.numpy as jnp
from jax import lax
from jax.experimental import pallas as pl
from jax.experimental.pallas import tpu as pltpu
from jax.sharding import PartitionSpec as P

E = 128
ROWS_DEV = 32768
POOL = 8
CHUNK = 64
SLOTS = POOL * CHUNK
DEAD = ROWS_DEV | (8 << 16)
TBLK = 2048
TSLOTS = 4
HID_SPLIT = 2
SORT8 = (
    (0, 2), (1, 3), (4, 6), (5, 7), (0, 4), (1, 5), (2, 6), (3, 7), (0, 1), (2, 3),
    (4, 5), (6, 7), (2, 4), (3, 5), (1, 4), (3, 6), (1, 2), (3, 4), (5, 6),
)


def prep_body(x_ref, pool_ref, list_ref, order_ref):
    shape = (CHUNK, 128)
    tables = x_ref.shape[0]
    lane = lax.broadcasted_iota(jnp.int32, shape, 1)
    bag = lax.broadcasted_iota(jnp.int32, shape, 0)
    table = lax.broadcasted_iota(jnp.int32, (8, 128), 1) & (tables - 1)
    live = jnp.zeros((8, 128), jnp.int32)
    for t in range(tables):
        live = jnp.where(table == t, pool_ref[t], live)
    live = jnp.concatenate([live] * (CHUNK // 8), axis=0)
    first = (lane // tables) * ROWS_DEV
    v = []
    for p in range(POOL):
        row = jnp.concatenate([x_ref[:, p, :]] * 4, axis=0).T - first
        ok = (row >= 0) & (row < ROWS_DEV) & (live > p)
        v.append(jnp.where(ok, row, ROWS_DEV))
    for a, b in SORT8:
        v[a], v[b] = jnp.minimum(v[a], v[b]), jnp.maximum(v[a], v[b])
    kept = sum((w < ROWS_DEV).astype(jnp.int32) for w in v)
    cols = [(POOL - kept) * CHUNK + bag]
    cols += [v[2 * k] | (v[2 * k + 1] << 16) for k in range(POOL // 2)]
    size = 2
    while size <= CHUNK:
        step = size // 2
        while step:
            upper = (bag & step) != 0
            small = ((bag & size) == 0) != upper
            other = [
                jnp.where(upper, pltpu.roll(c, step, 0), pltpu.roll(c, CHUNK - step, 0)) for c in cols
            ]
            take = jnp.where(small, other[0] - cols[0], cols[0] - other[0]) < 0
            cols = [jnp.where(take, o, c) for o, c in zip(other, cols)]
            step //= 2
        size *= 2
    key = cols[0]
    order = (((key & (CHUNK - 1)) | CHUNK) << 20).T
    for j in range(4):
        order_ref[:, j * CHUNK : (j + 1) * CHUNK] = order[j * tables : (j + 1) * tables, :]
    kept = POOL - (key >> 6)
    v = []
    for w in cols[1:]:
        v += [w & 0xFFFF, lax.shift_right_logical(w, 16)]
    tile = (8, 128)
    groups = []
    total = jnp.zeros((1, 128), jnp.int32)
    for g in range(CHUNK // 8):
        n = kept[8 * g : 8 * g + 1]
        shift = jnp.broadcast_to((8 * g - total) << 20, tile)
        n_all = jnp.broadcast_to(n, tile)
        for p in range(POOL):
            word = v[p][8 * g : 8 * g + 8] | (g << 16) | shift
            groups.append(jnp.where(n_all > p, word, DEAD))
        total = total + n
    for k in range(6):
        gap = 1 << k
        moves = [((w >> (20 + k)) & 1) != 0 for w in groups]
        new = []
        for i in range(64):
            stay = jnp.where(moves[i], DEAD, groups[i])
            if i + gap < 64:
                stay = jnp.where(moves[i + gap], groups[i + gap], stay)
            new.append(stay)
        groups = new
    head = lax.broadcasted_iota(jnp.int32, tile, 0) == 0
    mask = jnp.where(head, 0xFFFFF, 0xFFFF)
    groups = [w & mask for w in groups]
    groups[0] = groups[0] | jnp.where(head, jnp.broadcast_to(total << 20, tile), 0)
    for i in range(4):
        block = jnp.concatenate(groups[16 * i : 16 * i + 16], axis=0)
        block = block.T
        for j in range(4):
            rows = block[j * tables : (j + 1) * tables, :]
            if i >= 2:
                rows = rows | order_ref[:, (i - 2) * 128 : (i - 1) * 128]
            list_ref[pl.ds(4 * j + i, tables, stride=16), :] = rows


def prep(ids, pool_len):
    return pl.pallas_call(
        prep_body,
        out_shape=pltpu.VMEM((128 * 4, 128), jnp.int32),
        out_specs=pl.BlockSpec(memory_space=pltpu.VMEM),
        in_specs=[pl.BlockSpec(memory_space=pltpu.VMEM), pl.BlockSpec(memory_space=pltpu.SMEM)],
        scratch_shapes=[pltpu.VMEM((ids.shape[0], 4 * CHUNK), jnp.int32)],
        name="bag_lists",
    )(ids, pool_len)


def gather_body(quarter_ref, lists_ref, *refs, unroll, widen):
    if widen:
        table_ref, out_ref, tab, tbuf, tsem, smem, acc, lsem = refs
    else:
        tab, out_ref, smem, acc, lsem = refs
    quarter = quarter_ref[0]
    planes = out_ref.shape[0] // 2
    piece = 2 * SLOTS

    def list_copy(m):
        start = pl.multiple_of((4 * m + quarter) * piece, piece)
        return pltpu.make_async_copy(
            lists_ref.at[pl.ds(start, piece)],
            smem.at[pl.ds(pl.multiple_of(m * piece, piece), piece)],
            lsem.at[m],
        )

    if widen:

        def table_copy(b):
            slot = b % TSLOTS
            return pltpu.make_async_copy(
                table_ref.at[pl.ds(b * TBLK, TBLK)], tbuf.at[slot], tsem.at[slot]
            )

        blocks = ROWS_DEV // TBLK
        for b in range(TSLOTS):
            table_copy(b).start()
    for m in range(planes):
        list_copy(m).start()
    if widen:
        tab[pl.ds(ROWS_DEV, 8), :] = jnp.zeros((8, E), jnp.float32)
        for b in range(blocks):
            table_copy(b).wait()
            tab[pl.ds(b * TBLK, TBLK), :] = tbuf[b % TSLOTS].astype(jnp.float32)
            if b + TSLOTS < blocks:
                table_copy(b + TSLOTS).start()

    def level(at):
        head = smem[at]
        rows = [head & 0xFFFF] + [smem[at + i] for i in range(1, 8)]
        rows = jnp.concatenate([tab[pl.ds(r, 1), :] for r in rows], axis=0)
        return pl.multiple_of((head >> 13) & 0x78, 8), rows

    def chunk(c):
        base = c * SLOTS
        acc[...] = jnp.zeros(acc.shape, jnp.float32)
        levels = smem[base] >> 20

        def step(k, carry):
            at = base + k * (8 * unroll)
            for g, rows in [level(at + 8 * u) for u in range(unroll)]:
                acc[pl.ds(g, 8), :] += rows
            return carry

        lax.fori_loop(0, (levels + unroll - 1) >> (unroll.bit_length() - 1), step, 0)
        out_ref[c] = acc[pl.ds(0, CHUNK), :].astype(jnp.bfloat16)

    def plane(m, carry):
        list_copy(m).wait()
        chunk(2 * m)
        chunk(2 * m + 1)
        return carry

    lax.fori_loop(0, planes, plane, 0)


def gather(quarter, lists, table, planes, unroll=4, widen=False):
    vmem = pl.BlockSpec(memory_space=pltpu.VMEM)
    sums = pltpu.VMEM((2 * planes, CHUNK, E), jnp.bfloat16)
    scratch = [
        pltpu.SMEM((2 * planes * SLOTS,), jnp.int32),
        pltpu.VMEM((CHUNK + 8, E), jnp.float32),
        pltpu.SemaphoreType.DMA((planes,)),
    ]
    if widen:
        table = pltpu.with_memory_space_constraint(table, pltpu.HBM)
        scratch = [pltpu.VMEM((TSLOTS, TBLK, E), jnp.bfloat16), pltpu.SemaphoreType.DMA((TSLOTS,))] + scratch
    return pl.pallas_call(
        functools.partial(gather_body, unroll=unroll, widen=widen),
        out_shape=(sums, pltpu.VMEM((ROWS_DEV + 8, E), jnp.float32)) if widen else sums,
        in_specs=[
            pl.BlockSpec(memory_space=pltpu.SMEM),
            pl.BlockSpec(memory_space=pl.ANY),
            pl.BlockSpec(memory_space=pltpu.HBM) if widen else vmem,
        ],
        out_specs=(vmem, vmem) if widen else vmem,
        scratch_shapes=scratch,
        compiler_params=pltpu.CompilerParams(vmem_limit_bytes=(6 if widen else 4) * 2**20),
        name="bag_gather",
    )(quarter, lists, table)


def combine_body(y_ref, lists_ref, part_0, part_1, part_2, part_3, out_ref):
    y = y_ref[0]
    parts = (part_0, part_1, part_2, part_3)
    bag = lax.broadcasted_iota(jnp.int32, (CHUNK, 4 * CHUNK), 0)
    for c in range(out_ref.shape[0]):
        source = 8 * (c // 2) + 2 * y + c % 2
        words = lax.shift_right_logical(lists_ref[source], 20) & (CHUNK - 1)
        where = jnp.concatenate([words[2:3, :], words[3:4, :]], axis=1)
        pick = (bag == where).astype(jnp.float32).astype(jnp.bfloat16)
        rows = []
        for j in range(4):
            came = (y - j) & 3
            row = parts[3][c]
            for k in range(3):
                row = jnp.where(came == k, parts[k][c], row)
            rows.append(row)
        total = jnp.dot(pick, jnp.concatenate(rows, axis=0), preferred_element_type=jnp.float32)
        out_ref[c] = total.astype(jnp.bfloat16)


def combine(y, lists, parts):
    vmem = pl.BlockSpec(memory_space=pltpu.VMEM)
    return pl.pallas_call(
        combine_body,
        out_shape=pltpu.VMEM(parts[0].shape, jnp.bfloat16),
        in_specs=[pl.BlockSpec(memory_space=pltpu.SMEM)] + [vmem] * 5,
        out_specs=vmem,
        compiler_params=pltpu.CompilerParams(vmem_limit_bytes=4 * 2**20),
        name="bag_combine",
    )(y, lists, *[pltpu.with_memory_space_constraint(p, pltpu.VMEM) for p in parts])


def rows_body(pooled_ref, out_ref):
    for t in range(pooled_ref.shape[0]):
        out_ref[:, t * E : (t + 1) * E] = pooled_ref[t]


def feature_rows(pooled):
    tables, samples, _ = pooled.shape
    vmem = pl.BlockSpec(memory_space=pltpu.VMEM)
    return pl.pallas_call(
        rows_body,
        out_shape=pltpu.VMEM((samples, tables * E), jnp.bfloat16),
        in_specs=[vmem],
        out_specs=vmem,
        compiler_params=pltpu.CompilerParams(vmem_limit_bytes=2 * 2**20),
        name="feature_rows",
    )(pltpu.with_memory_space_constraint(pooled, pltpu.VMEM))


def swap(x, axis):
    return lax.all_to_all(jnp.broadcast_to(x[None], (2, *x.shape)), axis, 0, 0, tiled=True)


def body(indices, pool_len, tables, w_first, b_first, w_out):
    n_dev = lax.axis_size("dev")
    n_sec = lax.axis_size("section")
    n_tables = indices.shape[1]
    half = n_tables // n_sec
    section = lax.axis_index("section")
    dev = lax.axis_index("dev")
    lists = prep(jnp.transpose(indices, (1, 2, 0)), pool_len)
    ring = 4
    rows, cols = w_first.shape
    part = cols // HID_SPLIT
    planes = n_dev // ring
    levels = [[ring * p + y for p in range(planes)] for y in range(ring)]
    y = dev % ring
    q = dev % HID_SPLIT
    keep = lax.dynamic_slice(w_first, (0, q * part), (rows, part))
    give = lax.dynamic_slice(w_first, (0, (1 - q) * part), (rows, part))

    def along(x, k):
        return lax.ppermute(x, "dev", [(d, d // ring * ring + (d + k) % ring) for d in range(n_dev)])

    pieces = [keep, along(give, 1), along(keep, 2), along(give, 3)]
    pieces, lists = lax.optimization_barrier((pieces, lists))
    pieces = jnp.stack(pieces)
    pieces = [lax.dynamic_index_in_dim(pieces, (y - k) % ring, 0, False) for k in range(ring)]
    whole = lax.all_gather(jnp.concatenate(pieces), "dev", axis_index_groups=levels, tiled=True)
    both_axes = ("section", "dev")
    arrived = lax.all_to_all(lists.reshape(n_sec * n_dev, 4, 128), both_axes, 0, 0, tiled=True)
    line = lax.broadcasted_iota(jnp.int32, arrived.shape, 1)
    clean = jnp.where(line < 2, arrived, arrived & 0xFFFFF).reshape(-1)
    clean, tables = lax.optimization_barrier((clean, tables))
    parts = {}
    for k in (2, 1, 3, 0):
        quarter = ((y + k) % ring).reshape(1)
        if k == 2:
            sums, tab = gather(quarter, clean, tables, planes, widen=True)
        else:
            sums = gather(quarter, clean, tab, planes)
        parts[k] = along(sums, k) if k else sums
    pooled = combine(y.reshape(1), arrived, [parts[k] for k in range(ring)])
    pooled = pooled.reshape(planes, 2 * CHUNK, E)
    pooled = lax.all_to_all(pooled, "dev", 0, 0, axis_index_groups=levels, tiled=True)
    features = feature_rows(pooled)
    bias = lax.dynamic_slice(b_first, (q * part,), (part,)).astype(jnp.float32)
    scale = lax.dynamic_slice(w_out, (q * part,), (part,)).astype(jnp.float32)
    far = lax.ppermute(features, "dev", [(d, d ^ 1) for d in range(n_dev)])
    k_half = half * E

    def logits_of(mine):
        both = swap(mine, "section")
        pre_act = jnp.dot(both[0], whole[:k_half], preferred_element_type=jnp.float32)
        pre_act += jnp.dot(both[1], whole[k_half:], preferred_element_type=jnp.float32)
        hidden = jnp.maximum(pre_act + bias[None, :], 0.0)
        return jnp.sum(hidden * scale[None, :], axis=1)

    near = lax.all_gather(logits_of(features), "section").sum(0)
    far, near = lax.optimization_barrier((far, near))
    far_part = logits_of(far)

    def to_partner(x, turn):
        pairs = [(s * n_dev + d, (s ^ turn) * n_dev + (d ^ 1)) for s in range(n_sec) for d in range(n_dev)]
        return lax.ppermute(x, both_axes, pairs)

    return near + (to_partner(far_part, 0) + to_partner(far_part, 1))


def solution(mesh):
    placed = (
        P(("section", "dev"), None, None),
        P(),
        P(("section", "dev"), None),
        P("dev", "section"),
        P("section"),
        P("section"),
    )
    return jax.shard_map(body, mesh=mesh, in_specs=placed, out_specs=P("dev"), check_vma=False)
```

```python
import functools

import jax
import jax.numpy as jnp
from jax import lax
from jax.experimental import pallas as pl
from jax.experimental.pallas import tpu as pltpu
from jax.sharding import PartitionSpec as P


E = 128
ROWS_DEV = 32768
POOL = 8
CHUNK = 64
SLOTS = POOL * CHUNK
DEAD = ROWS_DEV | (8 << 16)
TBLK = 2048
TSLOTS = 4
HID_SPLIT = 2
WBLK = 512
SORT8 = (
    (0, 2), (1, 3), (4, 6), (5, 7), (0, 4), (1, 5), (2, 6), (3, 7), (0, 1), (2, 3),
    (4, 5), (6, 7), (2, 4), (3, 5), (1, 4), (3, 6), (1, 2), (3, 4), (5, 6),
)


def prep_body(x_ref, pool_ref, list_ref, order_ref):
    shape = (CHUNK, 128)
    tables = x_ref.shape[0]
    lane = lax.broadcasted_iota(jnp.int32, shape, 1)
    bag = lax.broadcasted_iota(jnp.int32, shape, 0)
    table = lax.broadcasted_iota(jnp.int32, (8, 128), 1) & (tables - 1)
    live = jnp.zeros((8, 128), jnp.int32)
    for t in range(tables):
        live = jnp.where(table == t, pool_ref[t], live)
    live = jnp.concatenate([live] * (CHUNK // 8), axis=0)
    first = (lane // tables) * ROWS_DEV
    v = []
    for p in range(POOL):
        row = jnp.concatenate([x_ref[:, p, :]] * 4, axis=0).T - first
        ok = (row >= 0) & (row < ROWS_DEV) & (live > p)
        v.append(jnp.where(ok, row, ROWS_DEV))
    for a, b in SORT8:
        v[a], v[b] = jnp.minimum(v[a], v[b]), jnp.maximum(v[a], v[b])
    kept = sum((w < ROWS_DEV).astype(jnp.int32) for w in v)
    cols = [(POOL - kept) * CHUNK + bag]
    cols += [v[2 * k] | (v[2 * k + 1] << 16) for k in range(POOL // 2)]
    size = 2
    while size <= CHUNK:
        step = size // 2
        while step:
            upper = (bag & step) != 0
            small = ((bag & size) == 0) != upper
            other = [
                jnp.where(upper, pltpu.roll(c, step, 0), pltpu.roll(c, CHUNK - step, 0)) for c in cols
            ]
            take = jnp.where(small, other[0] - cols[0], cols[0] - other[0]) < 0
            cols = [jnp.where(take, o, c) for o, c in zip(other, cols)]
            step //= 2
        size *= 2
    key = cols[0]
    order = (((key & (CHUNK - 1)) | CHUNK) << 20).T
    for j in range(4):
        order_ref[:, j * CHUNK : (j + 1) * CHUNK] = order[j * tables : (j + 1) * tables, :]
    kept = POOL - (key >> 6)
    v = []
    for w in cols[1:]:
        v += [w & 0xFFFF, lax.shift_right_logical(w, 16)]
    tile = (8, 128)
    groups = []
    total = jnp.zeros((1, 128), jnp.int32)
    for g in range(CHUNK // 8):
        n = kept[8 * g : 8 * g + 1]
        shift = jnp.broadcast_to((8 * g - total) << 20, tile)
        n_all = jnp.broadcast_to(n, tile)
        for p in range(POOL):
            word = v[p][8 * g : 8 * g + 8] | (g << 16) | shift
            groups.append(jnp.where(n_all > p, word, DEAD))
        total = total + n
    for k in range(6):
        gap = 1 << k
        moves = [((w >> (20 + k)) & 1) != 0 for w in groups]
        new = []
        for i in range(64):
            stay = jnp.where(moves[i], DEAD, groups[i])
            if i + gap < 64:
                stay = jnp.where(moves[i + gap], groups[i + gap], stay)
            new.append(stay)
        groups = new
    head = lax.broadcasted_iota(jnp.int32, tile, 0) == 0
    mask = jnp.where(head, 0xFFFFF, 0xFFFF)
    groups = [w & mask for w in groups]
    groups[0] = groups[0] | jnp.where(head, jnp.broadcast_to(total << 20, tile), 0)
    for i in range(4):
        block = jnp.concatenate(groups[16 * i : 16 * i + 16], axis=0)
        block = block.T
        for j in range(4):
            rows = block[j * tables : (j + 1) * tables, :]
            if i >= 2:
                rows = rows | order_ref[:, (i - 2) * 128 : (i - 1) * 128]
            list_ref[pl.ds(4 * j + i, tables, stride=16), :] = rows


def prep(ids, pool_len):
    return pl.pallas_call(
        prep_body,
        out_shape=pltpu.VMEM((128 * 4, 128), jnp.int32),
        out_specs=pl.BlockSpec(memory_space=pltpu.VMEM),
        in_specs=[pl.BlockSpec(memory_space=pltpu.VMEM), pl.BlockSpec(memory_space=pltpu.SMEM)],
        scratch_shapes=[pltpu.VMEM((ids.shape[0], 4 * CHUNK), jnp.int32)],
        name="bag_lists",
    )(ids, pool_len)


def gather_body(quarter_ref, lists_ref, *refs, unroll, widen):
    if widen:
        table_ref, out_ref, tab, tbuf, tsem, smem, acc, lsem = refs
    else:
        tab, out_ref, smem, acc, lsem = refs
    quarter = quarter_ref[0]
    planes = out_ref.shape[0] // 2
    piece = 2 * SLOTS

    def list_copy(m):
        start = pl.multiple_of((4 * m + quarter) * piece, piece)
        return pltpu.make_async_copy(
            lists_ref.at[pl.ds(start, piece)],
            smem.at[pl.ds(pl.multiple_of(m * piece, piece), piece)],
            lsem.at[m],
        )

    if widen:

        def table_copy(b):
            slot = b % TSLOTS
            return pltpu.make_async_copy(
                table_ref.at[pl.ds(b * TBLK, TBLK)], tbuf.at[slot], tsem.at[slot]
            )

        blocks = ROWS_DEV // TBLK
        for b in range(TSLOTS):
            table_copy(b).start()
    for m in range(planes):
        list_copy(m).start()
    if widen:
        tab[pl.ds(ROWS_DEV, 8), :] = jnp.zeros((8, E), jnp.float32)
        for b in range(blocks):
            table_copy(b).wait()
            tab[pl.ds(b * TBLK, TBLK), :] = tbuf[b % TSLOTS].astype(jnp.float32)
            if b + TSLOTS < blocks:
                table_copy(b + TSLOTS).start()

    def level(at):
        head = smem[at]
        rows = [head & 0xFFFF] + [smem[at + i] for i in range(1, 8)]
        rows = jnp.concatenate([tab[pl.ds(r, 1), :] for r in rows], axis=0)
        return pl.multiple_of((head >> 13) & 0x78, 8), rows

    def chunk(c):
        base = c * SLOTS
        acc[...] = jnp.zeros(acc.shape, jnp.float32)
        levels = smem[base] >> 20

        def step(k, carry):
            at = base + k * (8 * unroll)
            for g, rows in [level(at + 8 * u) for u in range(unroll)]:
                acc[pl.ds(g, 8), :] += rows
            return carry

        lax.fori_loop(0, (levels + unroll - 1) >> (unroll.bit_length() - 1), step, 0)
        out_ref[c] = acc[pl.ds(0, CHUNK), :].astype(jnp.bfloat16)

    def plane(m, carry):
        list_copy(m).wait()
        chunk(2 * m)
        chunk(2 * m + 1)
        return carry

    lax.fori_loop(0, planes, plane, 0)


def gather(quarter, lists, table, planes, unroll=4, widen=False):
    vmem = pl.BlockSpec(memory_space=pltpu.VMEM)
    sums = pltpu.VMEM((2 * planes, CHUNK, E), jnp.bfloat16)
    scratch = [
        pltpu.SMEM((2 * planes * SLOTS,), jnp.int32),
        pltpu.VMEM((CHUNK + 8, E), jnp.float32),
        pltpu.SemaphoreType.DMA((planes,)),
    ]
    if widen:
        table = pltpu.with_memory_space_constraint(table, pltpu.HBM)
        scratch = [pltpu.VMEM((TSLOTS, TBLK, E), jnp.bfloat16), pltpu.SemaphoreType.DMA((TSLOTS,))] + scratch
    return pl.pallas_call(
        functools.partial(gather_body, unroll=unroll, widen=widen),
        out_shape=(sums, pltpu.VMEM((ROWS_DEV + 8, E), jnp.float32)) if widen else sums,
        in_specs=[
            pl.BlockSpec(memory_space=pltpu.SMEM),
            pl.BlockSpec(memory_space=pl.ANY),
            pl.BlockSpec(memory_space=pltpu.HBM) if widen else vmem,
        ],
        out_specs=(vmem, vmem) if widen else vmem,
        scratch_shapes=scratch,
        compiler_params=pltpu.CompilerParams(vmem_limit_bytes=(6 if widen else 4) * 2**20),
        name="bag_gather",
    )(quarter, lists, table)


def combine_body(y_ref, lists_ref, part_0, part_1, part_2, part_3, out_ref):
    y = y_ref[0]
    parts = (part_0, part_1, part_2, part_3)
    bag = lax.broadcasted_iota(jnp.int32, (CHUNK, 4 * CHUNK), 0)
    for c in range(out_ref.shape[0]):
        source = 8 * (c // 2) + 2 * y + c % 2
        words = lax.shift_right_logical(lists_ref[source], 20) & (CHUNK - 1)
        where = jnp.concatenate([words[2:3, :], words[3:4, :]], axis=1)
        pick = (bag == where).astype(jnp.float32).astype(jnp.bfloat16)
        rows = []
        for j in range(4):
            came = (y - j) & 3
            row = parts[3][c]
            for k in range(3):
                row = jnp.where(came == k, parts[k][c], row)
            rows.append(row)
        total = jnp.dot(pick, jnp.concatenate(rows, axis=0), preferred_element_type=jnp.float32)
        out_ref[c] = total.astype(jnp.bfloat16)


def combine(y, lists, parts):
    vmem = pl.BlockSpec(memory_space=pltpu.VMEM)
    return pl.pallas_call(
        combine_body,
        out_shape=pltpu.VMEM(parts[0].shape, jnp.bfloat16),
        in_specs=[pl.BlockSpec(memory_space=pltpu.SMEM)] + [vmem] * 5,
        out_specs=vmem,
        compiler_params=pltpu.CompilerParams(vmem_limit_bytes=4 * 2**20),
        name="bag_combine",
    )(y, lists, *[pltpu.with_memory_space_constraint(p, pltpu.VMEM) for p in parts])


def rows_body(pooled_ref, out_ref):
    for t in range(pooled_ref.shape[0]):
        out_ref[:, t * E : (t + 1) * E] = pooled_ref[t]


def feature_rows(pooled):
    tables, samples, _ = pooled.shape
    vmem = pl.BlockSpec(memory_space=pltpu.VMEM)
    return pl.pallas_call(
        rows_body,
        out_shape=pltpu.VMEM((samples, tables * E), jnp.bfloat16),
        in_specs=[vmem],
        out_specs=vmem,
        compiler_params=pltpu.CompilerParams(vmem_limit_bytes=2 * 2**20),
        name="feature_rows",
    )(pltpu.with_memory_space_constraint(pooled, pltpu.VMEM))


def dense_body(both_ref, w_ref, bias_ref, scale_ref, *refs, stream):
    if stream:
        out_ref, kept, acc, sem = refs
        blocks = [pl.ds(b * WBLK, WBLK) for b in range(kept.shape[0] // WBLK)]
        copies = [pltpu.make_async_copy(w_ref.at[b], kept.at[b], sem.at[i]) for i, b in enumerate(blocks)]
        for copy in copies:
            copy.start()
    else:
        out_ref, acc = refs
        kept = w_ref
        blocks = [pl.ds(b * WBLK, WBLK) for b in range(kept.shape[0] // WBLK)]
    wide = both_ref.shape[2]
    for i, block in enumerate(blocks):
        if stream:
            copies[i].wait()
        at = i * WBLK
        x = both_ref[at // wide, :, at % wide : at % wide + WBLK]
        prod = jnp.dot(x, kept[block, :], preferred_element_type=jnp.float32)
        acc[...] = prod if i == 0 else acc[...] + prod
    part = jnp.maximum(acc[...] + bias_ref[...], 0.0) * scale_ref[...]
    lanes = sum(part[:, 128 * i : 128 * i + 128] for i in range(part.shape[1] // 128))
    out_ref[...] = jnp.sum(lanes.T, axis=0, keepdims=True)


def dense(both, weights, bias, scale, stream):
    vmem = pl.BlockSpec(memory_space=pltpu.VMEM)
    samples = both.shape[1]
    rows, units = weights.shape
    out = pltpu.VMEM((1, samples), jnp.float32)
    scratch = [pltpu.VMEM((samples, units), jnp.float32)]
    if stream:
        weights = pltpu.with_memory_space_constraint(weights, pltpu.HBM)
        scratch.append(pltpu.SemaphoreType.DMA((rows // WBLK,)))
    return pl.pallas_call(
        functools.partial(dense_body, stream=stream),
        out_shape=(out, pltpu.VMEM(weights.shape, weights.dtype)) if stream else out,
        in_specs=[vmem, pl.BlockSpec(memory_space=pltpu.HBM) if stream else vmem, vmem, vmem],
        out_specs=(vmem, vmem) if stream else vmem,
        scratch_shapes=scratch,
        compiler_params=pltpu.CompilerParams(vmem_limit_bytes=8 * 2**20),
        name="dense_near" if stream else "dense_far",
    )(pltpu.with_memory_space_constraint(both, pltpu.VMEM), weights, bias, scale)


def swap(x, axis):
    return lax.all_to_all(jnp.broadcast_to(x[None], (2, *x.shape)), axis, 0, 0, tiled=True)


def body(indices, pool_len, tables, w_first, b_first, w_out):
    n_dev = lax.axis_size("dev")
    n_sec = lax.axis_size("section")
    dev = lax.axis_index("dev")
    lists = prep(jnp.transpose(indices, (1, 2, 0)), pool_len)
    ring = 4
    rows, cols = w_first.shape
    part = cols // HID_SPLIT
    planes = n_dev // ring
    levels = [[ring * p + y for p in range(planes)] for y in range(ring)]
    y = dev % ring
    q = dev % HID_SPLIT
    keep = lax.dynamic_slice(w_first, (0, q * part), (rows, part))
    give = lax.dynamic_slice(w_first, (0, (1 - q) * part), (rows, part))

    def along(x, k):
        return lax.ppermute(x, "dev", [(d, d // ring * ring + (d + k) % ring) for d in range(n_dev)])

    pieces = [keep, along(give, 1), along(keep, 2), along(give, 3)]
    pieces = jnp.stack(pieces)
    pieces = [lax.dynamic_index_in_dim(pieces, (y - k) % ring, 0, False) for k in range(ring)]
    whole = lax.all_gather(jnp.concatenate(pieces), "dev", axis_index_groups=levels, tiled=True)
    both_axes = ("section", "dev")
    arrived = lax.all_to_all(lists.reshape(n_sec * n_dev, 4, 128), both_axes, 0, 0, tiled=True)
    line = lax.broadcasted_iota(jnp.int32, arrived.shape, 1)
    clean = jnp.where(line < 2, arrived, arrived & 0xFFFFF).reshape(-1)
    clean, tables = lax.optimization_barrier((clean, tables))
    parts = {}
    for k in (2, 1, 3, 0):
        quarter = ((y + k) % ring).reshape(1)
        if k == 2:
            sums, tab = gather(quarter, clean, tables, planes, widen=True)
        else:
            sums = gather(quarter, clean, tab, planes)
        parts[k] = along(sums, k) if k else sums
    pooled = combine(y.reshape(1), arrived, [parts[k] for k in range(ring)])
    pooled = pooled.reshape(planes, 2 * CHUNK, E)
    pooled = lax.all_to_all(pooled, "dev", 0, 0, axis_index_groups=levels, tiled=True)
    features = feature_rows(pooled)
    bias = lax.dynamic_slice(b_first, (q * part,), (part,)).astype(jnp.float32)
    scale = lax.dynamic_slice(w_out, (q * part,), (part,)).astype(jnp.float32)
    far = lax.ppermute(features, "dev", [(d, d ^ 1) for d in range(n_dev)])
    bias, scale = bias.reshape(1, part), scale.reshape(1, part)
    near, kept = dense(swap(features, "section"), whole, bias, scale, True)
    near = lax.all_gather(near.reshape(-1), "section")
    far, near = lax.optimization_barrier((far, near))
    far_part = dense(swap(far, "section"), kept, bias, scale, False).reshape(-1)
    far_part, near = lax.optimization_barrier((far_part, near))

    def to_partner(x, turn):
        pairs = [(s * n_dev + d, (s ^ turn) * n_dev + (d ^ 1)) for s in range(n_sec) for d in range(n_dev)]
        return lax.ppermute(x, both_axes, pairs)

    return (near[0] + near[1]) + (to_partner(far_part, 0) + to_partner(far_part, 1))


def solution(mesh):
    placed = (
        P(("section", "dev"), None, None),
        P(),
        P(("section", "dev"), None),
        P("dev", "section"),
        P("section"),
        P("section"),
    )
    return jax.shard_map(body, mesh=mesh, in_specs=placed, out_specs=P("dev"), check_vma=False)
```

```python
import functools

import jax
import jax.numpy as jnp
from jax import lax
from jax.experimental import pallas as pl
from jax.experimental.pallas import tpu as pltpu
from jax.sharding import PartitionSpec as P


E = 128
ROWS_DEV = 32768
POOL = 8
CHUNK = 64
SLOTS = POOL * CHUNK
DEAD = ROWS_DEV | (8 << 16)
TBLK = 2048
TSLOTS = 4
HID_SPLIT = 2
WBLK = 512
CALLS = (("c", 2, 0, 2), ("b", 1, 0, 2), ("d", 3, 0, 1), ("e", 3, 1, 1), ("a", 0, 0, 2))
SORT8 = (
    (0, 2), (1, 3), (4, 6), (5, 7), (0, 4), (1, 5), (2, 6), (3, 7), (0, 1), (2, 3),
    (4, 5), (6, 7), (2, 4), (3, 5), (1, 4), (3, 6), (1, 2), (3, 4), (5, 6),
)


def prep_body(x_ref, pool_ref, list_ref, order_ref):
    shape = (CHUNK, 128)
    tables = x_ref.shape[0]
    lane = lax.broadcasted_iota(jnp.int32, shape, 1)
    bag = lax.broadcasted_iota(jnp.int32, shape, 0)
    table = lax.broadcasted_iota(jnp.int32, (8, 128), 1) & (tables - 1)
    live = jnp.zeros((8, 128), jnp.int32)
    for t in range(tables):
        live = jnp.where(table == t, pool_ref[t], live)
    live = jnp.concatenate([live] * (CHUNK // 8), axis=0)
    first = (lane // tables) * ROWS_DEV
    v = []
    for p in range(POOL):
        row = jnp.concatenate([x_ref[:, p, :]] * 4, axis=0).T - first
        ok = (row >= 0) & (row < ROWS_DEV) & (live > p)
        v.append(jnp.where(ok, row, ROWS_DEV))
    for a, b in SORT8:
        v[a], v[b] = jnp.minimum(v[a], v[b]), jnp.maximum(v[a], v[b])
    kept = sum((w < ROWS_DEV).astype(jnp.int32) for w in v)
    cols = [(POOL - kept) * CHUNK + bag]
    cols += [v[2 * k] | (v[2 * k + 1] << 16) for k in range(POOL // 2)]
    size = 2
    while size <= CHUNK:
        step = size // 2
        while step:
            upper = (bag & step) != 0
            small = ((bag & size) == 0) != upper
            other = [
                jnp.where(upper, pltpu.roll(c, step, 0), pltpu.roll(c, CHUNK - step, 0)) for c in cols
            ]
            take = jnp.where(small, other[0] - cols[0], cols[0] - other[0]) < 0
            cols = [jnp.where(take, o, c) for o, c in zip(other, cols)]
            step //= 2
        size *= 2
    key = cols[0]
    order = (((key & (CHUNK - 1)) | CHUNK) << 20).T
    for j in range(4):
        order_ref[:, j * CHUNK : (j + 1) * CHUNK] = order[j * tables : (j + 1) * tables, :]
    kept = POOL - (key >> 6)
    v = []
    for w in cols[1:]:
        v += [w & 0xFFFF, lax.shift_right_logical(w, 16)]
    tile = (8, 128)
    groups = []
    total = jnp.zeros((1, 128), jnp.int32)
    for g in range(CHUNK // 8):
        n = kept[8 * g : 8 * g + 1]
        shift = jnp.broadcast_to((8 * g - total) << 20, tile)
        n_all = jnp.broadcast_to(n, tile)
        for p in range(POOL):
            word = v[p][8 * g : 8 * g + 8] | (g << 16) | shift
            groups.append(jnp.where(n_all > p, word, DEAD))
        total = total + n
    for k in range(6):
        gap = 1 << k
        moves = [((w >> (20 + k)) & 1) != 0 for w in groups]
        new = []
        for i in range(64):
            stay = jnp.where(moves[i], DEAD, groups[i])
            if i + gap < 64:
                stay = jnp.where(moves[i + gap], groups[i + gap], stay)
            new.append(stay)
        groups = new
    head = lax.broadcasted_iota(jnp.int32, tile, 0) == 0
    mask = jnp.where(head, 0xFFFFF, 0xFFFF)
    groups = [w & mask for w in groups]
    groups[0] = groups[0] | jnp.where(head, jnp.broadcast_to(total << 20, tile), 0)
    for i in range(4):
        block = jnp.concatenate(groups[16 * i : 16 * i + 16], axis=0)
        block = block.T
        for j in range(4):
            rows = block[j * tables : (j + 1) * tables, :]
            if i >= 2:
                rows = rows | order_ref[:, (i - 2) * 128 : (i - 1) * 128]
            list_ref[pl.ds(4 * j + i, tables, stride=16), :] = rows


def prep(ids, pool_len):
    return pl.pallas_call(
        prep_body,
        out_shape=pltpu.VMEM((128 * 4, 128), jnp.int32),
        out_specs=pl.BlockSpec(memory_space=pltpu.VMEM),
        in_specs=[pl.BlockSpec(memory_space=pltpu.VMEM), pl.BlockSpec(memory_space=pltpu.SMEM)],
        scratch_shapes=[pltpu.VMEM((ids.shape[0], 4 * CHUNK), jnp.int32)],
        name="bag_lists",
    )(ids, pool_len)


def gather_body(y_ref, lists_ref, *refs, unroll, widen, first, ahead):
    if widen:
        table_ref, out_ref, tab, tbuf, tsem, smem, acc, lsem = refs
    else:
        tab, out_ref, smem, acc, lsem = refs
    quarter = (y_ref[0] + ahead) & 3
    planes = out_ref.shape[0] // 2
    piece = 2 * SLOTS

    def list_copy(m):
        start = pl.multiple_of((4 * (first + m) + quarter) * piece, piece)
        return pltpu.make_async_copy(
            lists_ref.at[pl.ds(start, piece)],
            smem.at[pl.ds(pl.multiple_of(m * piece, piece), piece)],
            lsem.at[m],
        )

    if widen:

        def table_copy(b):
            slot = b % TSLOTS
            return pltpu.make_async_copy(
                table_ref.at[pl.ds(b * TBLK, TBLK)], tbuf.at[slot], tsem.at[slot]
            )

        blocks = ROWS_DEV // TBLK
        for b in range(TSLOTS):
            table_copy(b).start()
    for m in range(planes):
        list_copy(m).start()
    if widen:
        tab[pl.ds(ROWS_DEV, 8), :] = jnp.zeros((8, E), jnp.float32)
        for b in range(blocks):
            table_copy(b).wait()
            tab[pl.ds(b * TBLK, TBLK), :] = tbuf[b % TSLOTS].astype(jnp.float32)
            if b + TSLOTS < blocks:
                table_copy(b + TSLOTS).start()

    def level(at):
        head = smem[at]
        rows = [head & 0xFFFF] + [smem[at + i] for i in range(1, 8)]
        rows = jnp.concatenate([tab[pl.ds(r, 1), :] for r in rows], axis=0)
        return pl.multiple_of((head >> 13) & 0x78, 8), rows

    def chunk(c):
        base = c * SLOTS
        acc[...] = jnp.zeros(acc.shape, jnp.float32)
        levels = smem[base] >> 20

        def step(k, carry):
            at = base + k * (8 * unroll)
            for g, rows in [level(at + 8 * u) for u in range(unroll)]:
                acc[pl.ds(g, 8), :] += rows
            return carry

        lax.fori_loop(0, (levels + unroll - 1) >> (unroll.bit_length() - 1), step, 0)
        out_ref[c] = acc[pl.ds(0, CHUNK), :].astype(jnp.bfloat16)

    def plane(m, carry):
        list_copy(m).wait()
        chunk(2 * m)
        chunk(2 * m + 1)
        return carry

    lax.fori_loop(0, planes, plane, 0)


def gather(y, ahead, lists, table, planes, first=0, unroll=4, widen=False):
    vmem = pl.BlockSpec(memory_space=pltpu.VMEM)
    sums = pltpu.VMEM((2 * planes, CHUNK, E), jnp.bfloat16)
    scratch = [
        pltpu.SMEM((2 * planes * SLOTS,), jnp.int32),
        pltpu.VMEM((CHUNK + 8, E), jnp.float32),
        pltpu.SemaphoreType.DMA((planes,)),
    ]
    if widen:
        table = pltpu.with_memory_space_constraint(table, pltpu.HBM)
        scratch = [pltpu.VMEM((TSLOTS, TBLK, E), jnp.bfloat16), pltpu.SemaphoreType.DMA((TSLOTS,))] + scratch
    return pl.pallas_call(
        functools.partial(gather_body, unroll=unroll, widen=widen, first=first, ahead=ahead),
        out_shape=(sums, pltpu.VMEM((ROWS_DEV + 8, E), jnp.float32)) if widen else sums,
        in_specs=[
            pl.BlockSpec(memory_space=pltpu.SMEM),
            pl.BlockSpec(memory_space=pl.ANY),
            pl.BlockSpec(memory_space=pltpu.HBM) if widen else vmem,
        ],
        out_specs=(vmem, vmem) if widen else vmem,
        scratch_shapes=scratch,
        compiler_params=pltpu.CompilerParams(vmem_limit_bytes=(6 if widen else 4) * 2**20),
        name="bag_gather",
    )(y, lists, table)


def combine_body(y_ref, lists_ref, part_0, part_1, part_2, part_3, part_3b, out_ref):
    y = y_ref[0]
    parts = (part_0, part_1, part_2)
    half = part_3.shape[0]
    bag = lax.broadcasted_iota(jnp.int32, (CHUNK, 4 * CHUNK), 0)
    for c in range(out_ref.shape[0]):
        source = 8 * (c // 2) + 2 * y + c % 2
        words = lax.shift_right_logical(lists_ref[source], 20) & (CHUNK - 1)
        where = jnp.concatenate([words[2:3, :], words[3:4, :]], axis=1)
        pick = (bag == where).astype(jnp.float32).astype(jnp.bfloat16)
        rows = []
        for j in range(4):
            came = (y - j) & 3
            row = part_3[c] if c < half else part_3b[c - half]
            for k in range(3):
                row = jnp.where(came == k, parts[k][c], row)
            rows.append(row)
        total = jnp.dot(pick, jnp.concatenate(rows, axis=0), preferred_element_type=jnp.float32)
        out_ref[c] = total.astype(jnp.bfloat16)


def combine(y, lists, parts):
    vmem = pl.BlockSpec(memory_space=pltpu.VMEM)
    return pl.pallas_call(
        combine_body,
        out_shape=pltpu.VMEM(parts[0].shape, jnp.bfloat16),
        in_specs=[pl.BlockSpec(memory_space=pltpu.SMEM)] + [vmem] * (1 + len(parts)),
        out_specs=vmem,
        compiler_params=pltpu.CompilerParams(vmem_limit_bytes=4 * 2**20),
        name="bag_combine",
    )(y, lists, *[pltpu.with_memory_space_constraint(p, pltpu.VMEM) for p in parts])


def rows_body(pooled_ref, out_ref):
    for t in range(pooled_ref.shape[0]):
        out_ref[:, t * E : (t + 1) * E] = pooled_ref[t]


def feature_rows(pooled):
    tables, samples, _ = pooled.shape
    vmem = pl.BlockSpec(memory_space=pltpu.VMEM)
    return pl.pallas_call(
        rows_body,
        out_shape=pltpu.VMEM((samples, tables * E), jnp.bfloat16),
        in_specs=[vmem],
        out_specs=vmem,
        compiler_params=pltpu.CompilerParams(vmem_limit_bytes=2 * 2**20),
        name="feature_rows",
    )(pltpu.with_memory_space_constraint(pooled, pltpu.VMEM))


def dense_body(both_ref, w_ref, bias_ref, scale_ref, *refs, stream):
    if stream:
        out_ref, kept, acc, sem = refs
        blocks = [pl.ds(b * WBLK, WBLK) for b in range(kept.shape[0] // WBLK)]
        copies = [pltpu.make_async_copy(w_ref.at[b], kept.at[b], sem.at[i]) for i, b in enumerate(blocks)]
        for copy in copies:
            copy.start()
    else:
        out_ref, acc = refs
        kept = w_ref
        blocks = [pl.ds(b * WBLK, WBLK) for b in range(kept.shape[0] // WBLK)]
    wide = both_ref.shape[2]
    for i, block in enumerate(blocks):
        if stream:
            copies[i].wait()
        at = i * WBLK
        x = both_ref[at // wide, :, at % wide : at % wide + WBLK]
        prod = jnp.dot(x, kept[block, :], preferred_element_type=jnp.float32)
        acc[...] = prod if i == 0 else acc[...] + prod
    part = jnp.maximum(acc[...] + bias_ref[...], 0.0) * scale_ref[...]
    lanes = sum(part[:, 128 * i : 128 * i + 128] for i in range(part.shape[1] // 128))
    out_ref[...] = jnp.sum(lanes.T, axis=0, keepdims=True)


def dense(both, weights, bias, scale, stream):
    vmem = pl.BlockSpec(memory_space=pltpu.VMEM)
    samples = both.shape[1]
    rows, units = weights.shape
    out = pltpu.VMEM((1, samples), jnp.float32)
    scratch = [pltpu.VMEM((samples, units), jnp.float32)]
    if stream:
        weights = pltpu.with_memory_space_constraint(weights, pltpu.HBM)
        scratch.append(pltpu.SemaphoreType.DMA((rows // WBLK,)))
    return pl.pallas_call(
        functools.partial(dense_body, stream=stream),
        out_shape=(out, pltpu.VMEM(weights.shape, weights.dtype)) if stream else out,
        in_specs=[vmem, pl.BlockSpec(memory_space=pltpu.HBM) if stream else vmem, vmem, vmem],
        out_specs=(vmem, vmem) if stream else vmem,
        scratch_shapes=scratch,
        compiler_params=pltpu.CompilerParams(vmem_limit_bytes=8 * 2**20),
        name="dense_near" if stream else "dense_far",
    )(pltpu.with_memory_space_constraint(both, pltpu.VMEM), weights, bias, scale)


def swap(x, axis):
    return lax.all_to_all(jnp.broadcast_to(x[None], (2, *x.shape)), axis, 0, 0, tiled=True)


def body(indices, pool_len, tables, w_first, b_first, w_out):
    n_dev = lax.axis_size("dev")
    n_sec = lax.axis_size("section")
    dev = lax.axis_index("dev")
    lists = prep(jnp.transpose(indices, (1, 2, 0)), pool_len)
    ring = 4
    rows, cols = w_first.shape
    part = cols // HID_SPLIT
    planes = n_dev // ring
    levels = [[ring * p + y for p in range(planes)] for y in range(ring)]
    y = dev % ring
    q = dev % HID_SPLIT
    keep = lax.dynamic_slice(w_first, (0, q * part), (rows, part))
    give = lax.dynamic_slice(w_first, (0, (1 - q) * part), (rows, part))

    def along(x, k):
        return lax.ppermute(x, "dev", [(d, d // ring * ring + (d + k) % ring) for d in range(n_dev)])

    pieces = [keep, along(give, 1), along(keep, 2), along(give, 3)]
    pieces = jnp.stack(pieces)
    pieces = [lax.dynamic_index_in_dim(pieces, (y - k) % ring, 0, False) for k in range(ring)]
    whole = lax.all_gather(jnp.concatenate(pieces), "dev", axis_index_groups=levels, tiled=True)
    both_axes = ("section", "dev")
    arrived = lax.all_to_all(lists.reshape(n_sec * n_dev, 4, 128), both_axes, 0, 0, tiled=True)
    line = lax.broadcasted_iota(jnp.int32, arrived.shape, 1)
    clean = jnp.where(line < 2, arrived, arrived & 0xFFFFF).reshape(-1)
    clean, tables = lax.optimization_barrier((clean, tables))
    here = y.reshape(1)
    split = planes // 2
    parts, tab = {}, None
    for name, k, first, count in CALLS:
        first, count = first * split, count * split
        if tab is None:
            sums, tab = gather(here, k, clean, tables, count, first, widen=True)
        else:
            sums = gather(here, k, clean, tab, count, first)
        parts[name] = along(sums, k) if k else sums
    pooled = combine(here, arrived, [parts[name] for name in "abcde"])
    pooled = pooled.reshape(planes, 2 * CHUNK, E)
    pooled = lax.all_to_all(pooled, "dev", 0, 0, axis_index_groups=levels, tiled=True)
    features = feature_rows(pooled)
    bias = lax.dynamic_slice(b_first, (q * part,), (part,)).astype(jnp.float32)
    scale = lax.dynamic_slice(w_out, (q * part,), (part,)).astype(jnp.float32)
    far = lax.ppermute(features, "dev", [(d, d ^ 1) for d in range(n_dev)])
    bias, scale = bias.reshape(1, part), scale.reshape(1, part)
    near, kept = dense(swap(features, "section"), whole, bias, scale, True)
    near = lax.all_gather(near.reshape(-1), "section")
    far, near = lax.optimization_barrier((far, near))
    far_part = dense(swap(far, "section"), kept, bias, scale, False).reshape(-1)
    far_part, near = lax.optimization_barrier((far_part, near))

    def to_partner(x, turn):
        pairs = [(s * n_dev + d, (s ^ turn) * n_dev + (d ^ 1)) for s in range(n_sec) for d in range(n_dev)]
        return lax.ppermute(x, both_axes, pairs)

    return (near[0] + near[1]) + (to_partner(far_part, 0) + to_partner(far_part, 1))


def solution(mesh):
    placed = (
        P(("section", "dev"), None, None),
        P(),
        P(("section", "dev"), None),
        P("dev", "section"),
        P("section"),
        P("section"),
    )
    return jax.shard_map(body, mesh=mesh, in_specs=placed, out_specs=P("dev"), check_vma=False)
```

```python
import functools

import jax
import jax.numpy as jnp
from jax import lax
from jax.experimental import pallas as pl
from jax.experimental.pallas import tpu as pltpu
from jax.sharding import PartitionSpec as P


E = 128
ROWS_DEV = 32768
POOL = 8
CHUNK = 64
SLOTS = POOL * CHUNK
DEAD = ROWS_DEV | (8 << 16)
TBLK = 2048
TSLOTS = 4
LSLOTS = 4
HID_SPLIT = 2
WBLK = 512
CALLS = (("c", 2, 0, 2), ("b", 1, 0, 2), ("d", 3, 0, 1), ("e", 3, 1, 1), ("a", 0, 0, 2))
SORT8 = (
    (0, 2), (1, 3), (4, 6), (5, 7), (0, 4), (1, 5), (2, 6), (3, 7), (0, 1), (2, 3),
    (4, 5), (6, 7), (2, 4), (3, 5), (1, 4), (3, 6), (1, 2), (3, 4), (5, 6),
)


def prep_body(x_ref, pool_ref, list_ref, order_ref, group_ref):
    shape = (CHUNK, 128)
    tables = x_ref.shape[0]
    lane = lax.broadcasted_iota(jnp.int32, shape, 1)
    bag = lax.broadcasted_iota(jnp.int32, shape, 0)
    table = lax.broadcasted_iota(jnp.int32, (8, 128), 1) & (tables - 1)
    live = jnp.zeros((8, 128), jnp.int32)
    for t in range(tables):
        live = jnp.where(table == t, pool_ref[t], live)
    live = jnp.concatenate([live] * (CHUNK // 8), axis=0)
    first = (lane // tables) * ROWS_DEV
    v = []
    for p in range(POOL):
        row = jnp.concatenate([x_ref[:, p, :]] * 4, axis=0).T - first
        ok = (row >= 0) & (row < ROWS_DEV) & (live > p)
        v.append(jnp.where(ok, row, ROWS_DEV))
    for a, b in SORT8:
        v[a], v[b] = jnp.minimum(v[a], v[b]), jnp.maximum(v[a], v[b])
    kept = sum((w < ROWS_DEV).astype(jnp.int32) for w in v)
    cols = [(POOL - kept) * CHUNK + bag]
    cols += [v[2 * k] | (v[2 * k + 1] << 16) for k in range(POOL // 2)]
    size = 2
    while size <= CHUNK:
        step = size // 2
        while step:
            upper = (bag & step) != 0
            small = ((bag & size) == 0) != upper
            other = [
                jnp.where(upper, pltpu.roll(c, step, 0), pltpu.roll(c, CHUNK - step, 0)) for c in cols
            ]
            take = jnp.where(small, other[0] - cols[0], cols[0] - other[0]) < 0
            cols = [jnp.where(take, o, c) for o, c in zip(other, cols)]
            step //= 2
        size *= 2
    key = cols[0]
    order = (((key & (CHUNK - 1)) | CHUNK) << 20).T
    for j in range(4):
        order_ref[:, j * CHUNK : (j + 1) * CHUNK] = order[j * tables : (j + 1) * tables, :]
    kept = POOL - (key >> 6)
    v = []
    for w in cols[1:]:
        v += [w & 0xFFFF, lax.shift_right_logical(w, 16)]
    tile = (8, 128)
    groups = []
    total = jnp.zeros((1, 128), jnp.int32)
    for g in range(CHUNK // 8):
        n = kept[8 * g : 8 * g + 1]
        shift = jnp.broadcast_to((8 * g - total) << 20, tile)
        n_all = jnp.broadcast_to(n, tile)
        for p in range(POOL):
            word = v[p][8 * g : 8 * g + 8] | (g << 16) | shift
            groups.append(jnp.where(n_all > p, word, DEAD))
        total = total + n
    for k in range(6):
        gap = 1 << k
        moves = [((w >> (20 + k)) & 1) != 0 for w in groups]
        new = []
        for i in range(64):
            stay = jnp.where(moves[i], DEAD, groups[i])
            if i + gap < 64:
                stay = jnp.where(moves[i + gap], groups[i + gap], stay)
            new.append(stay)
        groups = new
    head = lax.broadcasted_iota(jnp.int32, tile, 0) == 0
    mask = jnp.where(head, 0xFFFFF, 0xFFFF)
    groups = [w & mask for w in groups]
    groups[0] = groups[0] | jnp.where(head, jnp.broadcast_to(total << 20, tile), 0)
    for k in range(64):
        group_ref[8 * k : 8 * k + 8, :] = groups[k]
    for i in range(4):
        block = [group_ref[pl.ds(2 * i + n, 64, stride=8), :] for n in range(2)]
        block = jnp.concatenate(block, axis=0).T
        for j in range(4):
            rows = block[j * tables : (j + 1) * tables, :]
            if i >= 2:
                rows = rows | order_ref[:, (i - 2) * 128 : (i - 1) * 128]
            list_ref[pl.ds(4 * j + i, tables, stride=16), :] = rows


def prep(ids, pool_len):
    return pl.pallas_call(
        prep_body,
        out_shape=pltpu.VMEM((128 * 4, 128), jnp.int32),
        out_specs=pl.BlockSpec(memory_space=pltpu.VMEM),
        in_specs=[pl.BlockSpec(memory_space=pltpu.VMEM), pl.BlockSpec(memory_space=pltpu.SMEM)],
        scratch_shapes=[pltpu.VMEM((ids.shape[0], 4 * CHUNK), jnp.int32), pltpu.VMEM((SLOTS, 128), jnp.int32)],
        name="bag_lists",
    )(ids, pool_len)


def gather_body(y_ref, lists_ref, *refs, unroll, widen, first, ahead):
    if widen:
        table_ref, out_ref, tab, tbuf, tsem, smem, acc, lsem = refs
    else:
        tab, out_ref, smem, acc, lsem = refs
    quarter = (y_ref[0] + ahead) & 3
    planes = out_ref.shape[0] // 2
    piece = 2 * SLOTS

    def list_copy(m, slot):
        start = pl.multiple_of((4 * (first + m) + quarter) * piece, piece)
        return pltpu.make_async_copy(
            lists_ref.at[pl.ds(start, piece)], smem.at[pl.ds(slot * piece, piece)], lsem.at[slot]
        )

    if widen:

        def table_copy(b):
            slot = b % TSLOTS
            return pltpu.make_async_copy(
                table_ref.at[pl.ds(b * TBLK, TBLK)], tbuf.at[slot], tsem.at[slot]
            )

        blocks = ROWS_DEV // TBLK
        for b in range(TSLOTS):
            table_copy(b).start()
    for slot in range(LSLOTS):
        list_copy(slot, slot).start()
    if widen:
        tab[pl.ds(ROWS_DEV, 8), :] = jnp.zeros((8, E), jnp.float32)
        for b in range(blocks):
            table_copy(b).wait()
            tab[pl.ds(b * TBLK, TBLK), :] = tbuf[b % TSLOTS].astype(jnp.float32)
            if b + TSLOTS < blocks:
                table_copy(b + TSLOTS).start()

    def chunk(slot, h, c):
        at = slot * piece + h * SLOTS
        words = [smem.at[pl.ds(at + 64 * i, 64)] for i in range(8)]
        acc[...] = jnp.zeros(acc.shape, jnp.float32)
        levels = words[0][0] >> 20

        def level(n):
            head = words[0][n]
            rows = [head & 0xFFFF] + [w[n] for w in words[1:]]
            rows = jnp.concatenate([tab[pl.ds(r, 1), :] for r in rows], axis=0)
            return pl.multiple_of((head >> 13) & 0x78, 8), rows

        def step(k, carry):
            for g, rows in [level(k * unroll + u) for u in range(unroll)]:
                acc[pl.ds(g, 8), :] += rows
            return carry

        lax.fori_loop(0, (levels + unroll - 1) >> (unroll.bit_length() - 1), step, 0)
        out_ref[c] = acc[pl.ds(0, CHUNK), :].astype(jnp.bfloat16)

    def round_of(n, carry):
        for slot in range(LSLOTS):
            m = n * LSLOTS + slot
            list_copy(m, slot).wait()
            for h in range(2):
                chunk(slot, h, 2 * m + h)

            @pl.when(m + LSLOTS < planes)
            def _():
                list_copy(m + LSLOTS, slot).start()

        return carry

    lax.fori_loop(0, planes // LSLOTS, round_of, 0)


def gather(y, ahead, lists, table, planes, first=0, unroll=4, widen=False):
    vmem = pl.BlockSpec(memory_space=pltpu.VMEM)
    sums = pltpu.VMEM((2 * planes, CHUNK, E), jnp.bfloat16)
    scratch = [
        pltpu.SMEM((LSLOTS * 2 * SLOTS,), jnp.int32),
        pltpu.VMEM((CHUNK + 8, E), jnp.float32),
        pltpu.SemaphoreType.DMA((LSLOTS,)),
    ]
    if widen:
        table = pltpu.with_memory_space_constraint(table, pltpu.HBM)
        scratch = [pltpu.VMEM((TSLOTS, TBLK, E), jnp.bfloat16), pltpu.SemaphoreType.DMA((TSLOTS,))] + scratch
    return pl.pallas_call(
        functools.partial(gather_body, unroll=unroll, widen=widen, first=first, ahead=ahead),
        out_shape=(sums, pltpu.VMEM((ROWS_DEV + 8, E), jnp.float32)) if widen else sums,
        in_specs=[
            pl.BlockSpec(memory_space=pltpu.SMEM),
            pl.BlockSpec(memory_space=pl.ANY),
            pl.BlockSpec(memory_space=pltpu.HBM) if widen else vmem,
        ],
        out_specs=(vmem, vmem) if widen else vmem,
        scratch_shapes=scratch,
        compiler_params=pltpu.CompilerParams(vmem_limit_bytes=(6 if widen else 4) * 2**20),
        name="bag_gather",
    )(y, lists, table)


def combine_body(y_ref, lists_ref, part_0, part_1, part_2, part_3, part_3b, out_ref):
    y = y_ref[0]
    parts = (part_0, part_1, part_2)
    half = part_3.shape[0]
    bag = lax.broadcasted_iota(jnp.int32, (CHUNK, 4 * CHUNK), 0)
    for c in range(out_ref.shape[0]):
        source = 8 * (c // 2) + 2 * y + c % 2
        words = lax.shift_right_logical(lists_ref[source], 20) & (CHUNK - 1)
        where = jnp.concatenate([words[2:3, :], words[3:4, :]], axis=1)
        pick = (bag == where).astype(jnp.float32).astype(jnp.bfloat16)
        rows = []
        for j in range(4):
            came = (y - j) & 3
            row = part_3[c] if c < half else part_3b[c - half]
            for k in range(3):
                row = jnp.where(came == k, parts[k][c], row)
            rows.append(row)
        total = jnp.dot(pick, jnp.concatenate(rows, axis=0), preferred_element_type=jnp.float32)
        out_ref[c] = total.astype(jnp.bfloat16)


def combine(y, lists, parts):
    vmem = pl.BlockSpec(memory_space=pltpu.VMEM)
    return pl.pallas_call(
        combine_body,
        out_shape=pltpu.VMEM(parts[0].shape, jnp.bfloat16),
        in_specs=[pl.BlockSpec(memory_space=pltpu.SMEM)] + [vmem] * (1 + len(parts)),
        out_specs=vmem,
        compiler_params=pltpu.CompilerParams(vmem_limit_bytes=4 * 2**20),
        name="bag_combine",
    )(y, lists, *[pltpu.with_memory_space_constraint(p, pltpu.VMEM) for p in parts])


def rows_body(pooled_ref, out_ref):
    for t in range(pooled_ref.shape[0]):
        out_ref[:, t * E : (t + 1) * E] = pooled_ref[t]


def feature_rows(pooled):
    tables, samples, _ = pooled.shape
    vmem = pl.BlockSpec(memory_space=pltpu.VMEM)
    return pl.pallas_call(
        rows_body,
        out_shape=pltpu.VMEM((samples, tables * E), jnp.bfloat16),
        in_specs=[vmem],
        out_specs=vmem,
        compiler_params=pltpu.CompilerParams(vmem_limit_bytes=2 * 2**20),
        name="feature_rows",
    )(pltpu.with_memory_space_constraint(pooled, pltpu.VMEM))


def dense_body(both_ref, w_ref, bias_ref, scale_ref, *refs, stream):
    if stream:
        out_ref, kept, acc, sem = refs
        blocks = [pl.ds(b * WBLK, WBLK) for b in range(kept.shape[0] // WBLK)]
        copies = [pltpu.make_async_copy(w_ref.at[b], kept.at[b], sem.at[i]) for i, b in enumerate(blocks)]
        for copy in copies:
            copy.start()
    else:
        out_ref, acc = refs
        kept = w_ref
        blocks = [pl.ds(b * WBLK, WBLK) for b in range(kept.shape[0] // WBLK)]
    wide = both_ref.shape[2]
    for i, block in enumerate(blocks):
        if stream:
            copies[i].wait()
        at = i * WBLK
        x = both_ref[at // wide, :, at % wide : at % wide + WBLK]
        prod = jnp.dot(x, kept[block, :], preferred_element_type=jnp.float32)
        acc[...] = prod if i == 0 else acc[...] + prod
    part = jnp.maximum(acc[...] + bias_ref[...], 0.0) * scale_ref[...]
    lanes = sum(part[:, 128 * i : 128 * i + 128] for i in range(part.shape[1] // 128))
    out_ref[...] = jnp.sum(lanes.T, axis=0, keepdims=True)


def dense(both, weights, bias, scale, stream):
    vmem = pl.BlockSpec(memory_space=pltpu.VMEM)
    samples = both.shape[1]
    rows, units = weights.shape
    out = pltpu.VMEM((1, samples), jnp.float32)
    scratch = [pltpu.VMEM((samples, units), jnp.float32)]
    if stream:
        weights = pltpu.with_memory_space_constraint(weights, pltpu.HBM)
        scratch.append(pltpu.SemaphoreType.DMA((rows // WBLK,)))
    return pl.pallas_call(
        functools.partial(dense_body, stream=stream),
        out_shape=(out, pltpu.VMEM(weights.shape, weights.dtype)) if stream else out,
        in_specs=[vmem, pl.BlockSpec(memory_space=pltpu.HBM) if stream else vmem, vmem, vmem],
        out_specs=(vmem, vmem) if stream else vmem,
        scratch_shapes=scratch,
        compiler_params=pltpu.CompilerParams(vmem_limit_bytes=8 * 2**20),
        name="dense_near" if stream else "dense_far",
    )(pltpu.with_memory_space_constraint(both, pltpu.VMEM), weights, bias, scale)


def swap(x, axis):
    return lax.all_to_all(jnp.broadcast_to(x[None], (2, *x.shape)), axis, 0, 0, tiled=True)


def body(indices, pool_len, tables, w_first, b_first, w_out):
    n_dev = lax.axis_size("dev")
    n_sec = lax.axis_size("section")
    dev = lax.axis_index("dev")
    lists = prep(jnp.transpose(indices, (1, 2, 0)), pool_len)
    ring = 4
    rows, cols = w_first.shape
    part = cols // HID_SPLIT
    planes = n_dev // ring
    levels = [[ring * p + y for p in range(planes)] for y in range(ring)]
    y = dev % ring
    q = dev % HID_SPLIT
    keep = lax.dynamic_slice(w_first, (0, q * part), (rows, part))
    give = lax.dynamic_slice(w_first, (0, (1 - q) * part), (rows, part))

    def along(x, k):
        return lax.ppermute(x, "dev", [(d, d // ring * ring + (d + k) % ring) for d in range(n_dev)])

    pieces = [keep, along(give, 1), along(keep, 2), along(give, 3)]
    pieces = jnp.stack(pieces)
    pieces = [lax.dynamic_index_in_dim(pieces, (y - k) % ring, 0, False) for k in range(ring)]
    whole = lax.all_gather(jnp.concatenate(pieces), "dev", axis_index_groups=levels, tiled=True)
    both_axes = ("section", "dev")
    arrived = lax.all_to_all(lists.reshape(n_sec * n_dev, 4, 128), both_axes, 0, 0, tiled=True)
    line = lax.broadcasted_iota(jnp.int32, arrived.shape, 1)
    clean = jnp.where(line < 2, arrived, arrived & 0xFFFFF).reshape(-1)
    clean, tables = lax.optimization_barrier((clean, tables))
    here = y.reshape(1)
    split = planes // 2
    parts, tab = {}, None
    for name, k, first, count in CALLS:
        first, count = first * split, count * split
        if tab is None:
            sums, tab = gather(here, k, clean, tables, count, first, widen=True)
        else:
            sums = gather(here, k, clean, tab, count, first)
        parts[name] = along(sums, k) if k else sums
    pooled = combine(here, arrived, [parts[name] for name in "abcde"])
    pooled = pooled.reshape(planes, 2 * CHUNK, E)
    pooled = lax.all_to_all(pooled, "dev", 0, 0, axis_index_groups=levels, tiled=True)
    features = feature_rows(pooled)
    bias = lax.dynamic_slice(b_first, (q * part,), (part,)).astype(jnp.float32)
    scale = lax.dynamic_slice(w_out, (q * part,), (part,)).astype(jnp.float32)
    far = lax.ppermute(features, "dev", [(d, d ^ 1) for d in range(n_dev)])
    bias, scale = bias.reshape(1, part), scale.reshape(1, part)
    near, kept = dense(swap(features, "section"), whole, bias, scale, True)
    near = lax.all_gather(near.reshape(-1), "section")
    far, near = lax.optimization_barrier((far, near))
    far_part = dense(swap(far, "section"), kept, bias, scale, False).reshape(-1)
    far_part, near = lax.optimization_barrier((far_part, near))

    def to_partner(x, turn):
        pairs = [(s * n_dev + d, (s ^ turn) * n_dev + (d ^ 1)) for s in range(n_sec) for d in range(n_dev)]
        return lax.ppermute(x, both_axes, pairs)

    return (near[0] + near[1]) + (to_partner(far_part, 0) + to_partner(far_part, 1))


def solution(mesh):
    placed = (
        P(("section", "dev"), None, None),
        P(),
        P(("section", "dev"), None),
        P("dev", "section"),
        P("section"),
        P("section"),
    )
    return jax.shard_map(body, mesh=mesh, in_specs=placed, out_specs=P("dev"), check_vma=False)
```

```python
import functools

import jax
import jax.numpy as jnp
from jax import lax
from jax.experimental import pallas as pl
from jax.experimental.pallas import tpu as pltpu
from jax.sharding import PartitionSpec as P


E = 128
ROWS_DEV = 32768
POOL = 8
CHUNK = 64
SLOTS = POOL * CHUNK
DEAD = ROWS_DEV | (8 << 16)
TBLK = 2048
TSLOTS = 4
LSLOTS = 4
HID_SPLIT = 2
WBLK = 512
CALLS = (("c", 2, 0, 2), ("b", 1, 0, 2), ("d", 3, 0, 1), ("e", 3, 1, 1), ("a", 0, 0, 2))
SORT8 = (
    (0, 2), (1, 3), (4, 6), (5, 7), (0, 4), (1, 5), (2, 6), (3, 7), (0, 1), (2, 3),
    (4, 5), (6, 7), (2, 4), (3, 5), (1, 4), (3, 6), (1, 2), (3, 4), (5, 6),
)


def prep_body(x_ref, pool_ref, list_ref, order_ref, group_ref):
    shape = (CHUNK, 128)
    tables = x_ref.shape[0]
    lane = lax.broadcasted_iota(jnp.int32, shape, 1)
    bag = lax.broadcasted_iota(jnp.int32, shape, 0)
    table = lax.broadcasted_iota(jnp.int32, (8, 128), 1) & (tables - 1)
    live = jnp.zeros((8, 128), jnp.int32)
    for t in range(tables):
        live = jnp.where(table == t, pool_ref[t], live)
    live = jnp.concatenate([live] * (CHUNK // 8), axis=0)
    first = (lane // tables) * ROWS_DEV
    v = []
    for p in range(POOL):
        row = jnp.concatenate([x_ref[:, p, :]] * 4, axis=0).T - first
        ok = (row >= 0) & (row < ROWS_DEV) & (live > p)
        v.append(jnp.where(ok, row, ROWS_DEV))
    for a, b in SORT8:
        v[a], v[b] = jnp.minimum(v[a], v[b]), jnp.maximum(v[a], v[b])
    kept = sum((w < ROWS_DEV).astype(jnp.int32) for w in v)
    cols = [(POOL - kept) * CHUNK + bag]
    cols += [v[2 * k] | (v[2 * k + 1] << 16) for k in range(POOL // 2)]
    size = 2
    while size <= CHUNK:
        step = size // 2
        while step:
            upper = (bag & step) != 0
            small = ((bag & size) == 0) != upper
            other = [
                jnp.where(upper, pltpu.roll(c, step, 0), pltpu.roll(c, CHUNK - step, 0)) for c in cols
            ]
            take = jnp.where(small, other[0] - cols[0], cols[0] - other[0]) < 0
            cols = [jnp.where(take, o, c) for o, c in zip(other, cols)]
            step //= 2
        size *= 2
    key = cols[0]
    order = (((key & (CHUNK - 1)) | CHUNK) << 20).T
    for j in range(4):
        order_ref[:, j * CHUNK : (j + 1) * CHUNK] = order[j * tables : (j + 1) * tables, :]
    kept = POOL - (key >> 6)
    v = []
    for w in cols[1:]:
        v += [w & 0xFFFF, lax.shift_right_logical(w, 16)]
    tile = (8, 128)
    groups = []
    total = jnp.zeros((1, 128), jnp.int32)
    for g in range(CHUNK // 8):
        n = kept[8 * g : 8 * g + 1]
        shift = jnp.broadcast_to((8 * g - total) << 20, tile)
        n_all = jnp.broadcast_to(n, tile)
        for p in range(POOL):
            word = v[p][8 * g : 8 * g + 8] | (g << 16) | shift
            groups.append(jnp.where(n_all > p, word, DEAD))
        total = total + n
    for k in range(6):
        gap = 1 << k
        moves = [((w >> (20 + k)) & 1) != 0 for w in groups]
        new = []
        for i in range(64):
            stay = jnp.where(moves[i], DEAD, groups[i])
            if i + gap < 64:
                stay = jnp.where(moves[i + gap], groups[i + gap], stay)
            new.append(stay)
        groups = new
    head = lax.broadcasted_iota(jnp.int32, tile, 0) == 0
    mask = jnp.where(head, 0xFFFFF, 0xFFFF)
    groups = [w & mask for w in groups]
    groups[0] = groups[0] | jnp.where(head, jnp.broadcast_to(total << 20, tile), 0)
    for k in range(64):
        group_ref[8 * k : 8 * k + 8, :] = groups[k]
    for i in range(4):
        block = [group_ref[pl.ds(2 * i + n, 64, stride=8), :] for n in range(2)]
        block = jnp.concatenate(block, axis=0).T
        for j in range(4):
            rows = block[j * tables : (j + 1) * tables, :]
            if i >= 2:
                rows = rows | order_ref[:, (i - 2) * 128 : (i - 1) * 128]
            list_ref[pl.ds(4 * j + i, tables, stride=16), :] = rows


def prep(ids, pool_len):
    return pl.pallas_call(
        prep_body,
        out_shape=pltpu.VMEM((128 * 4, 128), jnp.int32),
        out_specs=pl.BlockSpec(memory_space=pltpu.VMEM),
        in_specs=[pl.BlockSpec(memory_space=pltpu.VMEM), pl.BlockSpec(memory_space=pltpu.SMEM)],
        scratch_shapes=[pltpu.VMEM((ids.shape[0], 4 * CHUNK), jnp.int32), pltpu.VMEM((SLOTS, 128), jnp.int32)],
        name="bag_lists",
    )(ids, pool_len)


def gather_body(y_ref, lists_ref, *refs, unroll, widen, first, ahead):
    if widen:
        table_ref, out_ref, tab, tbuf, tsem, smem, acc, lsem = refs
    else:
        tab, out_ref, smem, acc, lsem = refs
    quarter = (y_ref[0] + ahead) & 3
    planes = out_ref.shape[0] // 2
    piece = 2 * SLOTS

    def list_copy(m, slot):
        start = pl.multiple_of((4 * (first + m) + quarter) * piece, piece)
        return pltpu.make_async_copy(
            lists_ref.at[pl.ds(start, piece)], smem.at[pl.ds(slot * piece, piece)], lsem.at[slot]
        )

    if widen:

        def table_copy(b):
            slot = b % TSLOTS
            return pltpu.make_async_copy(
                table_ref.at[pl.ds(b * TBLK, TBLK)], tbuf.at[slot], tsem.at[slot]
            )

        blocks = ROWS_DEV // TBLK
        for b in range(TSLOTS):
            table_copy(b).start()
    for slot in range(LSLOTS):
        list_copy(slot, slot).start()
    if widen:
        tab[pl.ds(ROWS_DEV, 8), :] = jnp.zeros((8, E), jnp.float32)
        for b in range(blocks):
            table_copy(b).wait()
            tab[pl.ds(b * TBLK, TBLK), :] = tbuf[b % TSLOTS].astype(jnp.float32)
            if b + TSLOTS < blocks:
                table_copy(b + TSLOTS).start()

    def chunk(slot, h, c):
        at = slot * piece + h * SLOTS
        words = [smem.at[pl.ds(at + 64 * i, 64)] for i in range(8)]
        acc[...] = jnp.zeros(acc.shape, jnp.float32)
        levels = words[0][0] >> 20

        def level(n):
            head = words[0][n]
            rows = [head & 0xFFFF] + [w[n] for w in words[1:]]
            rows = jnp.concatenate([tab[pl.ds(r, 1), :] for r in rows], axis=0)
            return pl.multiple_of((head >> 13) & 0x78, 8), rows

        def step(k, carry):
            for g, rows in [level(k * unroll + u) for u in range(unroll)]:
                acc[pl.ds(g, 8), :] += rows
            return carry

        lax.fori_loop(0, (levels + unroll - 1) >> (unroll.bit_length() - 1), step, 0)
        out_ref[c] = acc[pl.ds(0, CHUNK), :].astype(jnp.bfloat16)

    def round_of(n, carry):
        for slot in range(LSLOTS):
            m = n * LSLOTS + slot
            list_copy(m, slot).wait()
            for h in range(2):
                chunk(slot, h, 2 * m + h)

            @pl.when(m + LSLOTS < planes)
            def _():
                list_copy(m + LSLOTS, slot).start()

        return carry

    lax.fori_loop(0, planes // LSLOTS, round_of, 0)


def gather(y, ahead, lists, table, planes, first=0, unroll=4, widen=False):
    vmem = pl.BlockSpec(memory_space=pltpu.VMEM)
    sums = pltpu.VMEM((2 * planes, CHUNK, E), jnp.bfloat16)
    scratch = [
        pltpu.SMEM((LSLOTS * 2 * SLOTS,), jnp.int32),
        pltpu.VMEM((CHUNK + 8, E), jnp.float32),
        pltpu.SemaphoreType.DMA((LSLOTS,)),
    ]
    if widen:
        table = pltpu.with_memory_space_constraint(table, pltpu.HBM)
        scratch = [pltpu.VMEM((TSLOTS, TBLK, E), jnp.bfloat16), pltpu.SemaphoreType.DMA((TSLOTS,))] + scratch
    return pl.pallas_call(
        functools.partial(gather_body, unroll=unroll, widen=widen, first=first, ahead=ahead),
        out_shape=(sums, pltpu.VMEM((ROWS_DEV + 8, E), jnp.float32)) if widen else sums,
        in_specs=[
            pl.BlockSpec(memory_space=pltpu.SMEM),
            pl.BlockSpec(memory_space=pl.ANY),
            pl.BlockSpec(memory_space=pltpu.HBM) if widen else vmem,
        ],
        out_specs=(vmem, vmem) if widen else vmem,
        scratch_shapes=scratch,
        compiler_params=pltpu.CompilerParams(vmem_limit_bytes=(6 if widen else 4) * 2**20),
        name="bag_gather",
    )(y, lists, table)


def combine_body(y_ref, lists_ref, part_0, part_1, part_2, part_3, part_3b, out_ref):
    y = y_ref[0]
    parts = (part_0, part_1, part_2)
    half = part_3.shape[0]
    bag = lax.broadcasted_iota(jnp.int32, (CHUNK, 4 * CHUNK), 0)
    for c in range(out_ref.shape[0]):
        source = 8 * (c // 2) + 2 * y + c % 2
        words = lax.shift_right_logical(lists_ref[source], 20) & (CHUNK - 1)
        where = jnp.concatenate([words[2:3, :], words[3:4, :]], axis=1)
        pick = (bag == where).astype(jnp.float32).astype(jnp.bfloat16)
        rows = []
        for j in range(4):
            came = (y - j) & 3
            row = part_3[c] if c < half else part_3b[c - half]
            for k in range(3):
                row = jnp.where(came == k, parts[k][c], row)
            rows.append(row)
        total = jnp.dot(pick, jnp.concatenate(rows, axis=0), preferred_element_type=jnp.float32)
        out_ref[c] = total.astype(jnp.bfloat16)


def combine(y, lists, parts):
    vmem = pl.BlockSpec(memory_space=pltpu.VMEM)
    return pl.pallas_call(
        combine_body,
        out_shape=pltpu.VMEM(parts[0].shape, jnp.bfloat16),
        in_specs=[pl.BlockSpec(memory_space=pltpu.SMEM)] + [vmem] * (1 + len(parts)),
        out_specs=vmem,
        compiler_params=pltpu.CompilerParams(vmem_limit_bytes=4 * 2**20),
        name="bag_combine",
    )(y, lists, *[pltpu.with_memory_space_constraint(p, pltpu.VMEM) for p in parts])


def rows_body(pooled_ref, out_ref):
    for t in range(pooled_ref.shape[0]):
        out_ref[:, t * E : (t + 1) * E] = pooled_ref[t]


def feature_rows(pooled):
    tables, samples, _ = pooled.shape
    vmem = pl.BlockSpec(memory_space=pltpu.VMEM)
    return pl.pallas_call(
        rows_body,
        out_shape=pltpu.VMEM((samples, tables * E), jnp.bfloat16),
        in_specs=[vmem],
        out_specs=vmem,
        compiler_params=pltpu.CompilerParams(vmem_limit_bytes=2 * 2**20),
        name="feature_rows",
    )(pltpu.with_memory_space_constraint(pooled, pltpu.VMEM))


def dense_body(both_ref, w_ref, bias_ref, scale_ref, *refs, stream):
    if stream:
        out_ref, kept, acc, sem = refs
        blocks = [pl.ds(b * WBLK, WBLK) for b in range(kept.shape[0] // WBLK)]
        copies = [pltpu.make_async_copy(w_ref.at[b], kept.at[b], sem.at[i]) for i, b in enumerate(blocks)]
        for copy in copies:
            copy.start()
    else:
        out_ref, acc = refs
        kept = w_ref
        blocks = [pl.ds(b * WBLK, WBLK) for b in range(kept.shape[0] // WBLK)]
    wide = both_ref.shape[2]
    for i, block in enumerate(blocks):
        if stream:
            copies[i].wait()
        at = i * WBLK
        x = both_ref[at // wide, :, at % wide : at % wide + WBLK]
        prod = jnp.dot(x, kept[block, :], preferred_element_type=jnp.float32)
        acc[...] = prod if i == 0 else acc[...] + prod
    part = jnp.maximum(acc[...] + bias_ref[...], 0.0) * scale_ref[...]
    lanes = sum(part[:, 128 * i : 128 * i + 128] for i in range(part.shape[1] // 128))
    out_ref[...] = jnp.sum(lanes.T, axis=0, keepdims=True)


def dense(both, weights, bias, scale, stream):
    vmem = pl.BlockSpec(memory_space=pltpu.VMEM)
    samples = both.shape[1]
    rows, units = weights.shape
    out = pltpu.VMEM((1, samples), jnp.float32)
    scratch = [pltpu.VMEM((samples, units), jnp.float32)]
    if stream:
        weights = pltpu.with_memory_space_constraint(weights, pltpu.HBM)
        scratch.append(pltpu.SemaphoreType.DMA((rows // WBLK,)))
    return pl.pallas_call(
        functools.partial(dense_body, stream=stream),
        out_shape=(out, pltpu.VMEM(weights.shape, weights.dtype)) if stream else out,
        in_specs=[vmem, pl.BlockSpec(memory_space=pltpu.HBM) if stream else vmem, vmem, vmem],
        out_specs=(vmem, vmem) if stream else vmem,
        scratch_shapes=scratch,
        compiler_params=pltpu.CompilerParams(vmem_limit_bytes=8 * 2**20),
        name="dense_near" if stream else "dense_far",
    )(pltpu.with_memory_space_constraint(both, pltpu.VMEM), weights, bias, scale)


def swap(x, axis):
    return lax.all_to_all(jnp.broadcast_to(x[None], (2, *x.shape)), axis, 0, 0, tiled=True)


def body(indices, pool_len, tables, w_first, b_first, w_out):
    n_dev = lax.axis_size("dev")
    n_sec = lax.axis_size("section")
    dev = lax.axis_index("dev")
    lists = prep(jnp.transpose(indices, (1, 2, 0)), pool_len)
    ring = 4
    rows, cols = w_first.shape
    part = cols // HID_SPLIT
    planes = n_dev // ring
    levels = [[ring * p + y for p in range(planes)] for y in range(ring)]
    y = dev % ring
    q = dev % HID_SPLIT
    keep = lax.dynamic_slice(w_first, (0, q * part), (rows, part))
    give = lax.dynamic_slice(w_first, (0, (1 - q) * part), (rows, part))

    def along(x, k):
        return lax.ppermute(x, "dev", [(d, d // ring * ring + (d + k) % ring) for d in range(n_dev)])

    pieces = [keep, along(give, 1), along(keep, 2), along(give, 3)]
    pieces, lists = lax.optimization_barrier((pieces, lists))
    pieces = jnp.stack(pieces)
    pieces = [lax.dynamic_index_in_dim(pieces, (y - k) % ring, 0, False) for k in range(ring)]
    whole = lax.all_gather(jnp.concatenate(pieces), "dev", axis_index_groups=levels, tiled=True)
    both_axes = ("section", "dev")
    arrived = lax.all_to_all(lists.reshape(n_sec * n_dev, 4, 128), both_axes, 0, 0, tiled=True)
    line = lax.broadcasted_iota(jnp.int32, arrived.shape, 1)
    clean = jnp.where(line < 2, arrived, arrived & 0xFFFFF).reshape(-1)
    clean, tables = lax.optimization_barrier((clean, tables))
    here = y.reshape(1)
    split = planes // 2
    parts, tab = {}, None
    for name, k, first, count in CALLS:
        first, count = first * split, count * split
        if tab is None:
            sums, tab = gather(here, k, clean, tables, count, first, widen=True)
        else:
            sums = gather(here, k, clean, tab, count, first)
        parts[name] = along(sums, k) if k else sums
    pooled = combine(here, arrived, [parts[name] for name in "abcde"])
    pooled = pooled.reshape(planes, 2 * CHUNK, E)
    pooled = lax.all_to_all(pooled, "dev", 0, 0, axis_index_groups=levels, tiled=True)
    features = feature_rows(pooled)
    bias = lax.dynamic_slice(b_first, (q * part,), (part,)).astype(jnp.float32)
    scale = lax.dynamic_slice(w_out, (q * part,), (part,)).astype(jnp.float32)
    far = lax.ppermute(features, "dev", [(d, d ^ 1) for d in range(n_dev)])
    bias, scale = bias.reshape(1, part), scale.reshape(1, part)
    near, kept = dense(swap(features, "section"), whole, bias, scale, True)
    near = near.reshape(-1)
    far, near = lax.optimization_barrier((far, near))
    far_part = dense(swap(far, "section"), kept, bias, scale, False).reshape(-1)

    def moved(x, core, chip):
        pairs = [(s * n_dev + d, (s ^ core) * n_dev + (d ^ chip)) for s in range(n_sec) for d in range(n_dev)]
        return lax.ppermute(x, both_axes, pairs)

    return (near + moved(near, 1, 0)) + (moved(far_part, 0, 1) + moved(far_part, 1, 1))


def solution(mesh):
    placed = (
        P(("section", "dev"), None, None),
        P(),
        P(("section", "dev"), None),
        P("dev", "section"),
        P("section"),
        P("section"),
    )
    return jax.shard_map(body, mesh=mesh, in_specs=placed, out_specs=P("dev"), check_vma=False)
```

```python
import functools

import jax
import jax.numpy as jnp
from jax import lax
from jax.experimental import pallas as pl
from jax.experimental.pallas import tpu as pltpu
from jax.sharding import PartitionSpec as P


E = 128
ROWS_DEV = 32768
POOL = 8
CHUNK = 64
SLOTS = POOL * CHUNK
DEAD = ROWS_DEV | (8 << 16)
TBLK = 4096
TSLOTS = 4
LSLOTS = 4
HID_SPLIT = 2
WBLK = 512
CALLS = (("c", 2, 0, 2), ("b", 1, 0, 2), ("d", 3, 0, 1), ("e", 3, 1, 1), ("a", 0, 0, 2))
SORT8 = (
    (0, 2), (1, 3), (4, 6), (5, 7), (0, 4), (1, 5), (2, 6), (3, 7), (0, 1), (2, 3),
    (4, 5), (6, 7), (2, 4), (3, 5), (1, 4), (3, 6), (1, 2), (3, 4), (5, 6),
)


def prep_body(x_ref, pool_ref, list_ref, order_ref, group_ref):
    shape = (CHUNK, 128)
    tables = x_ref.shape[0]
    lane = lax.broadcasted_iota(jnp.int32, shape, 1)
    bag = lax.broadcasted_iota(jnp.int32, shape, 0)
    table = lax.broadcasted_iota(jnp.int32, (8, 128), 1) & (tables - 1)
    live = jnp.zeros((8, 128), jnp.int32)
    for t in range(tables):
        live = jnp.where(table == t, pool_ref[t], live)
    live = jnp.concatenate([live] * (CHUNK // 8), axis=0)
    first = (lane // tables) * ROWS_DEV
    v = []
    for p in range(POOL):
        row = jnp.concatenate([x_ref[:, p, :]] * 4, axis=0).T - first
        ok = (row >= 0) & (row < ROWS_DEV) & (live > p)
        v.append(jnp.where(ok, row, ROWS_DEV))
    for a, b in SORT8:
        v[a], v[b] = jnp.minimum(v[a], v[b]), jnp.maximum(v[a], v[b])
    kept = sum((w < ROWS_DEV).astype(jnp.int32) for w in v)
    cols = [(POOL - kept) * CHUNK + bag]
    cols += [v[2 * k] | (v[2 * k + 1] << 16) for k in range(POOL // 2)]
    size = 2
    while size <= CHUNK:
        step = size // 2
        while step:
            upper = (bag & step) != 0
            small = ((bag & size) == 0) != upper
            other = [
                jnp.where(upper, pltpu.roll(c, step, 0), pltpu.roll(c, CHUNK - step, 0)) for c in cols
            ]
            take = jnp.where(small, other[0] - cols[0], cols[0] - other[0]) < 0
            cols = [jnp.where(take, o, c) for o, c in zip(other, cols)]
            step //= 2
        size *= 2
    key = cols[0]
    order = (((key & (CHUNK - 1)) | CHUNK) << 20).T
    for j in range(4):
        order_ref[:, j * CHUNK : (j + 1) * CHUNK] = order[j * tables : (j + 1) * tables, :]
    kept = POOL - (key >> 6)
    v = []
    for w in cols[1:]:
        v += [w & 0xFFFF, lax.shift_right_logical(w, 16)]
    tile = (8, 128)
    groups = []
    total = jnp.zeros((1, 128), jnp.int32)
    for g in range(CHUNK // 8):
        n = kept[8 * g : 8 * g + 1]
        shift = jnp.broadcast_to((8 * g - total) << 20, tile)
        n_all = jnp.broadcast_to(n, tile)
        for p in range(POOL):
            word = v[p][8 * g : 8 * g + 8] | (g << 16) | shift
            groups.append(jnp.where(n_all > p, word, DEAD))
        total = total + n
    for k in range(6):
        gap = 1 << k
        moves = [((w >> (20 + k)) & 1) != 0 for w in groups]
        new = []
        for i in range(64):
            stay = jnp.where(moves[i], DEAD, groups[i])
            if i + gap < 64:
                stay = jnp.where(moves[i + gap], groups[i + gap], stay)
            new.append(stay)
        groups = new
    head = lax.broadcasted_iota(jnp.int32, tile, 0) == 0
    mask = jnp.where(head, 0xFFFFF, 0xFFFF)
    groups = [w & mask for w in groups]
    groups[0] = groups[0] | jnp.where(head, jnp.broadcast_to(total << 20, tile), 0)
    for k in range(64):
        group_ref[8 * k : 8 * k + 8, :] = groups[k]
    for i in range(4):
        block = [group_ref[pl.ds(2 * i + n, 64, stride=8), :] for n in range(2)]
        block = jnp.concatenate(block, axis=0).T
        for j in range(4):
            rows = block[j * tables : (j + 1) * tables, :]
            if i >= 2:
                rows = rows | order_ref[:, (i - 2) * 128 : (i - 1) * 128]
            list_ref[pl.ds(4 * j + i, tables, stride=16), :] = rows


def prep(ids, pool_len):
    return pl.pallas_call(
        prep_body,
        out_shape=pltpu.VMEM((128 * 4, 128), jnp.int32),
        out_specs=pl.BlockSpec(memory_space=pltpu.VMEM),
        in_specs=[pl.BlockSpec(memory_space=pltpu.VMEM), pl.BlockSpec(memory_space=pltpu.SMEM)],
        scratch_shapes=[pltpu.VMEM((ids.shape[0], 4 * CHUNK), jnp.int32), pltpu.VMEM((SLOTS, 128), jnp.int32)],
        name="bag_lists",
    )(ids, pool_len)


def gather_body(y_ref, lists_ref, *refs, unroll, widen, first, ahead):
    if widen:
        table_ref, out_ref, tab, tbuf, tsem, smem, acc, lsem = refs
    else:
        tab, out_ref, smem, acc, lsem = refs
    quarter = (y_ref[0] + ahead) & 3
    planes = out_ref.shape[0] // 2
    piece = 2 * SLOTS

    def list_copy(m, slot):
        start = pl.multiple_of((4 * (first + m) + quarter) * piece, piece)
        return pltpu.make_async_copy(
            lists_ref.at[pl.ds(start, piece)], smem.at[pl.ds(slot * piece, piece)], lsem.at[slot]
        )

    if widen:

        def table_copy(b):
            slot = b % TSLOTS
            return pltpu.make_async_copy(
                table_ref.at[pl.ds(b * TBLK, TBLK)], tbuf.at[slot], tsem.at[slot]
            )

        blocks = ROWS_DEV // TBLK
        for b in range(TSLOTS):
            table_copy(b).start()
    for slot in range(LSLOTS):
        list_copy(slot, slot).start()
    if widen:
        tab[pl.ds(ROWS_DEV, 8), :] = jnp.zeros((8, E), jnp.float32)
        for b in range(blocks):
            table_copy(b).wait()
            tab[pl.ds(b * TBLK, TBLK), :] = tbuf[b % TSLOTS].astype(jnp.float32)
            if b + TSLOTS < blocks:
                table_copy(b + TSLOTS).start()

    def chunk(slot, h, c):
        at = slot * piece + h * SLOTS
        words = [smem.at[pl.ds(at + 64 * i, 64)] for i in range(8)]
        acc[...] = jnp.zeros(acc.shape, jnp.float32)
        levels = words[0][0] >> 20

        def level(n):
            head = words[0][n]
            rows = [head & 0xFFFF] + [w[n] for w in words[1:]]
            rows = jnp.concatenate([tab[pl.ds(r, 1), :] for r in rows], axis=0)
            return pl.multiple_of((head >> 13) & 0x78, 8), rows

        def step(k, carry):
            for g, rows in [level(k * unroll + u) for u in range(unroll)]:
                acc[pl.ds(g, 8), :] += rows
            return carry

        lax.fori_loop(0, (levels + unroll - 1) >> (unroll.bit_length() - 1), step, 0)
        out_ref[c] = acc[pl.ds(0, CHUNK), :].astype(jnp.bfloat16)

    def round_of(n, carry):
        for slot in range(LSLOTS):
            m = n * LSLOTS + slot
            list_copy(m, slot).wait()
            for h in range(2):
                chunk(slot, h, 2 * m + h)

            @pl.when(m + LSLOTS < planes)
            def _():
                list_copy(m + LSLOTS, slot).start()

        return carry

    lax.fori_loop(0, planes // LSLOTS, round_of, 0)


def gather(y, ahead, lists, table, planes, first=0, unroll=4, widen=False):
    vmem = pl.BlockSpec(memory_space=pltpu.VMEM)
    sums = pltpu.VMEM((2 * planes, CHUNK, E), jnp.bfloat16)
    scratch = [
        pltpu.SMEM((LSLOTS * 2 * SLOTS,), jnp.int32),
        pltpu.VMEM((CHUNK + 8, E), jnp.float32),
        pltpu.SemaphoreType.DMA((LSLOTS,)),
    ]
    if widen:
        table = pltpu.with_memory_space_constraint(table, pltpu.HBM)
        scratch = [pltpu.VMEM((TSLOTS, TBLK, E), jnp.bfloat16), pltpu.SemaphoreType.DMA((TSLOTS,))] + scratch
    return pl.pallas_call(
        functools.partial(gather_body, unroll=unroll, widen=widen, first=first, ahead=ahead),
        out_shape=(sums, pltpu.VMEM((ROWS_DEV + 8, E), jnp.float32)) if widen else sums,
        in_specs=[
            pl.BlockSpec(memory_space=pltpu.SMEM),
            pl.BlockSpec(memory_space=pl.ANY),
            pl.BlockSpec(memory_space=pltpu.HBM) if widen else vmem,
        ],
        out_specs=(vmem, vmem) if widen else vmem,
        scratch_shapes=scratch,
        compiler_params=pltpu.CompilerParams(vmem_limit_bytes=(8 if widen else 4) * 2**20),
        name="bag_gather",
    )(y, lists, table)


def combine_body(y_ref, lists_ref, part_0, part_1, part_2, part_3, part_3b, out_ref):
    y = y_ref[0]
    parts = (part_0, part_1, part_2)
    half = part_3.shape[0]
    bag = lax.broadcasted_iota(jnp.int32, (CHUNK, 4 * CHUNK), 0)
    for c in range(out_ref.shape[0]):
        source = 8 * (c // 2) + 2 * y + c % 2
        words = lax.shift_right_logical(lists_ref[source], 20) & (CHUNK - 1)
        where = jnp.concatenate([words[2:3, :], words[3:4, :]], axis=1)
        pick = (bag == where).astype(jnp.float32).astype(jnp.bfloat16)
        rows = []
        for j in range(4):
            came = (y - j) & 3
            row = part_3[c] if c < half else part_3b[c - half]
            for k in range(3):
                row = jnp.where(came == k, parts[k][c], row)
            rows.append(row)
        total = jnp.dot(pick, jnp.concatenate(rows, axis=0), preferred_element_type=jnp.float32)
        out_ref[c] = total.astype(jnp.bfloat16)


def combine(y, lists, parts):
    vmem = pl.BlockSpec(memory_space=pltpu.VMEM)
    return pl.pallas_call(
        combine_body,
        out_shape=pltpu.VMEM(parts[0].shape, jnp.bfloat16),
        in_specs=[pl.BlockSpec(memory_space=pltpu.SMEM)] + [vmem] * (1 + len(parts)),
        out_specs=vmem,
        compiler_params=pltpu.CompilerParams(vmem_limit_bytes=4 * 2**20),
        name="bag_combine",
    )(y, lists, *[pltpu.with_memory_space_constraint(p, pltpu.VMEM) for p in parts])


def rows_body(pooled_ref, out_ref):
    for t in range(pooled_ref.shape[0]):
        out_ref[:, t * E : (t + 1) * E] = pooled_ref[t]


def feature_rows(pooled):
    tables, samples, _ = pooled.shape
    vmem = pl.BlockSpec(memory_space=pltpu.VMEM)
    return pl.pallas_call(
        rows_body,
        out_shape=pltpu.VMEM((samples, tables * E), jnp.bfloat16),
        in_specs=[vmem],
        out_specs=vmem,
        compiler_params=pltpu.CompilerParams(vmem_limit_bytes=2 * 2**20),
        name="feature_rows",
    )(pltpu.with_memory_space_constraint(pooled, pltpu.VMEM))


def dense_body(both_ref, w_ref, bias_ref, scale_ref, *refs, stream):
    if stream:
        out_ref, kept, acc, sem = refs
        blocks = [pl.ds(b * WBLK, WBLK) for b in range(kept.shape[0] // WBLK)]
        copies = [pltpu.make_async_copy(w_ref.at[b], kept.at[b], sem.at[i]) for i, b in enumerate(blocks)]
        for copy in copies:
            copy.start()
    else:
        out_ref, acc = refs
        kept = w_ref
        blocks = [pl.ds(b * WBLK, WBLK) for b in range(kept.shape[0] // WBLK)]
    wide = both_ref.shape[2]
    for i, block in enumerate(blocks):
        if stream:
            copies[i].wait()
        at = i * WBLK
        x = both_ref[at // wide, :, at % wide : at % wide + WBLK]
        prod = jnp.dot(x, kept[block, :], preferred_element_type=jnp.float32)
        acc[...] = prod if i == 0 else acc[...] + prod
    part = jnp.maximum(acc[...] + bias_ref[...], 0.0) * scale_ref[...]
    lanes = sum(part[:, 128 * i : 128 * i + 128] for i in range(part.shape[1] // 128))
    out_ref[...] = jnp.sum(lanes.T, axis=0, keepdims=True)


def dense(both, weights, bias, scale, stream):
    vmem = pl.BlockSpec(memory_space=pltpu.VMEM)
    samples = both.shape[1]
    rows, units = weights.shape
    out = pltpu.VMEM((1, samples), jnp.float32)
    scratch = [pltpu.VMEM((samples, units), jnp.float32)]
    if stream:
        weights = pltpu.with_memory_space_constraint(weights, pltpu.HBM)
        scratch.append(pltpu.SemaphoreType.DMA((rows // WBLK,)))
    return pl.pallas_call(
        functools.partial(dense_body, stream=stream),
        out_shape=(out, pltpu.VMEM(weights.shape, weights.dtype)) if stream else out,
        in_specs=[vmem, pl.BlockSpec(memory_space=pltpu.HBM) if stream else vmem, vmem, vmem],
        out_specs=(vmem, vmem) if stream else vmem,
        scratch_shapes=scratch,
        compiler_params=pltpu.CompilerParams(vmem_limit_bytes=8 * 2**20),
        name="dense_near" if stream else "dense_far",
    )(pltpu.with_memory_space_constraint(both, pltpu.VMEM), weights, bias, scale)


def swap(x, axis):
    return lax.all_to_all(jnp.broadcast_to(x[None], (2, *x.shape)), axis, 0, 0, tiled=True)


def body(indices, pool_len, tables, w_first, b_first, w_out):
    n_dev = lax.axis_size("dev")
    n_sec = lax.axis_size("section")
    dev = lax.axis_index("dev")
    lists = prep(jnp.transpose(indices, (1, 2, 0)), pool_len)
    ring = 4
    rows, cols = w_first.shape
    part = cols // HID_SPLIT
    planes = n_dev // ring
    levels = [[ring * p + y for p in range(planes)] for y in range(ring)]
    y = dev % ring
    q = dev % HID_SPLIT
    keep = lax.dynamic_slice(w_first, (0, q * part), (rows, part))
    give = lax.dynamic_slice(w_first, (0, (1 - q) * part), (rows, part))

    def along(x, k):
        return lax.ppermute(x, "dev", [(d, d // ring * ring + (d + k) % ring) for d in range(n_dev)])

    pieces = [keep, along(give, 1), along(keep, 2), along(give, 3)]
    pieces, lists = lax.optimization_barrier((pieces, lists))
    pieces = jnp.stack(pieces)
    pieces = [lax.dynamic_index_in_dim(pieces, (y - k) % ring, 0, False) for k in range(ring)]
    whole = lax.all_gather(jnp.concatenate(pieces), "dev", axis_index_groups=levels, tiled=True)
    both_axes = ("section", "dev")
    arrived = lax.all_to_all(lists.reshape(n_sec * n_dev, 4, 128), both_axes, 0, 0, tiled=True)
    line = lax.broadcasted_iota(jnp.int32, arrived.shape, 1)
    clean = jnp.where(line < 2, arrived, arrived & 0xFFFFF).reshape(-1)
    clean, tables = lax.optimization_barrier((clean, tables))
    here = y.reshape(1)
    split = planes // 2
    parts, tab = {}, None
    for name, k, first, count in CALLS:
        first, count = first * split, count * split
        if tab is None:
            sums, tab = gather(here, k, clean, tables, count, first, widen=True)
        else:
            sums = gather(here, k, clean, tab, count, first)
        parts[name] = along(sums, k) if k else sums
    pooled = combine(here, arrived, [parts[name] for name in "abcde"])
    pooled = pooled.reshape(planes, 2 * CHUNK, E)
    pooled = lax.all_to_all(pooled, "dev", 0, 0, axis_index_groups=levels, tiled=True)
    features = feature_rows(pooled)
    bias = lax.dynamic_slice(b_first, (q * part,), (part,)).astype(jnp.float32)
    scale = lax.dynamic_slice(w_out, (q * part,), (part,)).astype(jnp.float32)
    ways = [[d // ring * ring + (d + (1 if d % 2 == h else ring - 1)) % ring for d in range(n_dev)] for h in range(2)]
    far = [
        lax.ppermute(features[h * CHUNK : (h + 1) * CHUNK], "dev", list(enumerate(ways[h]))) for h in range(2)
    ]
    bias, scale = bias.reshape(1, part), scale.reshape(1, part)
    near, kept = dense(swap(features, "section"), whole, bias, scale, True)
    near = near.reshape(-1)

    def moved(x, core, way):
        pairs = [(s * n_dev + d, (s ^ core) * n_dev + way[d]) for s in range(n_sec) for d in range(n_dev)]
        return lax.ppermute(x, both_axes, pairs)

    near_2 = moved(near, 1, range(n_dev))
    far, near, near_2 = lax.optimization_barrier((far, near, near_2))
    far_part = dense(swap(jnp.concatenate(far), "section"), kept, bias, scale, False).reshape(2, CHUNK)
    back = [moved(far_part[h], core, ways[h]) for h in range(2) for core in range(2)]
    return (near + near_2) + jnp.concatenate([back[0] + back[1], back[2] + back[3]])


def solution(mesh):
    placed = (
        P(("section", "dev"), None, None),
        P(),
        P(("section", "dev"), None),
        P("dev", "section"),
        P("section"),
        P("section"),
    )
    return jax.shard_map(body, mesh=mesh, in_specs=placed, out_specs=P("dev"), check_vma=False)
```

```python
import functools

import jax
import jax.numpy as jnp
from jax import lax
from jax.experimental import pallas as pl
from jax.experimental.pallas import tpu as pltpu
from jax.sharding import PartitionSpec as P


E = 128
ROWS_DEV = 32768
POOL = 8
CHUNK = 64
SLOTS = POOL * CHUNK
DEAD = ROWS_DEV | (8 << 16)
TBLK = 4096
TSLOTS = 4
LSLOTS = 4
HID_SPLIT = 2
WBLK = 512
CALLS = (("c", 2, 0, 2), ("b", 1, 0, 2), ("d", 3, 0, 1), ("e", 3, 1, 1), ("a", 0, 0, 2))
SORT8 = (
    (0, 2), (1, 3), (4, 6), (5, 7), (0, 4), (1, 5), (2, 6), (3, 7), (0, 1), (2, 3),
    (4, 5), (6, 7), (2, 4), (3, 5), (1, 4), (3, 6), (1, 2), (3, 4), (5, 6),
)


def prep_body(x_ref, pool_ref, list_ref, order_ref, group_ref):
    shape = (CHUNK, 128)
    tables = x_ref.shape[0]
    lane = lax.broadcasted_iota(jnp.int32, shape, 1)
    bag = lax.broadcasted_iota(jnp.int32, shape, 0)
    table = lax.broadcasted_iota(jnp.int32, (8, 128), 1) & (tables - 1)
    live = jnp.zeros((8, 128), jnp.int32)
    for t in range(tables):
        live = jnp.where(table == t, pool_ref[t], live)
    live = jnp.concatenate([live] * (CHUNK // 8), axis=0)
    first = (lane // tables) * ROWS_DEV
    v = []
    for p in range(POOL):
        row = jnp.concatenate([x_ref[:, p, :]] * 4, axis=0).T - first
        ok = (row >= 0) & (row < ROWS_DEV) & (live > p)
        v.append(jnp.where(ok, row, ROWS_DEV))
    for a, b in SORT8:
        v[a], v[b] = jnp.minimum(v[a], v[b]), jnp.maximum(v[a], v[b])
    kept = sum((w < ROWS_DEV).astype(jnp.int32) for w in v)
    cols = [(POOL - kept) * CHUNK + bag]
    cols += [v[2 * k] | (v[2 * k + 1] << 16) for k in range(POOL // 2)]
    size = 2
    while size <= CHUNK:
        step = size // 2
        while step:
            upper = (bag & step) != 0
            small = ((bag & size) == 0) != upper
            other = [
                jnp.where(upper, pltpu.roll(c, step, 0), pltpu.roll(c, CHUNK - step, 0)) for c in cols
            ]
            take = jnp.where(small, other[0] - cols[0], cols[0] - other[0]) < 0
            cols = [jnp.where(take, o, c) for o, c in zip(other, cols)]
            step //= 2
        size *= 2
    key = cols[0]
    order = (((key & (CHUNK - 1)) | CHUNK) << 20).T
    for j in range(4):
        order_ref[:, j * CHUNK : (j + 1) * CHUNK] = order[j * tables : (j + 1) * tables, :]
    kept = POOL - (key >> 6)
    v = []
    for w in cols[1:]:
        v += [w & 0xFFFF, lax.shift_right_logical(w, 16)]
    tile = (8, 128)
    groups = []
    total = jnp.zeros((1, 128), jnp.int32)
    for g in range(CHUNK // 8):
        n = kept[8 * g : 8 * g + 1]
        shift = jnp.broadcast_to((8 * g - total) << 20, tile)
        n_all = jnp.broadcast_to(n, tile)
        for p in range(POOL):
            word = v[p][8 * g : 8 * g + 8] | (g << 16) | shift
            groups.append(jnp.where(n_all > p, word, DEAD))
        total = total + n
    for k in range(6):
        gap = 1 << k
        moves = [((w >> (20 + k)) & 1) != 0 for w in groups]
        new = []
        for i in range(64):
            stay = jnp.where(moves[i], DEAD, groups[i])
            if i + gap < 64:
                stay = jnp.where(moves[i + gap], groups[i + gap], stay)
            new.append(stay)
        groups = new
    head = lax.broadcasted_iota(jnp.int32, tile, 0) == 0
    mask = jnp.where(head, 0xFFFFF, 0xFFFF)
    groups = [w & mask for w in groups]
    groups[0] = groups[0] | jnp.where(head, jnp.broadcast_to(total << 20, tile), 0)
    for k in range(64):
        group_ref[8 * k : 8 * k + 8, :] = groups[k]
    for i in range(4):
        block = [group_ref[pl.ds(2 * i + n, 64, stride=8), :] for n in range(2)]
        block = jnp.concatenate(block, axis=0).T
        for j in range(4):
            rows = block[j * tables : (j + 1) * tables, :]
            if i >= 2:
                rows = rows | order_ref[:, (i - 2) * 128 : (i - 1) * 128]
            list_ref[pl.ds(4 * j + i, tables, stride=16), :] = rows


def prep(ids, pool_len):
    return pl.pallas_call(
        prep_body,
        out_shape=pltpu.VMEM((128 * 4, 128), jnp.int32),
        out_specs=pl.BlockSpec(memory_space=pltpu.VMEM),
        in_specs=[pl.BlockSpec(memory_space=pltpu.VMEM), pl.BlockSpec(memory_space=pltpu.SMEM)],
        scratch_shapes=[pltpu.VMEM((ids.shape[0], 4 * CHUNK), jnp.int32), pltpu.VMEM((SLOTS, 128), jnp.int32)],
        name="bag_lists",
    )(ids, pool_len)


def gather_body(y_ref, lists_ref, *refs, unroll, widen, first, ahead):
    if widen:
        table_ref, out_ref, tab, tbuf, tsem, smem, acc, lsem = refs
    else:
        tab, out_ref, smem, acc, lsem = refs
    quarter = (y_ref[0] + ahead) & 3
    planes = out_ref.shape[0] // 2
    piece = 2 * SLOTS

    def list_copy(m, slot):
        start = pl.multiple_of((4 * (first + m) + quarter) * piece, piece)
        return pltpu.make_async_copy(
            lists_ref.at[pl.ds(start, piece)], smem.at[pl.ds(slot * piece, piece)], lsem.at[slot]
        )

    if widen:

        def table_copy(b):
            slot = b % TSLOTS
            return pltpu.make_async_copy(
                table_ref.at[pl.ds(b * TBLK, TBLK)], tbuf.at[slot], tsem.at[slot]
            )

        blocks = ROWS_DEV // TBLK
        for b in range(TSLOTS):
            table_copy(b).start()
    for slot in range(LSLOTS):
        list_copy(slot, slot).start()
    if widen:
        tab[pl.ds(ROWS_DEV, 8), :] = jnp.zeros((8, E), jnp.float32)
        for b in range(blocks):
            table_copy(b).wait()
            tab[pl.ds(b * TBLK, TBLK), :] = tbuf[b % TSLOTS].astype(jnp.float32)
            if b + TSLOTS < blocks:
                table_copy(b + TSLOTS).start()

    def chunk(slot, h, c):
        at = slot * piece + h * SLOTS
        words = [smem.at[pl.ds(at + 64 * i, 64)] for i in range(8)]
        acc[...] = jnp.zeros(acc.shape, jnp.float32)
        levels = words[0][0] >> 20

        def level(n):
            head = words[0][n]
            rows = [head & 0xFFFF] + [w[n] for w in words[1:]]
            rows = jnp.concatenate([tab[pl.ds(r, 1), :] for r in rows], axis=0)
            return pl.multiple_of((head >> 13) & 0x78, 8), rows

        def step(k, carry):
            for g, rows in [level(k * unroll + u) for u in range(unroll)]:
                acc[pl.ds(g, 8), :] += rows
            return carry

        lax.fori_loop(0, (levels + unroll - 1) >> (unroll.bit_length() - 1), step, 0)
        out_ref[c] = acc[pl.ds(0, CHUNK), :].astype(jnp.bfloat16)

    def round_of(n, carry):
        for slot in range(LSLOTS):
            m = n * LSLOTS + slot
            list_copy(m, slot).wait()
            for h in range(2):
                chunk(slot, h, 2 * m + h)

            @pl.when(m + LSLOTS < planes)
            def _():
                list_copy(m + LSLOTS, slot).start()

        return carry

    lax.fori_loop(0, planes // LSLOTS, round_of, 0)


def gather(y, ahead, lists, table, planes, first=0, unroll=4, widen=False):
    vmem = pl.BlockSpec(memory_space=pltpu.VMEM)
    sums = pltpu.VMEM((2 * planes, CHUNK, E), jnp.bfloat16)
    scratch = [
        pltpu.SMEM((LSLOTS * 2 * SLOTS,), jnp.int32),
        pltpu.VMEM((CHUNK + 8, E), jnp.float32),
        pltpu.SemaphoreType.DMA((LSLOTS,)),
    ]
    if widen:
        table = pltpu.with_memory_space_constraint(table, pltpu.HBM)
        scratch = [pltpu.VMEM((TSLOTS, TBLK, E), jnp.bfloat16), pltpu.SemaphoreType.DMA((TSLOTS,))] + scratch
    return pl.pallas_call(
        functools.partial(gather_body, unroll=unroll, widen=widen, first=first, ahead=ahead),
        out_shape=(sums, pltpu.VMEM((ROWS_DEV + 8, E), jnp.float32)) if widen else sums,
        in_specs=[
            pl.BlockSpec(memory_space=pltpu.SMEM),
            pl.BlockSpec(memory_space=pl.ANY),
            pl.BlockSpec(memory_space=pltpu.HBM) if widen else vmem,
        ],
        out_specs=(vmem, vmem) if widen else vmem,
        scratch_shapes=scratch,
        compiler_params=pltpu.CompilerParams(vmem_limit_bytes=(8 if widen else 4) * 2**20),
        name="bag_gather",
    )(y, lists, table)


def combine_body(y_ref, lists_ref, part_0, part_1, part_2, part_3, part_3b, out_ref):
    y = y_ref[0]
    parts = (part_0, part_1, part_2)
    half = part_3.shape[0]
    bag = lax.broadcasted_iota(jnp.int32, (CHUNK, 4 * CHUNK), 0)
    for c in range(out_ref.shape[0]):
        source = 8 * (c // 2) + 2 * y + c % 2
        words = lax.shift_right_logical(lists_ref[source], 20) & (CHUNK - 1)
        where = jnp.concatenate([words[2:3, :], words[3:4, :]], axis=1)
        pick = (bag == where).astype(jnp.float32).astype(jnp.bfloat16)
        rows = []
        for j in range(4):
            came = (y - j) & 3
            row = part_3[c] if c < half else part_3b[c - half]
            for k in range(3):
                row = jnp.where(came == k, parts[k][c], row)
            rows.append(row)
        total = jnp.dot(pick, jnp.concatenate(rows, axis=0), preferred_element_type=jnp.float32)
        out_ref[c] = total.astype(jnp.bfloat16)


def combine(y, lists, parts):
    vmem = pl.BlockSpec(memory_space=pltpu.VMEM)
    return pl.pallas_call(
        combine_body,
        out_shape=pltpu.VMEM(parts[0].shape, jnp.bfloat16),
        in_specs=[pl.BlockSpec(memory_space=pltpu.SMEM)] + [vmem] * (1 + len(parts)),
        out_specs=vmem,
        compiler_params=pltpu.CompilerParams(vmem_limit_bytes=4 * 2**20),
        name="bag_combine",
    )(y, lists, *[pltpu.with_memory_space_constraint(p, pltpu.VMEM) for p in parts])


def rows_body(pooled_ref, out_ref):
    for t in range(pooled_ref.shape[0]):
        out_ref[:, t * E : (t + 1) * E] = pooled_ref[t]


def feature_rows(pooled):
    tables, samples, _ = pooled.shape
    vmem = pl.BlockSpec(memory_space=pltpu.VMEM)
    return pl.pallas_call(
        rows_body,
        out_shape=pltpu.VMEM((samples, tables * E), jnp.bfloat16),
        in_specs=[vmem],
        out_specs=vmem,
        compiler_params=pltpu.CompilerParams(vmem_limit_bytes=2 * 2**20),
        name="feature_rows",
    )(pltpu.with_memory_space_constraint(pooled, pltpu.VMEM))


def dense_body(both_ref, w_ref, bias_ref, scale_ref, *refs, stream):
    if stream:
        out_ref, kept, acc, sem = refs
        blocks = [pl.ds(b * WBLK, WBLK) for b in range(kept.shape[0] // WBLK)]
        copies = [pltpu.make_async_copy(w_ref.at[b], kept.at[b], sem.at[i]) for i, b in enumerate(blocks)]
        for copy in copies:
            copy.start()
    else:
        out_ref, acc = refs
        kept = w_ref
        blocks = [pl.ds(b * WBLK, WBLK) for b in range(kept.shape[0] // WBLK)]
    wide = both_ref.shape[2]
    for i, block in enumerate(blocks):
        if stream:
            copies[i].wait()
        at = i * WBLK
        x = both_ref[at // wide, :, at % wide : at % wide + WBLK]
        prod = jnp.dot(x, kept[block, :], preferred_element_type=jnp.float32)
        acc[...] = prod if i == 0 else acc[...] + prod
    part = jnp.maximum(acc[...] + bias_ref[...], 0.0) * scale_ref[...]
    lanes = sum(part[:, 128 * i : 128 * i + 128] for i in range(part.shape[1] // 128))
    out_ref[...] = jnp.sum(lanes.T, axis=0, keepdims=True)


def dense(both, weights, bias, scale, stream):
    vmem = pl.BlockSpec(memory_space=pltpu.VMEM)
    samples = both.shape[1]
    rows, units = weights.shape
    out = pltpu.VMEM((1, samples), jnp.float32)
    scratch = [pltpu.VMEM((samples, units), jnp.float32)]
    if stream:
        weights = pltpu.with_memory_space_constraint(weights, pltpu.HBM)
        scratch.append(pltpu.SemaphoreType.DMA((rows // WBLK,)))
    return pl.pallas_call(
        functools.partial(dense_body, stream=stream),
        out_shape=(out, pltpu.VMEM(weights.shape, weights.dtype)) if stream else out,
        in_specs=[vmem, pl.BlockSpec(memory_space=pltpu.HBM) if stream else vmem, vmem, vmem],
        out_specs=(vmem, vmem) if stream else vmem,
        scratch_shapes=scratch,
        compiler_params=pltpu.CompilerParams(vmem_limit_bytes=8 * 2**20),
        name="dense_near" if stream else "dense_far",
    )(pltpu.with_memory_space_constraint(both, pltpu.VMEM), weights, bias, scale)


def swap(x, axis):
    return lax.all_to_all(jnp.broadcast_to(x[None], (2, *x.shape)), axis, 0, 0, tiled=True)


def body(indices, pool_len, tables, w_first, b_first, w_out):
    n_dev = lax.axis_size("dev")
    n_sec = lax.axis_size("section")
    dev = lax.axis_index("dev")
    lists = prep(jnp.transpose(indices, (1, 2, 0)), pool_len)
    ring = 4
    rows, cols = w_first.shape
    part = cols // HID_SPLIT
    planes = n_dev // ring
    levels = [[ring * p + y for p in range(planes)] for y in range(ring)]
    y = dev % ring
    q = dev % HID_SPLIT
    keep = lax.dynamic_slice(w_first, (0, q * part), (rows, part))
    give = lax.dynamic_slice(w_first, (0, (1 - q) * part), (rows, part))

    def along(x, k):
        return lax.ppermute(x, "dev", [(d, d // ring * ring + (d + k) % ring) for d in range(n_dev)])

    pieces = [keep, along(give, 1), along(keep, 2), along(give, 3)]
    pieces, lists = lax.optimization_barrier((pieces, lists))
    pieces = jnp.stack(pieces)
    pieces = [lax.dynamic_index_in_dim(pieces, (y - k) % ring, 0, False) for k in range(ring)]
    whole = lax.all_gather(jnp.concatenate(pieces), "dev", axis_index_groups=levels, tiled=True)
    both_axes = ("section", "dev")
    arrived = lax.all_to_all(lists.reshape(n_sec * n_dev, 4, 128), both_axes, 0, 0, tiled=True)
    line = lax.broadcasted_iota(jnp.int32, arrived.shape, 1)
    clean = jnp.where(line < 2, arrived, arrived & 0xFFFFF).reshape(-1)
    clean, tables = lax.optimization_barrier((clean, tables))
    here = y.reshape(1)
    split = planes // 2
    parts, tab = {}, None
    for name, k, first, count in CALLS:
        first, count = first * split, count * split
        if tab is None:
            sums, tab = gather(here, k, clean, tables, count, first, widen=True)
        else:
            sums = gather(here, k, clean, tab, count, first)
        parts[name] = along(sums, k) if k else sums
    pooled = combine(here, arrived, [parts[name] for name in "abcde"])
    pooled = pooled.reshape(planes, 2 * CHUNK, E)
    pooled = lax.all_to_all(pooled, "dev", 0, 0, axis_index_groups=levels, tiled=True)
    features = feature_rows(pooled)
    bias = lax.dynamic_slice(b_first, (q * part,), (part,)).astype(jnp.float32)
    scale = lax.dynamic_slice(w_out, (q * part,), (part,)).astype(jnp.float32)
    ways = [[d // ring * ring + (d + (1 if d % 2 == h else ring - 1)) % ring for d in range(n_dev)] for h in range(2)]
    far = [
        lax.ppermute(features[h * CHUNK : (h + 1) * CHUNK], "dev", list(enumerate(ways[h]))) for h in range(2)
    ]
    bias, scale = bias.reshape(1, part), scale.reshape(1, part)
    near, kept = dense(swap(features, "section"), whole, bias, scale, True)
    near = near.reshape(-1)

    def moved(x, core, way):
        pairs = [(s * n_dev + d, (s ^ core) * n_dev + way[d]) for s in range(n_sec) for d in range(n_dev)]
        return lax.ppermute(x, both_axes, pairs)

    far, near = lax.optimization_barrier((far, near))
    near_2 = moved(near, 1, range(n_dev))
    far_part = dense(swap(jnp.concatenate(far), "section"), kept, bias, scale, False).reshape(-1)
    far_part = (far_part + moved(far_part, 1, range(n_dev))).reshape(2, CHUNK)
    return (near + near_2) + jnp.concatenate([moved(far_part[h], 0, ways[h]) for h in range(2)])


def solution(mesh):
    placed = (
        P(("section", "dev"), None, None),
        P(),
        P(("section", "dev"), None),
        P("dev", "section"),
        P("section"),
        P("section"),
    )
    return jax.shard_map(body, mesh=mesh, in_specs=placed, out_specs=P("dev"), check_vma=False)
```

```python
import functools

import jax
import jax.numpy as jnp
from jax import lax
from jax.experimental import pallas as pl
from jax.experimental.pallas import tpu as pltpu
from jax.sharding import PartitionSpec as P


E = 128
ROWS_DEV = 32768
POOL = 8
CHUNK = 64
SLOTS = POOL * CHUNK
DEAD = ROWS_DEV | (8 << 16)
TBLK = 4096
TSLOTS = 4
LSLOTS = 4
HID_SPLIT = 2
WBLK = 512
CALLS = (("c", 2, 0, 2), ("b", 1, 0, 2), ("d", 3, 0, 1), ("e", 3, 1, 1), ("a", 0, 0, 2))
SORT8 = (
    (0, 2), (1, 3), (4, 6), (5, 7), (0, 4), (1, 5), (2, 6), (3, 7), (0, 1), (2, 3),
    (4, 5), (6, 7), (2, 4), (3, 5), (1, 4), (3, 6), (1, 2), (3, 4), (5, 6),
)


def prep_body(x_ref, pool_ref, list_ref, order_ref, group_ref):
    shape = (CHUNK, 128)
    tables = x_ref.shape[0]
    lane = lax.broadcasted_iota(jnp.int32, shape, 1)
    bag = lax.broadcasted_iota(jnp.int32, shape, 0)
    table = lax.broadcasted_iota(jnp.int32, (8, 128), 1) & (tables - 1)
    live = jnp.zeros((8, 128), jnp.int32)
    for t in range(tables):
        live = jnp.where(table == t, pool_ref[t], live)
    live = jnp.concatenate([live] * (CHUNK // 8), axis=0)
    first = (lane // tables) * ROWS_DEV
    v = []
    for p in range(POOL):
        row = jnp.concatenate([x_ref[:, p, :]] * 4, axis=0).T - first
        ok = (row >= 0) & (row < ROWS_DEV) & (live > p)
        v.append(jnp.where(ok, row, ROWS_DEV))
    for a, b in SORT8:
        v[a], v[b] = jnp.minimum(v[a], v[b]), jnp.maximum(v[a], v[b])
    kept = sum((w < ROWS_DEV).astype(jnp.int32) for w in v)
    cols = [(POOL - kept) * CHUNK + bag]
    cols += [v[2 * k] | (v[2 * k + 1] << 16) for k in range(POOL // 2)]
    size = 2
    while size <= CHUNK:
        step = size // 2
        while step:
            upper = (bag & step) != 0
            small = ((bag & size) == 0) != upper
            other = [
                jnp.where(upper, pltpu.roll(c, step, 0), pltpu.roll(c, CHUNK - step, 0)) for c in cols
            ]
            take = jnp.where(small, other[0] - cols[0], cols[0] - other[0]) < 0
            cols = [jnp.where(take, o, c) for o, c in zip(other, cols)]
            step //= 2
        size *= 2
    key = cols[0]
    order = (((key & (CHUNK - 1)) | CHUNK) << 20).T
    for j in range(4):
        order_ref[:, j * CHUNK : (j + 1) * CHUNK] = order[j * tables : (j + 1) * tables, :]
    kept = POOL - (key >> 6)
    v = []
    for w in cols[1:]:
        v += [w & 0xFFFF, lax.shift_right_logical(w, 16)]
    tile = (8, 128)
    groups = []
    total = jnp.zeros((1, 128), jnp.int32)
    for g in range(CHUNK // 8):
        n = kept[8 * g : 8 * g + 1]
        shift = jnp.broadcast_to((8 * g - total) << 20, tile)
        n_all = jnp.broadcast_to(n, tile)
        for p in range(POOL):
            word = v[p][8 * g : 8 * g + 8] | (g << 16) | shift
            groups.append(jnp.where(n_all > p, word, DEAD))
        total = total + n
    for k in range(6):
        gap = 1 << k
        moves = [((w >> (20 + k)) & 1) != 0 for w in groups]
        new = []
        for i in range(64):
            stay = jnp.where(moves[i], DEAD, groups[i])
            if i + gap < 64:
                stay = jnp.where(moves[i + gap], groups[i + gap], stay)
            new.append(stay)
        groups = new
    head = lax.broadcasted_iota(jnp.int32, tile, 0) == 0
    mask = jnp.where(head, 0xFFFFF, 0xFFFF)
    groups = [w & mask for w in groups]
    groups[0] = groups[0] | jnp.where(head, jnp.broadcast_to(total << 20, tile), 0)
    for k in range(64):
        group_ref[8 * k : 8 * k + 8, :] = groups[k]
    for i in range(4):
        block = [group_ref[pl.ds(2 * i + n, 64, stride=8), :] for n in range(2)]
        block = jnp.concatenate(block, axis=0).T
        for j in range(4):
            rows = block[j * tables : (j + 1) * tables, :]
            if i >= 2:
                rows = rows | order_ref[:, (i - 2) * 128 : (i - 1) * 128]
            list_ref[pl.ds(4 * j + i, tables, stride=16), :] = rows


def prep(ids, pool_len):
    return pl.pallas_call(
        prep_body,
        out_shape=pltpu.VMEM((128 * 4, 128), jnp.int32),
        out_specs=pl.BlockSpec(memory_space=pltpu.VMEM),
        in_specs=[pl.BlockSpec(memory_space=pltpu.VMEM), pl.BlockSpec(memory_space=pltpu.SMEM)],
        scratch_shapes=[pltpu.VMEM((ids.shape[0], 4 * CHUNK), jnp.int32), pltpu.VMEM((SLOTS, 128), jnp.int32)],
        name="bag_lists",
    )(ids, pool_len)


def gather_body(y_ref, lists_ref, *refs, unroll, widen, first, ahead):
    if widen:
        table_ref, out_ref, tab, tbuf, tsem, smem, acc, lsem = refs
    else:
        tab, out_ref, smem, acc, lsem = refs
    quarter = (y_ref[0] + ahead) & 3
    planes = out_ref.shape[0] // 2
    piece = 2 * SLOTS

    def list_copy(m, slot):
        start = pl.multiple_of((4 * (first + m) + quarter) * piece, piece)
        return pltpu.make_async_copy(
            lists_ref.at[pl.ds(start, piece)], smem.at[pl.ds(slot * piece, piece)], lsem.at[slot]
        )

    if widen:

        def table_copy(b):
            slot = b % TSLOTS
            return pltpu.make_async_copy(
                table_ref.at[pl.ds(b * TBLK, TBLK)], tbuf.at[slot], tsem.at[slot]
            )

        blocks = ROWS_DEV // TBLK
        for b in range(TSLOTS):
            table_copy(b).start()
    for slot in range(LSLOTS):
        list_copy(slot, slot).start()
    if widen:
        tab[pl.ds(ROWS_DEV, 8), :] = jnp.zeros((8, E), jnp.float32)
        for b in range(blocks):
            table_copy(b).wait()
            tab[pl.ds(b * TBLK, TBLK), :] = tbuf[b % TSLOTS].astype(jnp.float32)
            if b + TSLOTS < blocks:
                table_copy(b + TSLOTS).start()

    def chunk(slot, h, c):
        at = slot * piece + h * SLOTS
        words = [smem.at[pl.ds(at + 64 * i, 64)] for i in range(8)]
        acc[...] = jnp.zeros(acc.shape, jnp.float32)
        levels = words[0][0] >> 20

        def level(n):
            head = words[0][n]
            rows = [head & 0xFFFF] + [w[n] for w in words[1:]]
            rows = jnp.concatenate([tab[pl.ds(r, 1), :] for r in rows], axis=0)
            return pl.multiple_of((head >> 13) & 0x78, 8), rows

        def step(k, carry):
            for g, rows in [level(k * unroll + u) for u in range(unroll)]:
                acc[pl.ds(g, 8), :] += rows
            return carry

        lax.fori_loop(0, (levels + unroll - 1) >> (unroll.bit_length() - 1), step, 0)
        out_ref[c] = acc[pl.ds(0, CHUNK), :].astype(jnp.bfloat16)

    def round_of(n, carry):
        for slot in range(LSLOTS):
            m = n * LSLOTS + slot
            list_copy(m, slot).wait()
            for h in range(2):
                chunk(slot, h, 2 * m + h)

            @pl.when(m + LSLOTS < planes)
            def _():
                list_copy(m + LSLOTS, slot).start()

        return carry

    lax.fori_loop(0, planes // LSLOTS, round_of, 0)


def gather(y, ahead, lists, table, planes, first=0, unroll=4, widen=False):
    vmem = pl.BlockSpec(memory_space=pltpu.VMEM)
    sums = pltpu.VMEM((2 * planes, CHUNK, E), jnp.bfloat16)
    scratch = [
        pltpu.SMEM((LSLOTS * 2 * SLOTS,), jnp.int32),
        pltpu.VMEM((CHUNK + 8, E), jnp.float32),
        pltpu.SemaphoreType.DMA((LSLOTS,)),
    ]
    if widen:
        table = pltpu.with_memory_space_constraint(table, pltpu.HBM)
        scratch = [pltpu.VMEM((TSLOTS, TBLK, E), jnp.bfloat16), pltpu.SemaphoreType.DMA((TSLOTS,))] + scratch
    return pl.pallas_call(
        functools.partial(gather_body, unroll=unroll, widen=widen, first=first, ahead=ahead),
        out_shape=(sums, pltpu.VMEM((ROWS_DEV + 8, E), jnp.float32)) if widen else sums,
        in_specs=[
            pl.BlockSpec(memory_space=pltpu.SMEM),
            pl.BlockSpec(memory_space=pl.ANY),
            pl.BlockSpec(memory_space=pltpu.HBM) if widen else vmem,
        ],
        out_specs=(vmem, vmem) if widen else vmem,
        scratch_shapes=scratch,
        compiler_params=pltpu.CompilerParams(vmem_limit_bytes=(8 if widen else 4) * 2**20),
        name="bag_gather",
    )(y, lists, table)


def combine_body(y_ref, lists_ref, part_0, part_1, part_2, part_3, part_3b, out_ref):
    y = y_ref[0]
    parts = (part_0, part_1, part_2)
    half = part_3.shape[0]
    bag = lax.broadcasted_iota(jnp.int32, (CHUNK, 4 * CHUNK), 0)
    for c in range(out_ref.shape[0]):
        source = 8 * (c // 2) + 2 * y + c % 2
        words = lax.shift_right_logical(lists_ref[source], 20) & (CHUNK - 1)
        where = jnp.concatenate([words[2:3, :], words[3:4, :]], axis=1)
        pick = (bag == where).astype(jnp.float32).astype(jnp.bfloat16)
        rows = []
        for j in range(4):
            came = (y - j) & 3
            row = part_3[c] if c < half else part_3b[c - half]
            for k in range(3):
                row = jnp.where(came == k, parts[k][c], row)
            rows.append(row)
        total = jnp.dot(pick, jnp.concatenate(rows, axis=0), preferred_element_type=jnp.float32)
        out_ref[c] = total.astype(jnp.bfloat16)


def combine(y, lists, parts):
    vmem = pl.BlockSpec(memory_space=pltpu.VMEM)
    return pl.pallas_call(
        combine_body,
        out_shape=pltpu.VMEM(parts[0].shape, jnp.bfloat16),
        in_specs=[pl.BlockSpec(memory_space=pltpu.SMEM)] + [vmem] * (1 + len(parts)),
        out_specs=vmem,
        compiler_params=pltpu.CompilerParams(vmem_limit_bytes=4 * 2**20),
        name="bag_combine",
    )(y, lists, *[pltpu.with_memory_space_constraint(p, pltpu.VMEM) for p in parts])


def rows_body(pooled_ref, out_ref):
    for t in range(pooled_ref.shape[0]):
        out_ref[:, t * E : (t + 1) * E] = pooled_ref[t]


def feature_rows(pooled):
    tables, samples, _ = pooled.shape
    vmem = pl.BlockSpec(memory_space=pltpu.VMEM)
    return pl.pallas_call(
        rows_body,
        out_shape=pltpu.VMEM((samples, tables * E), jnp.bfloat16),
        in_specs=[vmem],
        out_specs=vmem,
        compiler_params=pltpu.CompilerParams(vmem_limit_bytes=2 * 2**20),
        name="feature_rows",
    )(pltpu.with_memory_space_constraint(pooled, pltpu.VMEM))


def dense_body(section_ref, own_ref, other_ref, w_ref, bias_ref, scale_ref, *refs, stream):
    section = section_ref[0]
    wide = own_ref.shape[1]
    per = wide // WBLK
    blocks = []
    for i in range(2 * per):
        side = section if i < per else 1 - section
        blocks.append(pl.ds(pl.multiple_of(side * wide + i % per * WBLK, WBLK), WBLK))
    if stream:
        out_ref, kept, acc, sem = refs
        copies = [pltpu.make_async_copy(w_ref.at[b], kept.at[b], sem.at[i]) for i, b in enumerate(blocks)]
        for copy in copies:
            copy.start()
    else:
        out_ref, acc = refs
        kept = w_ref
    for i, block in enumerate(blocks):
        if stream:
            copies[i].wait()
        at = i % per * WBLK
        x = (own_ref if i < per else other_ref)[:, at : at + WBLK]
        prod = jnp.dot(x, kept[block, :], preferred_element_type=jnp.float32)
        acc[...] = acc[...] + prod if i else prod
    part = jnp.maximum(acc[...] + bias_ref[...], 0.0) * scale_ref[...]
    lanes = sum(part[:, 128 * i : 128 * i + 128] for i in range(part.shape[1] // 128))
    out_ref[...] = jnp.sum(lanes.T, axis=0, keepdims=True)


def dense(section, own, other, weights, bias, scale, stream):
    vmem = pl.BlockSpec(memory_space=pltpu.VMEM)
    samples = own.shape[0]
    rows, units = weights.shape
    out = pltpu.VMEM((1, samples), jnp.float32)
    scratch = [pltpu.VMEM((samples, units), jnp.float32)]
    if stream:
        weights = pltpu.with_memory_space_constraint(weights, pltpu.HBM)
        scratch.append(pltpu.SemaphoreType.DMA((rows // WBLK,)))
    return pl.pallas_call(
        functools.partial(dense_body, stream=stream),
        out_shape=(out, pltpu.VMEM(weights.shape, weights.dtype)) if stream else out,
        in_specs=[
            pl.BlockSpec(memory_space=pltpu.SMEM),
            vmem,
            vmem,
            pl.BlockSpec(memory_space=pltpu.HBM) if stream else vmem,
            vmem,
            vmem,
        ],
        out_specs=(vmem, vmem) if stream else vmem,
        scratch_shapes=scratch,
        compiler_params=pltpu.CompilerParams(vmem_limit_bytes=8 * 2**20),
        name="dense_near" if stream else "dense_far",
    )(
        section,
        pltpu.with_memory_space_constraint(own, pltpu.VMEM),
        pltpu.with_memory_space_constraint(other, pltpu.VMEM),
        weights,
        bias,
        scale,
    )


def body(indices, pool_len, tables, w_first, b_first, w_out):
    n_dev = lax.axis_size("dev")
    n_sec = lax.axis_size("section")
    section = lax.axis_index("section")
    dev = lax.axis_index("dev")
    lists = prep(jnp.transpose(indices, (1, 2, 0)), pool_len)
    ring = 4
    rows, cols = w_first.shape
    part = cols // HID_SPLIT
    planes = n_dev // ring
    levels = [[ring * p + y for p in range(planes)] for y in range(ring)]
    y = dev % ring
    q = dev % HID_SPLIT
    keep = lax.dynamic_slice(w_first, (0, q * part), (rows, part))
    give = lax.dynamic_slice(w_first, (0, (1 - q) * part), (rows, part))

    def along(x, k):
        return lax.ppermute(x, "dev", [(d, d // ring * ring + (d + k) % ring) for d in range(n_dev)])

    pieces = [keep, along(give, 1), along(keep, 2), along(give, 3)]
    pieces, lists = lax.optimization_barrier((pieces, lists))
    pieces = jnp.stack(pieces)
    pieces = [lax.dynamic_index_in_dim(pieces, (y - k) % ring, 0, False) for k in range(ring)]
    whole = lax.all_gather(jnp.concatenate(pieces), "dev", axis_index_groups=levels, tiled=True)
    both_axes = ("section", "dev")
    arrived = lax.all_to_all(lists.reshape(n_sec * n_dev, 4, 128), both_axes, 0, 0, tiled=True)
    line = lax.broadcasted_iota(jnp.int32, arrived.shape, 1)
    clean = jnp.where(line < 2, arrived, arrived & 0xFFFFF).reshape(-1)
    clean, tables = lax.optimization_barrier((clean, tables))
    here = y.reshape(1)
    split = planes // 2
    parts, tab = {}, None
    for name, k, first, count in CALLS:
        first, count = first * split, count * split
        if tab is None:
            sums, tab = gather(here, k, clean, tables, count, first, widen=True)
        else:
            sums = gather(here, k, clean, tab, count, first)
        parts[name] = along(sums, k) if k else sums
    pooled = combine(here, arrived, [parts[name] for name in "abcde"])
    pooled = pooled.reshape(planes, 2 * CHUNK, E)
    pooled = lax.all_to_all(pooled, "dev", 0, 0, axis_index_groups=levels, tiled=True)
    features = feature_rows(pooled)
    bias = lax.dynamic_slice(b_first, (q * part,), (part,)).astype(jnp.float32)
    scale = lax.dynamic_slice(w_out, (q * part,), (part,)).astype(jnp.float32)
    ways = [[d // ring * ring + (d + (1 if d % 2 == h else ring - 1)) % ring for d in range(n_dev)] for h in range(2)]
    far = [
        lax.ppermute(features[h * CHUNK : (h + 1) * CHUNK], "dev", list(enumerate(ways[h]))) for h in range(2)
    ]
    bias, scale = bias.reshape(1, part), scale.reshape(1, part)
    core = section.reshape(1)

    def crossed(x):
        return lax.ppermute(x, "section", [(0, 1), (1, 0)])

    near, kept = dense(core, features, crossed(features), whole, bias, scale, True)
    near = near.reshape(-1)

    def moved(x, turn, way):
        pairs = [(s * n_dev + d, (s ^ turn) * n_dev + way[d]) for s in range(n_sec) for d in range(n_dev)]
        return lax.ppermute(x, both_axes, pairs)

    far, near = lax.optimization_barrier((far, near))
    near_2 = moved(near, 1, range(n_dev))
    far = jnp.concatenate(far)
    far_part = dense(core, far, crossed(far), kept, bias, scale, False).reshape(-1)
    far_part = (far_part + moved(far_part, 1, range(n_dev))).reshape(2, CHUNK)
    return (near + near_2) + jnp.concatenate([moved(far_part[h], 0, ways[h]) for h in range(2)])


def solution(mesh):
    placed = (
        P(("section", "dev"), None, None),
        P(),
        P(("section", "dev"), None),
        P("dev", "section"),
        P("section"),
        P("section"),
    )
    return jax.shard_map(body, mesh=mesh, in_specs=placed, out_specs=P("dev"), check_vma=False)
```

```python
import functools

import jax
import jax.numpy as jnp
from jax import lax
from jax.experimental import pallas as pl
from jax.experimental.pallas import tpu as pltpu
from jax.sharding import PartitionSpec as P


E = 128
ROWS_DEV = 32768
POOL = 8
CHUNK = 64
SLOTS = POOL * CHUNK
DEAD = ROWS_DEV | (8 << 16)
TBLK = 4096
TSLOTS = 4
LSLOTS = 4
HID_SPLIT = 2
WBLK = 512
CALLS = (("c", 2, 0, 2), ("b", 1, 0, 2), ("d", 3, 0, 1), ("e", 3, 1, 1), ("a", 0, 0, 2))
SORT8 = (
    (0, 2), (1, 3), (4, 6), (5, 7), (0, 4), (1, 5), (2, 6), (3, 7), (0, 1), (2, 3),
    (4, 5), (6, 7), (2, 4), (3, 5), (1, 4), (3, 6), (1, 2), (3, 4), (5, 6),
)


def prep_body(x_ref, pool_ref, list_ref, order_ref, group_ref):
    shape = (CHUNK, 128)
    tables = x_ref.shape[0]
    lane = lax.broadcasted_iota(jnp.int32, shape, 1)
    bag = lax.broadcasted_iota(jnp.int32, shape, 0)
    table = lax.broadcasted_iota(jnp.int32, (8, 128), 1) & (tables - 1)
    live = jnp.zeros((8, 128), jnp.int32)
    for t in range(tables):
        live = jnp.where(table == t, pool_ref[t], live)
    live = jnp.concatenate([live] * (CHUNK // 8), axis=0)
    first = (lane // tables) * ROWS_DEV
    v = []
    for p in range(POOL):
        row = jnp.concatenate([x_ref[:, p, :]] * 4, axis=0).T - first
        ok = (row >= 0) & (row < ROWS_DEV) & (live > p)
        v.append(jnp.where(ok, row, ROWS_DEV))
    for a, b in SORT8:
        v[a], v[b] = jnp.minimum(v[a], v[b]), jnp.maximum(v[a], v[b])
    kept = sum((w < ROWS_DEV).astype(jnp.int32) for w in v)
    cols = [(POOL - kept) * CHUNK + bag]
    cols += [v[2 * k] | (v[2 * k + 1] << 16) for k in range(POOL // 2)]
    size = 2
    while size <= CHUNK:
        step = size // 2
        while step:
            upper = (bag & step) != 0
            small = ((bag & size) == 0) != upper
            other = [
                jnp.where(upper, pltpu.roll(c, step, 0), pltpu.roll(c, CHUNK - step, 0)) for c in cols
            ]
            take = jnp.where(small, other[0] - cols[0], cols[0] - other[0]) < 0
            cols = [jnp.where(take, o, c) for o, c in zip(other, cols)]
            step //= 2
        size *= 2
    key = cols[0]
    order = (((key & (CHUNK - 1)) | CHUNK) << 20).T
    for j in range(4):
        order_ref[:, j * CHUNK : (j + 1) * CHUNK] = order[j * tables : (j + 1) * tables, :]
    kept = POOL - (key >> 6)
    v = []
    for w in cols[1:]:
        v += [w & 0xFFFF, lax.shift_right_logical(w, 16)]
    tile = (8, 128)
    groups = []
    total = jnp.zeros((1, 128), jnp.int32)
    for g in range(CHUNK // 8):
        n = kept[8 * g : 8 * g + 1]
        shift = jnp.broadcast_to((8 * g - total) << 20, tile)
        n_all = jnp.broadcast_to(n, tile)
        for p in range(POOL):
            word = v[p][8 * g : 8 * g + 8] | (g << 16) | shift
            groups.append(jnp.where(n_all > p, word, DEAD))
        total = total + n
    for k in range(6):
        gap = 1 << k
        moves = [((w >> (20 + k)) & 1) != 0 for w in groups]
        new = []
        for i in range(64):
            stay = jnp.where(moves[i], DEAD, groups[i])
            if i + gap < 64:
                stay = jnp.where(moves[i + gap], groups[i + gap], stay)
            new.append(stay)
        groups = new
    head = lax.broadcasted_iota(jnp.int32, tile, 0) == 0
    mask = jnp.where(head, 0xFFFFF, 0xFFFF)
    groups = [w & mask for w in groups]
    groups[0] = groups[0] | jnp.where(head, jnp.broadcast_to(total << 20, tile), 0)
    for k in range(64):
        group_ref[8 * k : 8 * k + 8, :] = groups[k]
    for i in range(4):
        block = [group_ref[pl.ds(2 * i + n, 64, stride=8), :] for n in range(2)]
        block = jnp.concatenate(block, axis=0).T
        for j in range(4):
            rows = block[j * tables : (j + 1) * tables, :]
            if i >= 2:
                rows = rows | order_ref[:, (i - 2) * 128 : (i - 1) * 128]
            list_ref[pl.ds(4 * j + i, tables, stride=16), :] = rows


def prep(ids, pool_len):
    return pl.pallas_call(
        prep_body,
        out_shape=pltpu.VMEM((128 * 4, 128), jnp.int32),
        out_specs=pl.BlockSpec(memory_space=pltpu.VMEM),
        in_specs=[pl.BlockSpec(memory_space=pltpu.VMEM), pl.BlockSpec(memory_space=pltpu.SMEM)],
        scratch_shapes=[pltpu.VMEM((ids.shape[0], 4 * CHUNK), jnp.int32), pltpu.VMEM((SLOTS, 128), jnp.int32)],
        name="bag_lists",
    )(ids, pool_len)


def gather_body(y_ref, lists_ref, *refs, unroll, widen, first, ahead):
    if widen:
        table_ref, out_ref, tab, tbuf, tsem, smem, acc, lsem = refs
    else:
        tab, out_ref, smem, acc, lsem = refs
    quarter = (y_ref[0] + ahead) & 3
    planes = out_ref.shape[0] // 2
    piece = 2 * SLOTS

    def list_copy(m, slot):
        start = pl.multiple_of((4 * (first + m) + quarter) * piece, piece)
        return pltpu.make_async_copy(
            lists_ref.at[pl.ds(start, piece)], smem.at[pl.ds(slot * piece, piece)], lsem.at[slot]
        )

    if widen:

        def table_copy(b):
            slot = b % TSLOTS
            return pltpu.make_async_copy(
                table_ref.at[pl.ds(b * TBLK, TBLK)], tbuf.at[slot], tsem.at[slot]
            )

        blocks = ROWS_DEV // TBLK
        for b in range(TSLOTS):
            table_copy(b).start()
    for slot in range(LSLOTS):
        list_copy(slot, slot).start()
    if widen:
        tab[pl.ds(ROWS_DEV, 8), :] = jnp.zeros((8, E), jnp.float32)
        for b in range(blocks):
            table_copy(b).wait()
            tab[pl.ds(b * TBLK, TBLK), :] = tbuf[b % TSLOTS].astype(jnp.float32)
            if b + TSLOTS < blocks:
                table_copy(b + TSLOTS).start()

    def chunk(slot, h, c):
        at = slot * piece + h * SLOTS
        words = [smem.at[pl.ds(at + 64 * i, 64)] for i in range(8)]
        acc[...] = jnp.zeros(acc.shape, jnp.float32)
        levels = words[0][0] >> 20

        def level(n):
            head = words[0][n]
            rows = [head & 0xFFFF] + [w[n] for w in words[1:]]
            rows = jnp.concatenate([tab[pl.ds(r, 1), :] for r in rows], axis=0)
            return pl.multiple_of((head >> 13) & 0x78, 8), rows

        def step(k, carry):
            for g, rows in [level(k * unroll + u) for u in range(unroll)]:
                acc[pl.ds(g, 8), :] += rows
            return carry

        lax.fori_loop(0, (levels + unroll - 1) >> (unroll.bit_length() - 1), step, 0)
        out_ref[c] = acc[pl.ds(0, CHUNK), :].astype(jnp.bfloat16)

    def round_of(n, carry):
        for slot in range(LSLOTS):
            m = n * LSLOTS + slot
            list_copy(m, slot).wait()
            for h in range(2):
                chunk(slot, h, 2 * m + h)

            @pl.when(m + LSLOTS < planes)
            def _():
                list_copy(m + LSLOTS, slot).start()

        return carry

    lax.fori_loop(0, planes // LSLOTS, round_of, 0)


def gather(y, ahead, lists, table, planes, first=0, unroll=4, widen=False):
    vmem = pl.BlockSpec(memory_space=pltpu.VMEM)
    sums = pltpu.VMEM((2 * planes, CHUNK, E), jnp.bfloat16)
    scratch = [
        pltpu.SMEM((LSLOTS * 2 * SLOTS,), jnp.int32),
        pltpu.VMEM((CHUNK + 8, E), jnp.float32),
        pltpu.SemaphoreType.DMA((LSLOTS,)),
    ]
    if widen:
        table = pltpu.with_memory_space_constraint(table, pltpu.HBM)
        scratch = [pltpu.VMEM((TSLOTS, TBLK, E), jnp.bfloat16), pltpu.SemaphoreType.DMA((TSLOTS,))] + scratch
    return pl.pallas_call(
        functools.partial(gather_body, unroll=unroll, widen=widen, first=first, ahead=ahead),
        out_shape=(sums, pltpu.VMEM((ROWS_DEV + 8, E), jnp.float32)) if widen else sums,
        in_specs=[
            pl.BlockSpec(memory_space=pltpu.SMEM),
            pl.BlockSpec(memory_space=pl.ANY),
            pl.BlockSpec(memory_space=pltpu.HBM) if widen else vmem,
        ],
        out_specs=(vmem, vmem) if widen else vmem,
        scratch_shapes=scratch,
        compiler_params=pltpu.CompilerParams(vmem_limit_bytes=(8 if widen else 4) * 2**20),
        name="bag_gather",
    )(y, lists, table)


def combine_body(y_ref, lists_ref, part_0, part_1, part_2, part_3, part_3b, out_ref):
    y = y_ref[0]
    parts = (part_0, part_1, part_2)
    half = part_3.shape[0]
    bag = lax.broadcasted_iota(jnp.int32, (CHUNK, 4 * CHUNK), 0)
    for c in range(out_ref.shape[0]):
        source = 8 * (c // 2) + 2 * y + c % 2
        words = lax.shift_right_logical(lists_ref[source], 20) & (CHUNK - 1)
        where = jnp.concatenate([words[2:3, :], words[3:4, :]], axis=1)
        pick = (bag == where).astype(jnp.float32).astype(jnp.bfloat16)
        rows = []
        for j in range(4):
            came = (y - j) & 3
            row = part_3[c] if c < half else part_3b[c - half]
            for k in range(3):
                row = jnp.where(came == k, parts[k][c], row)
            rows.append(row)
        total = jnp.dot(pick, jnp.concatenate(rows, axis=0), preferred_element_type=jnp.float32)
        out_ref[c] = total.astype(jnp.bfloat16)


def combine(y, lists, parts):
    vmem = pl.BlockSpec(memory_space=pltpu.VMEM)
    return pl.pallas_call(
        combine_body,
        out_shape=pltpu.VMEM(parts[0].shape, jnp.bfloat16),
        in_specs=[pl.BlockSpec(memory_space=pltpu.SMEM)] + [vmem] * (1 + len(parts)),
        out_specs=vmem,
        compiler_params=pltpu.CompilerParams(vmem_limit_bytes=4 * 2**20),
        name="bag_combine",
    )(y, lists, *[pltpu.with_memory_space_constraint(p, pltpu.VMEM) for p in parts])


def rows_body(pooled_ref, out_ref):
    for t in range(pooled_ref.shape[0]):
        out_ref[:, t * E : (t + 1) * E] = pooled_ref[t]


def feature_rows(pooled):
    tables, samples, _ = pooled.shape
    vmem = pl.BlockSpec(memory_space=pltpu.VMEM)
    return pl.pallas_call(
        rows_body,
        out_shape=pltpu.VMEM((samples, tables * E), jnp.bfloat16),
        in_specs=[vmem],
        out_specs=vmem,
        compiler_params=pltpu.CompilerParams(vmem_limit_bytes=2 * 2**20),
        name="feature_rows",
    )(pltpu.with_memory_space_constraint(pooled, pltpu.VMEM))


def dense_body(section_ref, own_ref, other_ref, w_ref, bias_ref, scale_ref, *refs, stream):
    section = section_ref[0]
    wide = own_ref.shape[1]
    per = wide // WBLK
    blocks = []
    for i in range(2 * per):
        side = section if i < per else 1 - section
        blocks.append(pl.ds(pl.multiple_of(side * wide + i % per * WBLK, WBLK), WBLK))
    if stream:
        out_ref, kept, acc, sem = refs
        copies = [pltpu.make_async_copy(w_ref.at[b], kept.at[b], sem.at[i]) for i, b in enumerate(blocks)]
        for copy in copies:
            copy.start()
    else:
        out_ref, acc = refs
        kept = w_ref
    for i, block in enumerate(blocks):
        if stream:
            copies[i].wait()
        at = i % per * WBLK
        x = (own_ref if i < per else other_ref)[:, at : at + WBLK]
        prod = jnp.dot(x, kept[block, :], preferred_element_type=jnp.float32)
        acc[...] = acc[...] + prod if i else prod
    part = jnp.maximum(acc[...] + bias_ref[...], 0.0) * scale_ref[...]
    lanes = sum(part[:, 128 * i : 128 * i + 128] for i in range(part.shape[1] // 128))
    out_ref[...] = jnp.sum(lanes.T, axis=0, keepdims=True)


def dense(section, own, other, weights, bias, scale, stream):
    vmem = pl.BlockSpec(memory_space=pltpu.VMEM)
    samples = own.shape[0]
    rows, units = weights.shape
    out = pltpu.VMEM((1, samples), jnp.float32)
    scratch = [pltpu.VMEM((samples, units), jnp.float32)]
    if stream:
        weights = pltpu.with_memory_space_constraint(weights, pltpu.HBM)
        scratch.append(pltpu.SemaphoreType.DMA((rows // WBLK,)))
    return pl.pallas_call(
        functools.partial(dense_body, stream=stream),
        out_shape=(out, pltpu.VMEM(weights.shape, weights.dtype)) if stream else out,
        in_specs=[
            pl.BlockSpec(memory_space=pltpu.SMEM),
            vmem,
            vmem,
            pl.BlockSpec(memory_space=pltpu.HBM) if stream else vmem,
            vmem,
            vmem,
        ],
        out_specs=(vmem, vmem) if stream else vmem,
        scratch_shapes=scratch,
        compiler_params=pltpu.CompilerParams(vmem_limit_bytes=8 * 2**20),
        name="dense_near" if stream else "dense_far",
    )(
        section,
        pltpu.with_memory_space_constraint(own, pltpu.VMEM),
        pltpu.with_memory_space_constraint(other, pltpu.VMEM),
        weights,
        bias,
        scale,
    )


def body(indices, pool_len, tables, w_first, b_first, w_out):
    n_dev = lax.axis_size("dev")
    n_sec = lax.axis_size("section")
    section = lax.axis_index("section")
    dev = lax.axis_index("dev")
    lists = prep(jnp.transpose(indices, (1, 2, 0)), pool_len)
    ring = 4
    rows, cols = w_first.shape
    part = cols // HID_SPLIT
    planes = n_dev // ring
    levels = [[ring * p + y for p in range(planes)] for y in range(ring)]
    y = dev % ring
    q = dev % HID_SPLIT
    keep = lax.dynamic_slice(w_first, (0, q * part), (rows, part))
    give = lax.dynamic_slice(w_first, (0, (1 - q) * part), (rows, part))

    def along(x, k):
        return lax.ppermute(x, "dev", [(d, d // ring * ring + (d + k) % ring) for d in range(n_dev)])

    pieces = [keep, along(give, 1), along(keep, 2), along(give, 3)]
    pieces, lists = lax.optimization_barrier((pieces, lists))
    pieces = jnp.stack(pieces)
    pieces = [lax.dynamic_index_in_dim(pieces, (y - k) % ring, 0, False) for k in range(ring)]
    whole = lax.all_gather(jnp.concatenate(pieces), "dev", axis_index_groups=levels, tiled=True)
    both_axes = ("section", "dev")
    arrived = lax.all_to_all(lists.reshape(n_sec * n_dev, 4, 128), both_axes, 0, 0, tiled=True)
    line = lax.broadcasted_iota(jnp.int32, arrived.shape, 1)
    clean = jnp.where(line < 2, arrived, arrived & 0xFFFFF).reshape(-1)
    clean, tables = lax.optimization_barrier((clean, tables))
    here = y.reshape(1)
    split = planes // 2
    parts, tab = {}, None
    for name, k, first, count in CALLS:
        first, count = first * split, count * split
        if tab is None:
            sums, tab = gather(here, k, clean, tables, count, first, widen=True)
        else:
            sums = gather(here, k, clean, tab, count, first)
        parts[name] = along(sums, k) if k else sums
    pooled = combine(here, arrived, [parts[name] for name in "abcde"])
    pooled = pooled.reshape(planes, 2 * CHUNK, E)
    pooled = lax.all_to_all(pooled, "dev", 0, 0, axis_index_groups=levels, tiled=True)
    features = feature_rows(pooled)
    bias = lax.dynamic_slice(b_first, (q * part,), (part,)).astype(jnp.float32)
    scale = lax.dynamic_slice(w_out, (q * part,), (part,)).astype(jnp.float32)
    ways = [[d // ring * ring + (d + (1 if d % 2 == h else ring - 1)) % ring for d in range(n_dev)] for h in range(2)]
    far = [features[h * CHUNK : (h + 1) * CHUNK] for h in range(2)]
    far = [lax.ppermute(far[h], "dev", list(enumerate(ways[h]))) for h in range(2)]
    bias, scale = bias.reshape(1, part), scale.reshape(1, part)
    core = section.reshape(1)

    def crossed(x):
        return lax.ppermute(x, "section", [(0, 1), (1, 0)])

    other = crossed(features)
    near, kept = dense(core, features, other, whole, bias, scale, True)
    near = near.reshape(-1)

    def moved(x, turn, way):
        pairs = [(s * n_dev + d, (s ^ turn) * n_dev + way[d]) for s in range(n_sec) for d in range(n_dev)]
        return lax.ppermute(x, both_axes, pairs)

    far, near = lax.optimization_barrier((far, near))
    near_2 = moved(near, 1, range(n_dev))
    far = jnp.concatenate(far)
    far_part = dense(core, far, crossed(far), kept, bias, scale, False).reshape(-1)
    far_part = (far_part + moved(far_part, 1, range(n_dev))).reshape(2, CHUNK)
    return (near + near_2) + jnp.concatenate([moved(far_part[h], 0, ways[h]) for h in range(2)])


def solution(mesh):
    placed = (
        P(("section", "dev"), None, None),
        P(),
        P(("section", "dev"), None),
        P("dev", "section"),
        P("section"),
        P("section"),
    )
    return jax.shard_map(body, mesh=mesh, in_specs=placed, out_specs=P("dev"), check_vma=False)
```
